8 devices in a mesh: dp: 1 (over z), tp: 2 (over y), sp: 4 (over x, core).
Axes of the slice: x: 2, y: 2, z: 1, core: 2. Of those that a mesh axis runs over, the one named last changes fastest.
Arguments:
- k_cache: bfloat16 [4, 4, 4, 8192, 64], P(None, 'dp', 'tp', 'sp')
- v_cache: bfloat16 [4, 4, 4, 8192, 64], P(None, 'dp', 'tp', 'sp')
- lengths: int32 [4], P('dp')
- hidden: bfloat16 [4, 2048], P(('dp', 'sp'))
- ln_gain: bfloat16 [4, 2048], replicated
- w_query: bfloat16 [4, 2048, 2048], P(None, None, 'tp')
- w_key: bfloat16 [4, 2048, 256], P(None, None, 'tp')
- w_value: bfloat16 [4, 2048, 256], P(None, None, 'tp')
- w_out: bfloat16 [4, 2048, 2048], P(None, 'tp')
- w_gate: bfloat16 [4, 2048, 5632], P(None, None, 'tp')
- w_up: bfloat16 [4, 2048, 5632], P(None, None, 'tp')
- w_down: bfloat16 [4, 5632, 2048], P(None, 'tp')
Outputs:
- output 1: bfloat16 [4, 2048], P(('dp', 'sp'))
- output 2: bfloat16 [3, 4, 4, 4096, 64], P(None, ('dp', 'sp'), 'tp')
- output 3: bfloat16 [3, 4, 4, 4096, 64], P(None, ('dp', 'sp'), 'tp')
- output 4: bfloat16 [4, 4, 8192, 64], P(('dp', 'sp'), 'tp')
- output 5: bfloat16 [4, 4, 8192, 64], P(('dp', 'sp'), 'tp')
All inputs are finite; a program needn't handle non-finite values.
Results may differ from the reference program's by a relative error of at most 0.02.
Values are sent between devices in bfloat16 or wider.
A program may use at most 1 GiB of HBM per device.

```python
import jax
import jax.numpy as jnp
from jax import lax

N_ROWS = 4
SEQ_LEN = 8192
MODEL_DIM = 2048
N_HEADS = 32
KV_HEADS = 4
HEAD_DIM = 64
FFN_DIM = 5632
WINDOW = 4096
ROPE_BASE = 50000
N_LAYERS = 4
NORM_EPS = 1e-5


def scaled_normal(key_in, shape, fan_in, spread=1.0):
    return (jax.random.normal(key_in, shape, jnp.float32) * (spread * fan_in ** -0.5)).astype(jnp.bfloat16)


def draw_lengths(len_key):
    key_lo, key_hi = jax.random.split(len_key)
    lengths = jax.random.randint(key_lo, (N_ROWS,), WINDOW + 1, SEQ_LEN, jnp.int32)
    order = jax.random.permutation(key_hi, N_ROWS)
    lengths = lengths.at[order[0]].set(SEQ_LEN - 1)
    return lengths.at[order[1]].set(WINDOW + 1)


def setup_inputs(seed: int = 0, part: int = 0) -> dict:
    base_key = jax.random.key(seed)
    part_key = jax.random.fold_in(base_key, part)
    part_keys = jax.random.split(part_key, 3)
    cache_shape = (N_LAYERS, N_ROWS, KV_HEADS, SEQ_LEN, HEAD_DIM)
    k_cache = (2.5 * jax.random.normal(part_keys[0], cache_shape, jnp.float32)).astype(jnp.bfloat16)
    v_cache = jax.random.normal(part_keys[1], cache_shape, jnp.float32).astype(jnp.bfloat16)
    hidden = jax.random.normal(part_keys[2], (N_ROWS, MODEL_DIM), jnp.float32).astype(jnp.bfloat16)
    lengths = draw_lengths(jax.random.fold_in(part_key, 3))
    shared = jax.random.split(jax.random.fold_in(base_key, 1000), 8)
    q_width = N_HEADS * HEAD_DIM
    kv_width = KV_HEADS * HEAD_DIM
    ln_gain = jax.random.uniform(shared[0], (N_LAYERS, MODEL_DIM), jnp.float32, 0.5, 1.5).astype(jnp.bfloat16)
    return {
        "k_cache": k_cache,
        "v_cache": v_cache,
        "lengths": lengths,
        "hidden": hidden,
        "ln_gain": ln_gain,
        "w_query": scaled_normal(shared[1], (N_LAYERS, MODEL_DIM, q_width), MODEL_DIM),
        "w_key": scaled_normal(shared[2], (N_LAYERS, MODEL_DIM, kv_width), MODEL_DIM, 8.0),
        "w_value": scaled_normal(shared[3], (N_LAYERS, MODEL_DIM, kv_width), MODEL_DIM, 2.0),
        "w_out": scaled_normal(shared[4], (N_LAYERS, q_width, MODEL_DIM), q_width),
        "w_gate": scaled_normal(shared[5], (N_LAYERS, MODEL_DIM, FFN_DIM), MODEL_DIM),
        "w_up": scaled_normal(shared[6], (N_LAYERS, MODEL_DIM, FFN_DIM), MODEL_DIM),
        "w_down": scaled_normal(shared[7], (N_LAYERS, FFN_DIM, MODEL_DIM), FFN_DIM),
    }


def layer_norm(rows_in, gain):
    rows32 = rows_in.astype(jnp.float32)
    centered = rows32 - rows32.mean(axis=-1, keepdims=True)
    variance = (centered * centered).mean(axis=-1, keepdims=True)
    scaled = centered * lax.rsqrt(variance + NORM_EPS)
    return (scaled * gain.astype(jnp.float32)).astype(jnp.bfloat16)


def rotary(proj, positions, n_groups):
    half_dim = HEAD_DIM // 2
    inv_freq = 1.0 / (ROPE_BASE ** (jnp.arange(half_dim, dtype=jnp.float32) * 2.0 / HEAD_DIM))
    angles = positions.astype(jnp.float32)[:, None] * inv_freq[None, :]
    cosine = jnp.cos(angles)[:, None, :]
    sine = jnp.sin(angles)[:, None, :]
    heads = proj.reshape(proj.shape[0], n_groups, HEAD_DIM)
    first = heads[..., :half_dim]
    second = heads[..., half_dim:]
    turned = jnp.concatenate([first * cosine - second * sine, second * cosine + first * sine], axis=-1)
    return turned.reshape(proj.shape)


def attend(query, keys, values, key_valid):
    group_size = N_HEADS // KV_HEADS

    def one_row(row):
        q_row, k_row, v_row, ok_row = row
        grouped = q_row.reshape(KV_HEADS, group_size, HEAD_DIM).astype(jnp.float32)
        scores = jnp.einsum("kgd,ksd->kgs", grouped, k_row.astype(jnp.float32)) * HEAD_DIM ** -0.5
        scores = jnp.where(ok_row[None, None, :], scores, -1e30)
        weights = jax.nn.softmax(scores, axis=-1).astype(jnp.bfloat16)
        mixed = jnp.einsum("kgs,ksd->kgd", weights.astype(jnp.float32), v_row.astype(jnp.float32))
        return mixed.astype(jnp.bfloat16).reshape(N_HEADS * HEAD_DIM)

    return lax.map(one_row, (query, keys, values, key_valid))


def reference(k_cache, v_cache, lengths, hidden, ln_gain, w_query, w_key, w_value, w_out, w_gate, w_up, w_down):
    slot_ids = jnp.arange(WINDOW, dtype=jnp.int32)
    slot_pos = lengths[:, None] - (lengths[:, None] - slot_ids[None, :]) % WINDOW
    seq_ids = jnp.arange(SEQ_LEN, dtype=jnp.int32)
    window_valid = jnp.ones((N_ROWS, WINDOW), dtype=jnp.bool_)
    global_valid = seq_ids[None, :] <= lengths[:, None]
    before_new = (seq_ids[None, :] < lengths[:, None])[:, None, :, None]
    at_new = (seq_ids[None, :] == lengths[:, None])[:, None, :, None]
    slot_new = (slot_pos == lengths[:, None])[:, None, :, None]
    slot_index = slot_pos[:, None, :, None]
    residual = hidden
    windows_k = []
    windows_v = []
    for layer in range(N_LAYERS):
        sliding = layer < N_LAYERS - 1
        normed = layer_norm(residual, ln_gain[layer])
        query = jnp.dot(normed, w_query[layer], preferred_element_type=jnp.float32)
        key_new = jnp.dot(normed, w_key[layer], preferred_element_type=jnp.float32)
        value_new = jnp.dot(normed, w_value[layer], preferred_element_type=jnp.float32)
        if sliding:
            query = rotary(query, lengths, N_HEADS)
            key_new = rotary(key_new, lengths, KV_HEADS)
        query = query.astype(jnp.bfloat16).reshape(N_ROWS, N_HEADS, HEAD_DIM)
        key_new = key_new.astype(jnp.bfloat16).reshape(N_ROWS, KV_HEADS, 1, HEAD_DIM)
        value_new = value_new.astype(jnp.bfloat16).reshape(N_ROWS, KV_HEADS, 1, HEAD_DIM)
        if sliding:
            keys = jnp.where(slot_new, key_new, jnp.take_along_axis(k_cache[layer], slot_index, axis=2))
            values = jnp.where(slot_new, value_new, jnp.take_along_axis(v_cache[layer], slot_index, axis=2))
            windows_k.append(keys)
            windows_v.append(values)
            key_valid = window_valid
        else:
            keys = jnp.where(at_new, key_new, jnp.where(before_new, k_cache[layer], 0))
            values = jnp.where(at_new, value_new, jnp.where(before_new, v_cache[layer], 0))
            key_valid = global_valid
        mixed = attend(query, keys, values, key_valid)
        attn_out = jnp.dot(mixed, w_out[layer], preferred_element_type=jnp.float32)
        gate_proj = jnp.dot(normed, w_gate[layer], preferred_element_type=jnp.float32)
        up_proj = jnp.dot(normed, w_up[layer], preferred_element_type=jnp.float32)
        activated = (jax.nn.silu(gate_proj) * up_proj).astype(jnp.bfloat16)
        mlp_out = jnp.dot(activated, w_down[layer], preferred_element_type=jnp.float32)
        residual = (residual.astype(jnp.float32) + attn_out + mlp_out).astype(jnp.bfloat16)
    return residual, jnp.stack(windows_k), jnp.stack(windows_v), keys, values
```

```python
import functools

import jax
import jax.numpy as jnp
from jax import lax
from jax.experimental import pallas as pl
from jax.experimental.pallas import tpu as pltpu
from jax.sharding import PartitionSpec as P


WINDOW = 4096
ROPE_BASE = 50000
NORM_EPS = 1e-5
SHARD = 2048
CHUNK = 128
HEAD_DIM = 64
DEPTH = 4
TILE = 256
CROSS = [(0, 2), (2, 0), (1, 3), (3, 1)]
CROSS_SWAP = [(0, 3), (3, 0), (1, 2), (2, 1)]
PARTNER = [(0, 1), (1, 0), (2, 3), (3, 2)]

VMEM = pl.BlockSpec(memory_space=pltpu.VMEM)
SMEM = pl.BlockSpec(memory_space=pltpu.SMEM)
ANY = pl.BlockSpec(memory_space=pltpu.HBM)


def params(mib=40, **extra):
    return pltpu.CompilerParams(vmem_limit_bytes=mib * 2**20, **extra)


def place():
    sp = lax.axis_index("sp")
    return sp, lax.rem(sp, 2), sp // 2


def far_chunks(length, on_first_chip):
    turn = length - WINDOW
    start = jnp.where(on_first_chip, 0, (turn + 1) // CHUNK)
    count = jnp.where(on_first_chip, (turn + CHUNK - 1) // CHUNK, WINDOW // CHUNK - (turn + 1) // CHUNK)
    return start, count


def swap_kernel(layers, k_ref, v_ref, far_o, near_o, send_sem, recv_sem):
    sp, core, chip = place()
    peer = sp + 1 - 2 * core
    barrier = pltpu.get_barrier_semaphore()
    pl.semaphore_signal(barrier, inc=1, device_id={"sp": peer}, device_id_type=pl.DeviceIdType.MESH)
    pl.semaphore_wait(barrier, 1)
    far_rows = pl.ds(2 * (1 - chip), 2)

    def send(src, dst, i):
        return pltpu.make_async_remote_copy(
            src_ref=src, dst_ref=dst, send_sem=send_sem.at[i], recv_sem=recv_sem.at[i],
            device_id={"sp": peer}, device_id_type=pl.DeviceIdType.MESH)

    copies = []
    for i, (layer, sliding) in enumerate(layers):
        if sliding:
            @pl.when(core == 0)
            def _(layer=layer, i=i):
                send(v_ref.at[layer, far_rows], far_o.at[i], 3 * i).start()

            @pl.when(core == 1)
            def _(layer=layer, i=i):
                send(k_ref.at[layer, far_rows], far_o.at[i], 3 * i).start()

            copies.append(send(k_ref.at[layer, far_rows], far_o.at[i], 3 * i))
        pair = [send(k_ref.at[layer, peer], near_o.at[i, 0], 3 * i + 1),
                send(v_ref.at[layer, peer], near_o.at[i, 1], 3 * i + 2)]
        for copy in pair:
            copy.start()
        copies += pair
    for copy in copies:
        copy.wait()


def swap(layers, k_t, v_t, collective_id):
    n = len(layers)
    block = jax.ShapeDtypeStruct((n, 2, 2, HEAD_DIM, SHARD), jnp.bfloat16)
    return pl.pallas_call(
        functools.partial(swap_kernel, layers),
        out_shape=[block, block],
        in_specs=[ANY, ANY], out_specs=[ANY, ANY],
        scratch_shapes=[pltpu.SemaphoreType.DMA((3 * n,)), pltpu.SemaphoreType.DMA((3 * n,))],
        compiler_params=params(60, collective_id=collective_id, has_side_effects=True),
        cost_estimate=pl.CostEstimate(flops=10**9, bytes_accessed=4 * 2**20, transcendentals=0),
        name="swap",
    )(k_t, v_t)


def payload_kernel(layer, k_ref, v_ref, same_o, cross_o, sems):
    sp, core, chip = place()
    rows = (sp + 2 - 4 * chip, 2 * (1 - chip) + 1 - core)
    copies = [pltpu.make_async_copy(ref.at[layer, row], out.at[i], sems.at[2 * j + i])
              for j, (row, out) in enumerate(zip(rows, (same_o, cross_o)))
              for i, ref in enumerate((k_ref, v_ref))]
    for copy in copies:
        copy.start()
    for copy in copies:
        copy.wait()


def payload(layer, k_t, v_t):
    block = jax.ShapeDtypeStruct((2, 2, HEAD_DIM, SHARD), jnp.bfloat16)
    return pl.pallas_call(
        functools.partial(payload_kernel, layer),
        out_shape=[block, block],
        in_specs=[ANY, ANY], out_specs=[VMEM, VMEM],
        scratch_shapes=[pltpu.SemaphoreType.DMA((4,))],
        compiler_params=params(60),
        cost_estimate=pl.CostEstimate(flops=10**9, bytes_accessed=4 * 2**20, transcendentals=0),
        name="payload",
    )(k_t, v_t)


def swap_partials(part_ref, other_ref, sems):
    tp_peer = 1 - lax.axis_index("tp")
    barrier = pltpu.get_barrier_semaphore()
    pl.semaphore_signal(barrier, inc=1, device_id={"tp": tp_peer}, device_id_type=pl.DeviceIdType.MESH)
    pl.semaphore_wait(barrier, 1)
    copy = pltpu.make_async_remote_copy(
        src_ref=part_ref, dst_ref=other_ref, send_sem=sems.at[0], recv_sem=sems.at[1],
        device_id={"tp": tp_peer}, device_id_type=pl.DeviceIdType.MESH)
    copy.start()
    copy.wait()


def front_kernel(layer, sliding, exchange, *refs):
    if exchange:
        (h_ref, part_ref, gain_ref, cos_ref, sin_ref, wq, wk, wv, wg, wu, wd,
         q_o, k_o, v_o, m_o, h_o,
         wq_b, wk_b, wv_b, wg_b, wu_b, wd_b, qkv_sem, mlp_sem, other_ref, rdma_sem) = refs
    else:
        (h_ref, gain_ref, cos_ref, sin_ref, wq, wk, wv, wg, wu, wd,
         q_o, k_o, v_o, m_o, h_o,
         wq_b, wk_b, wv_b, wg_b, wu_b, wd_b, qkv_sem, mlp_sem) = refs
    n_tiles = wg.shape[2] // TILE
    qkv = [pltpu.make_async_copy(src.at[layer], dst, qkv_sem.at[i])
           for i, (src, dst) in enumerate(((wq, wq_b), (wk, wk_b), (wv, wv_b)))]

    def tile_copies(j, slot):
        cols = pl.ds(pl.multiple_of(j * TILE, TILE), TILE)
        return [pltpu.make_async_copy(wg.at[layer, :, cols], wg_b.at[slot], mlp_sem.at[0, slot]),
                pltpu.make_async_copy(wu.at[layer, :, cols], wu_b.at[slot], mlp_sem.at[1, slot]),
                pltpu.make_async_copy(wd.at[layer, cols, :], wd_b.at[slot], mlp_sem.at[2, slot])]

    for copy in qkv:
        copy.start()
    for j in range(DEPTH):
        for copy in tile_copies(j, j):
            copy.start()

    rows = h_ref[...].astype(jnp.float32)
    if exchange:
        swap_partials(part_ref, other_ref, rdma_sem)
        rows = (rows + (part_ref[...] + other_ref[...])).astype(jnp.bfloat16).astype(jnp.float32)
    h_o[...] = rows.astype(jnp.bfloat16)
    centered = rows - rows.mean(axis=-1, keepdims=True)
    variance = (centered * centered).mean(axis=-1, keepdims=True)
    scaled = centered * lax.rsqrt(variance + NORM_EPS)
    normed = (scaled * gain_ref[layer:layer + 1, :].astype(jnp.float32)).astype(jnp.bfloat16)
    normed = jnp.broadcast_to(normed, (8, normed.shape[1]))

    def rotate(x):
        if not sliding:
            return x
        width = x.shape[1]
        first = lax.broadcasted_iota(jnp.int32, x.shape, 1) % HEAD_DIM < HEAD_DIM // 2
        swapped = jnp.where(first, pltpu.roll(x, width - HEAD_DIM // 2, 1), pltpu.roll(x, HEAD_DIM // 2, 1))
        return x * cos_ref[:, :width] + swapped * sin_ref[:, :width]

    for copy in qkv:
        copy.wait()
    q_o[...] = rotate(jnp.dot(normed, wq_b[...], preferred_element_type=jnp.float32))[:1].astype(jnp.bfloat16)
    k_o[...] = rotate(jnp.dot(normed, wk_b[...], preferred_element_type=jnp.float32))[:1].astype(jnp.bfloat16)
    v_o[...] = jnp.dot(normed, wv_b[...], preferred_element_type=jnp.float32)[:1].astype(jnp.bfloat16)

    def tile_step(j, total):
        slot = lax.rem(j, DEPTH)
        for copy in tile_copies(j, slot):
            copy.wait()
        gate = jnp.dot(normed, wg_b[slot], preferred_element_type=jnp.float32)
        up = jnp.dot(normed, wu_b[slot], preferred_element_type=jnp.float32)
        act = (jax.nn.silu(gate) * up).astype(jnp.bfloat16)
        total = total + jnp.dot(act, wd_b[slot], preferred_element_type=jnp.float32)

        @pl.when(j + DEPTH < n_tiles)
        def _():
            for copy in tile_copies(j + DEPTH, slot):
                copy.start()

        return total

    total = lax.fori_loop(0, n_tiles, tile_step, jnp.zeros((8, m_o.shape[1]), jnp.float32))
    m_o[...] = total[:1]


def front(layer, sliding, h, part, gain, cos, sin, weights):
    exchange = part is not None
    dim = h.shape[1]
    q_width, kv_width = weights[0].shape[2], weights[1].shape[2]
    out = [jax.ShapeDtypeStruct((1, q_width), jnp.bfloat16), jax.ShapeDtypeStruct((1, kv_width), jnp.bfloat16),
           jax.ShapeDtypeStruct((1, kv_width), jnp.bfloat16), jax.ShapeDtypeStruct((1, dim), jnp.float32),
           jax.ShapeDtypeStruct((1, dim), jnp.bfloat16)]
    scratch = [pltpu.VMEM((dim, q_width), jnp.bfloat16), pltpu.VMEM((dim, kv_width), jnp.bfloat16),
               pltpu.VMEM((dim, kv_width), jnp.bfloat16), pltpu.VMEM((DEPTH, dim, TILE), jnp.bfloat16),
               pltpu.VMEM((DEPTH, dim, TILE), jnp.bfloat16), pltpu.VMEM((DEPTH, TILE, dim), jnp.bfloat16),
               pltpu.SemaphoreType.DMA((3,)), pltpu.SemaphoreType.DMA((3, DEPTH))]
    args = [h]
    extra = {}
    if exchange:
        args.append(part)
        scratch += [pltpu.VMEM((1, dim), jnp.float32), pltpu.SemaphoreType.DMA((2,))]
        extra = dict(collective_id=layer, has_side_effects=True)
    args += [gain, cos, sin]
    return pl.pallas_call(
        functools.partial(front_kernel, layer, sliding, exchange),
        out_shape=out,
        in_specs=[VMEM] * len(args) + [ANY] * 6,
        out_specs=[VMEM] * 5,
        scratch_shapes=scratch,
        compiler_params=params(**extra),
        cost_estimate=pl.CostEstimate(flops=6 * 10**9, bytes_accessed=40 * 10**6, transcendentals=0),
    )(*args, *weights)


def final_kernel(h_ref, part_ref, out_ref, other_ref, sems):
    swap_partials(part_ref, other_ref, sems)
    out_ref[...] = (h_ref[...].astype(jnp.float32) + (part_ref[...] + other_ref[...])).astype(jnp.bfloat16)


def final(h, part):
    return pl.pallas_call(
        final_kernel,
        out_shape=jax.ShapeDtypeStruct(h.shape, jnp.bfloat16),
        in_specs=[VMEM, VMEM], out_specs=VMEM,
        scratch_shapes=[pltpu.VMEM(part.shape, jnp.float32), pltpu.SemaphoreType.DMA((2,))],
        compiler_params=pltpu.CompilerParams(collective_id=8, has_side_effects=True),
        name="final",
    )(h, part)


def pack_kernel(layer, n_chunks, lengths, k_ref, v_ref, recv_ref, out_ref, sem):
    _, core, chip = place()
    far_row = 2 * (1 - chip)
    start0, count0 = far_chunks(lengths[far_row], chip == 1)
    start1, _ = far_chunks(lengths[far_row + 1], chip == 1)
    per_shard = SHARD // CHUNK

    def step(j, carry):
        second = j >= count0
        row = jnp.where(second, 1, 0)
        piece = jnp.clip(jnp.where(second, start1 + j - count0, start0 + j), 0, 2 * per_shard - 1)
        own = (piece // per_shard) == core
        lanes = pl.ds(pl.multiple_of(lax.rem(piece, per_shard) * CHUNK, CHUNK), CHUNK)

        @pl.when(own & (core == 0))
        def _():
            pltpu.make_async_copy(k_ref.at[layer, far_row + row, :, :, lanes], out_ref.at[j], sem).start()

        @pl.when(own & (core == 1))
        def _():
            pltpu.make_async_copy(v_ref.at[layer, far_row + row, :, :, lanes], out_ref.at[j], sem).start()

        @pl.when(jnp.logical_not(own))
        def _():
            pltpu.make_async_copy(recv_ref.at[0, row, :, :, lanes], out_ref.at[j], sem).start()

        return carry

    lax.fori_loop(0, n_chunks, step, 0)
    pltpu.make_async_copy(out_ref, out_ref, sem).wait()


def pack(layer, n_chunks, lengths, k_t, v_t, recv):
    return pl.pallas_call(
        functools.partial(pack_kernel, layer, n_chunks),
        out_shape=jax.ShapeDtypeStruct((n_chunks, 2, HEAD_DIM, CHUNK), jnp.bfloat16),
        in_specs=[SMEM, ANY, ANY, ANY], out_specs=VMEM,
        scratch_shapes=[pltpu.SemaphoreType.DMA],
        compiler_params=params(60),
        cost_estimate=pl.CostEstimate(flops=10**9, bytes_accessed=4 * 2**20, transcendentals=0),
    )(lengths, k_t, v_t, recv)


def as_column(row, base):
    wide = jnp.broadcast_to(row[:, base:base + HEAD_DIM].astype(jnp.float32), (HEAD_DIM, HEAD_DIM))
    eye = (lax.broadcasted_iota(jnp.int32, wide.shape, 0) == lax.broadcasted_iota(jnp.int32, wide.shape, 1))
    return jnp.sum(jnp.where(eye, wide, 0.0), axis=1, keepdims=True).astype(jnp.bfloat16)


def spread_mask(group):
    shape = (group, group * HEAD_DIM)
    return lax.broadcasted_iota(jnp.int32, shape, 1) // HEAD_DIM == lax.broadcasted_iota(jnp.int32, shape, 0)


def attend(q_ref, k_buf, v_buf, last):
    kv_local = k_buf.shape[0]
    group = q_ref.shape[1] // (kv_local * HEAD_DIM)
    width = group * HEAD_DIM
    spread = spread_mask(group)
    fold = (lax.broadcasted_iota(jnp.int32, (HEAD_DIM, width), 1) % HEAD_DIM
            == lax.broadcasted_iota(jnp.int32, (HEAD_DIM, width), 0)).astype(jnp.bfloat16)
    rows = []
    for head in range(kv_local):
        q_row = q_ref[:, head * width:(head + 1) * width].astype(jnp.float32)
        q_wide = jnp.where(spread, jnp.broadcast_to(q_row, spread.shape), 0.0).astype(jnp.bfloat16)
        q = lax.dot_general(q_wide, fold, (((1,), (1,)), ((), ())), preferred_element_type=jnp.float32)
        scores = jnp.dot(q.astype(jnp.bfloat16), k_buf[head], preferred_element_type=jnp.float32) * HEAD_DIM ** -0.5
        if last is not None:
            valid = lax.broadcasted_iota(jnp.int32, scores.shape, 1) <= last
            scores = jnp.where(valid, scores, -1e30)
        top = jnp.max(scores, axis=1, keepdims=True)
        expd = jnp.exp(scores - top)
        weights = (expd / jnp.sum(expd, axis=1, keepdims=True)).astype(jnp.bfloat16)
        mixed = lax.dot_general(weights, v_buf[head], (((1,), (1,)), ((), ())), preferred_element_type=jnp.float32)
        wide = jnp.dot(mixed.astype(jnp.bfloat16), fold, preferred_element_type=jnp.float32)
        rows.append(jnp.sum(jnp.where(spread, wide, 0.0), axis=0, keepdims=True).astype(jnp.bfloat16))
    return rows


def project_out(rows, wo_b, mlp_ref, part_o):
    total = mlp_ref[...]
    width = rows[0].shape[1]
    for head, row in enumerate(rows):
        wide = jnp.broadcast_to(row, (8, width))
        total = total + jnp.dot(wide, wo_b[head * width:(head + 1) * width, :], preferred_element_type=jnp.float32)[:1]
    part_o[...] = total


def window_kernel(layer, n_far, aliased, *refs):
    (lengths, q_ref, knew_ref, vnew_ref, mlp_ref, k_ref, v_ref, near_ref, mine_ref, other_ref, wo) = refs[:11]
    refs = refs[13:] if aliased else refs[11:]
    part_o, wk_o, wv_o, k_buf, v_buf, k_far, v_far, wo_b, near_sem, far_sem, wo_sem, out_sem = refs
    row, core, chip = place()
    turn = lengths[row] - WINDOW
    start, _ = far_chunks(lengths[row], chip == 0)
    _, count0 = far_chunks(lengths[2 * chip], chip == 0)
    base = jnp.where(core == 0, 0, count0)
    first = jnp.clip(base, 0, mine_ref.shape[0] - n_far)
    shift = base - first - start
    own = pl.ds(pl.multiple_of(core * SHARD, SHARD), SHARD)
    peer = pl.ds(pl.multiple_of((1 - core) * SHARD, SHARD), SHARD)
    loads = [pltpu.make_async_copy(k_ref.at[layer, row], k_buf.at[:, :, own], near_sem.at[0]),
             pltpu.make_async_copy(v_ref.at[layer, row], v_buf.at[:, :, own], near_sem.at[1]),
             pltpu.make_async_copy(near_ref.at[0, 0], k_buf.at[:, :, peer], near_sem.at[2]),
             pltpu.make_async_copy(near_ref.at[0, 1], v_buf.at[:, :, peer], near_sem.at[3])]
    chunks = pl.ds(first, n_far)

    @pl.when(core == 0)
    def _():
        pltpu.make_async_copy(mine_ref.at[chunks], k_far, far_sem.at[0]).start()
        pltpu.make_async_copy(other_ref.at[chunks], v_far, far_sem.at[1]).start()

    @pl.when(core == 1)
    def _():
        pltpu.make_async_copy(other_ref.at[chunks], k_far, far_sem.at[0]).start()
        pltpu.make_async_copy(mine_ref.at[chunks], v_far, far_sem.at[1]).start()

    for copy in loads:
        copy.start()
    wo_copy = pltpu.make_async_copy(wo.at[layer], wo_b, wo_sem)
    wo_copy.start()
    k_new = [as_column(knew_ref[...], head * HEAD_DIM) for head in range(2)]
    v_new = [as_column(vnew_ref[...], head * HEAD_DIM) for head in range(2)]
    for copy in loads:
        copy.wait()
    pltpu.make_async_copy(mine_ref.at[chunks], k_far, far_sem.at[0]).wait()
    pltpu.make_async_copy(mine_ref.at[chunks], v_far, far_sem.at[1]).wait()

    def step(c, carry):
        lanes = pl.ds(pl.multiple_of(c * CHUNK, CHUNK), CHUNK)
        piece = jnp.clip(c + shift, 0, n_far - 1)
        slots = c * CHUNK + lax.broadcasted_iota(jnp.int32, (HEAD_DIM, CHUNK), 1)
        from_far = jnp.where(chip == 0, turn - slots, slots - turn) > 0
        is_new = slots == turn
        for head in range(2):
            for buf, far, new in ((k_buf, k_far, k_new), (v_buf, v_far, v_new)):
                near = buf[head, :, lanes]
                mixed = jnp.where(from_far, far[piece, head], near)
                buf[head, :, lanes] = jnp.where(is_new, jnp.broadcast_to(new[head], near.shape), mixed)
        return carry

    lax.fori_loop(0, WINDOW // CHUNK, step, 0)
    stores = [pltpu.make_async_copy(k_buf, wk_o.at[layer], out_sem.at[0]),
              pltpu.make_async_copy(v_buf, wv_o.at[layer], out_sem.at[1])]
    for copy in stores:
        copy.start()
    rows = attend(q_ref, k_buf, v_buf, None)
    wo_copy.wait()
    project_out(rows, wo_b, mlp_ref, part_o)
    for copy in stores:
        copy.wait()


def window(layer, lengths, q, k_new, v_new, mlp, k_t, v_t, near, mine, other, wo, outs):
    n_far = min(WINDOW // CHUNK, mine.shape[0])
    aliased = outs is not None
    args = [lengths, q, k_new, v_new, mlp, k_t, v_t, near, mine, other, wo]
    specs = [SMEM] + [VMEM] * 4 + [ANY] * 6
    aliases = {}
    if aliased:
        args += list(outs)
        specs += [ANY, ANY]
        aliases = {11: 1, 12: 2}
    buf = pltpu.VMEM((2, HEAD_DIM, WINDOW), jnp.bfloat16)
    far = pltpu.VMEM((n_far, 2, HEAD_DIM, CHUNK), jnp.bfloat16)
    out = jax.ShapeDtypeStruct((3, 2, HEAD_DIM, WINDOW), jnp.bfloat16)
    return pl.pallas_call(
        functools.partial(window_kernel, layer, n_far, aliased),
        out_shape=[jax.ShapeDtypeStruct(mlp.shape, jnp.float32), out, out],
        in_specs=specs, out_specs=[VMEM, ANY, ANY],
        scratch_shapes=[buf, buf, far, far, pltpu.VMEM(wo.shape[1:], jnp.bfloat16),
                        pltpu.SemaphoreType.DMA((4,)), pltpu.SemaphoreType.DMA((2,)),
                        pltpu.SemaphoreType.DMA, pltpu.SemaphoreType.DMA((2,))],
        input_output_aliases=aliases,
        compiler_params=params(),
        cost_estimate=pl.CostEstimate(flops=3 * 10**9, bytes_accessed=12 * 2**20, transcendentals=0),
    )(*args)


def global_kernel(layer, slot, lengths, q_ref, knew_ref, vnew_ref, mlp_ref, k_ref, v_ref, p1_ref, p2_ref, p3_ref, wo,
                  part_o, gk_o, gv_o, k_buf, v_buf, wo_b, load_sem, wo_sem, out_sem):
    row, core, chip = place()
    last = lengths[row]
    across = row + 2 - 4 * chip
    sources = (row + 1 - 2 * core, across, across + 1 - 2 * core)
    loads = [pltpu.make_async_copy(k_ref.at[layer, row], k_buf.at[:, :, pl.ds(pl.multiple_of(row * SHARD, SHARD), SHARD)], load_sem.at[0]),
             pltpu.make_async_copy(v_ref.at[layer, row], v_buf.at[:, :, pl.ds(pl.multiple_of(row * SHARD, SHARD), SHARD)], load_sem.at[1])]
    for i, ref in enumerate((p1_ref.at[slot], p2_ref, p3_ref)):
        lanes = pl.ds(pl.multiple_of(sources[i] * SHARD, SHARD), SHARD)
        loads += [pltpu.make_async_copy(ref.at[0], k_buf.at[:, :, lanes], load_sem.at[2 + 2 * i]),
                  pltpu.make_async_copy(ref.at[1], v_buf.at[:, :, lanes], load_sem.at[3 + 2 * i])]
    for copy in loads:
        copy.start()
    wo_copy = pltpu.make_async_copy(wo.at[layer], wo_b, wo_sem)
    wo_copy.start()
    k_new = [as_column(knew_ref[...], head * HEAD_DIM) for head in range(2)]
    v_new = [as_column(vnew_ref[...], head * HEAD_DIM) for head in range(2)]
    for copy in loads:
        copy.wait()

    def step(c, carry):
        lanes = pl.ds(pl.multiple_of(c * CHUNK, CHUNK), CHUNK)
        slots = c * CHUNK + lax.broadcasted_iota(jnp.int32, (HEAD_DIM, CHUNK), 1)
        for head in range(2):
            for buf, new in ((k_buf, k_new), (v_buf, v_new)):
                near = buf[head, :, lanes]
                kept = jnp.where(slots < last, near, jnp.zeros_like(near))
                buf[head, :, lanes] = jnp.where(slots == last, jnp.broadcast_to(new[head], near.shape), kept)
        return carry

    lax.fori_loop(WINDOW // CHUNK, 2 * WINDOW // CHUNK, step, 0)
    stores = [pltpu.make_async_copy(k_buf, gk_o, out_sem.at[0]), pltpu.make_async_copy(v_buf, gv_o, out_sem.at[1])]
    for copy in stores:
        copy.start()
    rows = attend(q_ref, k_buf, v_buf, last)
    wo_copy.wait()
    project_out(rows, wo_b, mlp_ref, part_o)
    for copy in stores:
        copy.wait()


def global_layer(layer, slot, lengths, q, k_new, v_new, mlp, k_t, v_t, pieces, wo):
    buf = pltpu.VMEM((2, HEAD_DIM, 4 * SHARD), jnp.bfloat16)
    out = jax.ShapeDtypeStruct((2, HEAD_DIM, 4 * SHARD), jnp.bfloat16)
    return pl.pallas_call(
        functools.partial(global_kernel, layer, slot),
        out_shape=[jax.ShapeDtypeStruct(mlp.shape, jnp.float32), out, out],
        in_specs=[SMEM] + [VMEM] * 4 + [ANY] * 6, out_specs=[VMEM, ANY, ANY],
        scratch_shapes=[buf, buf, pltpu.VMEM(wo.shape[1:], jnp.bfloat16), pltpu.SemaphoreType.DMA((8,)),
                        pltpu.SemaphoreType.DMA, pltpu.SemaphoreType.DMA((2,))],
        compiler_params=params(),
        cost_estimate=pl.CostEstimate(flops=3 * 10**9, bytes_accessed=14 * 2**20, transcendentals=0),
        name="global",
    )(lengths, q, k_new, v_new, mlp, k_t, v_t, *pieces, wo)


def decode(n_chunks, k_t, v_t, lengths, hidden, ln_gain, w_query, w_key, w_value, w_out, w_gate, w_up, w_down):
    n_layers = w_query.shape[0]
    my_length = lengths[lax.axis_index("sp")]
    half_dim = HEAD_DIM // 2
    inv_freq = 1.0 / (ROPE_BASE ** (jnp.arange(half_dim, dtype=jnp.float32) * 2.0 / HEAD_DIM))
    angles = my_length.astype(jnp.float32) * inv_freq
    cosine, sine = jnp.cos(angles), jnp.sin(angles)
    n_heads = w_query.shape[2] // HEAD_DIM
    cos = jnp.tile(jnp.concatenate([cosine, cosine]), n_heads)[None]
    sin = jnp.tile(jnp.concatenate([-sine, sine]), n_heads)[None]

    last = n_layers - 1
    streams = []
    for layer in range(last):
        traded = ((layer, True),) if layer < last - 1 else ((layer, True), (last, False))
        far, near = swap(traded, k_t, v_t, 5 + layer)
        packed = pack(layer, n_chunks, lengths, k_t, v_t, far)
        mine = lax.ppermute(packed, "sp", CROSS)
        other = lax.ppermute(mine, "sp", PARTNER)
        streams.append((near, mine, other))
    same, crossed = payload(last, k_t, v_t)
    same = lax.ppermute(same, "sp", CROSS)
    crossed = lax.ppermute(crossed, "sp", CROSS_SWAP)

    residual, part, outs = hidden, None, None
    for layer in range(n_layers):
        sliding = layer < last
        q, k_new, v_new, mlp, residual = front(layer, sliding, residual, part, ln_gain, cos, sin,
                                               (w_query, w_key, w_value, w_gate, w_up, w_down))
        if sliding:
            near_l, mine, other = streams[layer]
            part, *outs = window(layer, lengths, q, k_new, v_new, mlp, k_t, v_t, near_l, mine, other, w_out, outs)
        else:
            part, global_k, global_v = global_layer(layer, 1, lengths, q, k_new, v_new, mlp, k_t, v_t,
                                                    (near, same, crossed), w_out)
    return final(residual, part), outs[0], outs[1], global_k, global_v


def solution(mesh):
    cache_spec = P(None, "dp", "tp", "sp", None)
    row_spec = P(("dp", "sp"), None)
    col_spec = P(None, None, "tp")
    inner_spec = P(None, "tp", None)
    window_spec = P(None, ("dp", "sp"), "tp", None, None)
    global_spec = P(("dp", "sp"), "tp", None, None)
    in_specs = (cache_spec, cache_spec, P("dp"), row_spec, P(None, None), col_spec, col_spec, col_spec, inner_spec, col_spec, col_spec, inner_spec)
    out_specs = (row_spec, window_spec, window_spec, global_spec, global_spec)

    def device_step(k_cache, v_cache, *rest):
        k_t, v_t = jnp.swapaxes(k_cache, 3, 4), jnp.swapaxes(v_cache, 3, 4)
        h, wk, wv, gk, gv = decode(64, k_t, v_t, *rest)
        turn = lambda x: jnp.swapaxes(x, -1, -2)
        return h, turn(wk)[:, None], turn(wv)[:, None], turn(gk)[None], turn(gv)[None]

    return jax.shard_map(device_step, mesh=mesh, in_specs=in_specs, out_specs=out_specs, check_vma=False)
```

```python
import functools

import jax
import jax.numpy as jnp
from jax import lax
from jax.experimental import pallas as pl
from jax.experimental.pallas import tpu as pltpu
from jax.sharding import PartitionSpec as P


WINDOW = 4096
ROPE_BASE = 50000
NORM_EPS = 1e-5
SHARD = 2048
CHUNK = 128
HEAD_DIM = 64
DEPTH = 4
TILE = 256
CROSS = [(0, 2), (2, 0), (1, 3), (3, 1)]
CROSS_SWAP = [(0, 3), (3, 0), (1, 2), (2, 1)]
PARTNER = [(0, 1), (1, 0), (2, 3), (3, 2)]

VMEM = pl.BlockSpec(memory_space=pltpu.VMEM)
SMEM = pl.BlockSpec(memory_space=pltpu.SMEM)
ANY = pl.BlockSpec(memory_space=pltpu.HBM)


def params(mib=40, **extra):
    return pltpu.CompilerParams(vmem_limit_bytes=mib * 2**20, **extra)


def place():
    sp = lax.axis_index("sp")
    return sp, lax.rem(sp, 2), sp // 2


def far_chunks(length, on_first_chip):
    turn = length - WINDOW
    start = jnp.where(on_first_chip, 0, (turn + 1) // CHUNK)
    count = jnp.where(on_first_chip, (turn + CHUNK - 1) // CHUNK, WINDOW // CHUNK - (turn + 1) // CHUNK)
    return start, count


def swap_kernel(layers, k_ref, v_ref, far_o, near_o, send_sem, recv_sem):
    sp, core, chip = place()
    peer = sp + 1 - 2 * core
    barrier = pltpu.get_barrier_semaphore()
    pl.semaphore_signal(barrier, inc=1, device_id={"sp": peer}, device_id_type=pl.DeviceIdType.MESH)
    pl.semaphore_wait(barrier, 1)
    far_rows = pl.ds(2 * (1 - chip), 2)

    def send(src, dst, i):
        return pltpu.make_async_remote_copy(
            src_ref=src, dst_ref=dst, send_sem=send_sem.at[i], recv_sem=recv_sem.at[i],
            device_id={"sp": peer}, device_id_type=pl.DeviceIdType.MESH)

    copies = []
    for i, (layer, sliding) in enumerate(layers):
        if sliding:
            @pl.when(core == 0)
            def _(layer=layer, i=i):
                send(v_ref.at[layer, far_rows], far_o.at[i], 3 * i).start()

            @pl.when(core == 1)
            def _(layer=layer, i=i):
                send(k_ref.at[layer, far_rows], far_o.at[i], 3 * i).start()

            copies.append(send(k_ref.at[layer, far_rows], far_o.at[i], 3 * i))
        pair = [send(k_ref.at[layer, peer], near_o.at[i, 0], 3 * i + 1),
                send(v_ref.at[layer, peer], near_o.at[i, 1], 3 * i + 2)]
        for copy in pair:
            copy.start()
        copies += pair
    for copy in copies:
        copy.wait()


def swap(layers, k_t, v_t, collective_id):
    n = len(layers)
    block = jax.ShapeDtypeStruct((n, 2, 2, HEAD_DIM, SHARD), jnp.bfloat16)
    return pl.pallas_call(
        functools.partial(swap_kernel, layers),
        out_shape=[block, block],
        in_specs=[ANY, ANY], out_specs=[ANY, ANY],
        scratch_shapes=[pltpu.SemaphoreType.DMA((3 * n,)), pltpu.SemaphoreType.DMA((3 * n,))],
        compiler_params=params(60, collective_id=collective_id, has_side_effects=True),
        cost_estimate=pl.CostEstimate(flops=10**9, bytes_accessed=4 * 2**20, transcendentals=0),
        name="swap",
    )(k_t, v_t)


def payload_kernel(layer, k_ref, v_ref, same_o, cross_o, sems):
    sp, core, chip = place()
    rows = (sp + 2 - 4 * chip, 2 * (1 - chip) + 1 - core)
    copies = [pltpu.make_async_copy(ref.at[layer, row], out.at[i], sems.at[2 * j + i])
              for j, (row, out) in enumerate(zip(rows, (same_o, cross_o)))
              for i, ref in enumerate((k_ref, v_ref))]
    for copy in copies:
        copy.start()
    for copy in copies:
        copy.wait()


def payload(layer, k_t, v_t):
    block = jax.ShapeDtypeStruct((2, 2, HEAD_DIM, SHARD), jnp.bfloat16)
    return pl.pallas_call(
        functools.partial(payload_kernel, layer),
        out_shape=[block, block],
        in_specs=[ANY, ANY], out_specs=[VMEM, VMEM],
        scratch_shapes=[pltpu.SemaphoreType.DMA((4,))],
        compiler_params=params(60),
        cost_estimate=pl.CostEstimate(flops=10**9, bytes_accessed=4 * 2**20, transcendentals=0),
        name="payload",
    )(k_t, v_t)


def swap_partials(part_ref, other_ref, sems):
    tp_peer = 1 - lax.axis_index("tp")
    barrier = pltpu.get_barrier_semaphore()
    pl.semaphore_signal(barrier, inc=1, device_id={"tp": tp_peer}, device_id_type=pl.DeviceIdType.MESH)
    pl.semaphore_wait(barrier, 1)
    copy = pltpu.make_async_remote_copy(
        src_ref=part_ref, dst_ref=other_ref, send_sem=sems.at[0], recv_sem=sems.at[1],
        device_id={"tp": tp_peer}, device_id_type=pl.DeviceIdType.MESH)
    copy.start()
    copy.wait()


def front_kernel(layer, sliding, exchange, *refs):
    if exchange:
        (h_ref, part_ref, gain_ref, cos_ref, sin_ref, wq, wk, wv, wg, wu, wd,
         q_o, k_o, v_o, m_o, h_o,
         wq_b, wk_b, wv_b, wg_b, wu_b, wd_b, qkv_sem, mlp_sem, other_ref, rdma_sem) = refs
    else:
        (h_ref, gain_ref, cos_ref, sin_ref, wq, wk, wv, wg, wu, wd,
         q_o, k_o, v_o, m_o, h_o,
         wq_b, wk_b, wv_b, wg_b, wu_b, wd_b, qkv_sem, mlp_sem) = refs
    n_tiles = wg.shape[2] // TILE
    qkv = [pltpu.make_async_copy(src.at[layer], dst, qkv_sem.at[i])
           for i, (src, dst) in enumerate(((wq, wq_b), (wk, wk_b), (wv, wv_b)))]

    def tile_copies(j, slot):
        cols = pl.ds(pl.multiple_of(j * TILE, TILE), TILE)
        return [pltpu.make_async_copy(wg.at[layer, :, cols], wg_b.at[slot], mlp_sem.at[0, slot]),
                pltpu.make_async_copy(wu.at[layer, :, cols], wu_b.at[slot], mlp_sem.at[1, slot]),
                pltpu.make_async_copy(wd.at[layer, cols, :], wd_b.at[slot], mlp_sem.at[2, slot])]

    for copy in qkv:
        copy.start()
    for j in range(DEPTH):
        for copy in tile_copies(j, j):
            copy.start()

    rows = h_ref[...].astype(jnp.float32)
    if exchange:
        swap_partials(part_ref, other_ref, rdma_sem)
        rows = (rows + (part_ref[...] + other_ref[...])).astype(jnp.bfloat16).astype(jnp.float32)
    h_o[...] = rows.astype(jnp.bfloat16)
    centered = rows - rows.mean(axis=-1, keepdims=True)
    variance = (centered * centered).mean(axis=-1, keepdims=True)
    scaled = centered * lax.rsqrt(variance + NORM_EPS)
    normed = (scaled * gain_ref[layer:layer + 1, :].astype(jnp.float32)).astype(jnp.bfloat16)
    normed = jnp.broadcast_to(normed, (8, normed.shape[1]))

    def rotate(x):
        if not sliding:
            return x
        width = x.shape[1]
        first = lax.broadcasted_iota(jnp.int32, x.shape, 1) % HEAD_DIM < HEAD_DIM // 2
        swapped = jnp.where(first, pltpu.roll(x, width - HEAD_DIM // 2, 1), pltpu.roll(x, HEAD_DIM // 2, 1))
        return x * cos_ref[:, :width] + swapped * sin_ref[:, :width]

    def query_step(j, carry):
        cols = pl.ds(pl.multiple_of(j * TILE, TILE), TILE)
        query = jnp.dot(normed, wq_b[:, cols], preferred_element_type=jnp.float32)
        q_o[:, cols] = rotate(query)[:1].astype(jnp.bfloat16)
        return carry

    for copy in qkv:
        copy.wait()
    lax.fori_loop(0, wq_b.shape[1] // TILE, query_step, 0)
    k_o[...] = rotate(jnp.dot(normed, wk_b[...], preferred_element_type=jnp.float32))[:1].astype(jnp.bfloat16)
    v_o[...] = jnp.dot(normed, wv_b[...], preferred_element_type=jnp.float32)[:1].astype(jnp.bfloat16)

    def tile_step(j, total):
        slot = lax.rem(j, DEPTH)
        for copy in tile_copies(j, slot):
            copy.wait()
        gate = jnp.dot(normed, wg_b[slot], preferred_element_type=jnp.float32)
        up = jnp.dot(normed, wu_b[slot], preferred_element_type=jnp.float32)
        act = (jax.nn.silu(gate) * up).astype(jnp.bfloat16)
        total = total + jnp.dot(act, wd_b[slot], preferred_element_type=jnp.float32)

        @pl.when(j + DEPTH < n_tiles)
        def _():
            for copy in tile_copies(j + DEPTH, slot):
                copy.start()

        return total

    total = lax.fori_loop(0, n_tiles, tile_step, jnp.zeros((8, m_o.shape[1]), jnp.float32))
    m_o[...] = total[:1]


def front(layer, sliding, h, part, gain, cos, sin, weights):
    exchange = part is not None
    dim = h.shape[1]
    q_width, kv_width = weights[0].shape[2], weights[1].shape[2]
    out = [jax.ShapeDtypeStruct((1, q_width), jnp.bfloat16), jax.ShapeDtypeStruct((1, kv_width), jnp.bfloat16),
           jax.ShapeDtypeStruct((1, kv_width), jnp.bfloat16), jax.ShapeDtypeStruct((1, dim), jnp.float32),
           jax.ShapeDtypeStruct((1, dim), jnp.bfloat16)]
    scratch = [pltpu.VMEM((dim, q_width), jnp.bfloat16), pltpu.VMEM((dim, kv_width), jnp.bfloat16),
               pltpu.VMEM((dim, kv_width), jnp.bfloat16), pltpu.VMEM((DEPTH, dim, TILE), jnp.bfloat16),
               pltpu.VMEM((DEPTH, dim, TILE), jnp.bfloat16), pltpu.VMEM((DEPTH, TILE, dim), jnp.bfloat16),
               pltpu.SemaphoreType.DMA((3,)), pltpu.SemaphoreType.DMA((3, DEPTH))]
    args = [h]
    extra = {}
    if exchange:
        args.append(part)
        scratch += [pltpu.VMEM((1, dim), jnp.float32), pltpu.SemaphoreType.DMA((2,))]
        extra = dict(collective_id=layer, has_side_effects=True)
    args += [gain, cos, sin]
    return pl.pallas_call(
        functools.partial(front_kernel, layer, sliding, exchange),
        out_shape=out,
        in_specs=[VMEM] * len(args) + [ANY] * 6,
        out_specs=[VMEM] * 5,
        scratch_shapes=scratch,
        compiler_params=params(**extra),
        cost_estimate=pl.CostEstimate(flops=6 * 10**9, bytes_accessed=40 * 10**6, transcendentals=0),
    )(*args, *weights)


def final_kernel(h_ref, part_ref, out_ref, other_ref, sems):
    swap_partials(part_ref, other_ref, sems)
    out_ref[...] = (h_ref[...].astype(jnp.float32) + (part_ref[...] + other_ref[...])).astype(jnp.bfloat16)


def final(h, part):
    return pl.pallas_call(
        final_kernel,
        out_shape=jax.ShapeDtypeStruct(h.shape, jnp.bfloat16),
        in_specs=[VMEM, VMEM], out_specs=VMEM,
        scratch_shapes=[pltpu.VMEM(part.shape, jnp.float32), pltpu.SemaphoreType.DMA((2,))],
        compiler_params=pltpu.CompilerParams(collective_id=8, has_side_effects=True),
        name="final",
    )(h, part)


def pack_kernel(layer, n_chunks, lengths, k_ref, v_ref, recv_ref, out_ref, sem):
    _, core, chip = place()
    far_row = 2 * (1 - chip)
    start0, count0 = far_chunks(lengths[far_row], chip == 1)
    start1, _ = far_chunks(lengths[far_row + 1], chip == 1)
    per_shard = SHARD // CHUNK

    def step(j, carry):
        second = j >= count0
        row = jnp.where(second, 1, 0)
        piece = jnp.clip(jnp.where(second, start1 + j - count0, start0 + j), 0, 2 * per_shard - 1)
        own = (piece // per_shard) == core
        lanes = pl.ds(pl.multiple_of(lax.rem(piece, per_shard) * CHUNK, CHUNK), CHUNK)

        @pl.when(own & (core == 0))
        def _():
            pltpu.make_async_copy(k_ref.at[layer, far_row + row, :, :, lanes], out_ref.at[j], sem).start()

        @pl.when(own & (core == 1))
        def _():
            pltpu.make_async_copy(v_ref.at[layer, far_row + row, :, :, lanes], out_ref.at[j], sem).start()

        @pl.when(jnp.logical_not(own))
        def _():
            pltpu.make_async_copy(recv_ref.at[0, row, :, :, lanes], out_ref.at[j], sem).start()

        return carry

    lax.fori_loop(0, n_chunks, step, 0)
    pltpu.make_async_copy(out_ref, out_ref, sem).wait()


def pack(layer, n_chunks, lengths, k_t, v_t, recv):
    return pl.pallas_call(
        functools.partial(pack_kernel, layer, n_chunks),
        out_shape=jax.ShapeDtypeStruct((n_chunks, 2, HEAD_DIM, CHUNK), jnp.bfloat16),
        in_specs=[SMEM, ANY, ANY, ANY], out_specs=VMEM,
        scratch_shapes=[pltpu.SemaphoreType.DMA],
        compiler_params=params(60),
        cost_estimate=pl.CostEstimate(flops=10**9, bytes_accessed=4 * 2**20, transcendentals=0),
    )(lengths, k_t, v_t, recv)


def as_column(row, base):
    wide = jnp.broadcast_to(row[:, base:base + HEAD_DIM].astype(jnp.float32), (HEAD_DIM, HEAD_DIM))
    eye = (lax.broadcasted_iota(jnp.int32, wide.shape, 0) == lax.broadcasted_iota(jnp.int32, wide.shape, 1))
    return jnp.sum(jnp.where(eye, wide, 0.0), axis=1, keepdims=True).astype(jnp.bfloat16)


def spread_mask(group):
    shape = (group, group * HEAD_DIM)
    return lax.broadcasted_iota(jnp.int32, shape, 1) // HEAD_DIM == lax.broadcasted_iota(jnp.int32, shape, 0)


def attend(q_ref, k_buf, v_buf, last, wo_b, wo_copy, mlp_ref, part_o):
    kv_local = k_buf.shape[0]
    width = q_ref.shape[1] // kv_local
    spread = spread_mask(width // HEAD_DIM)
    fold = (lax.broadcasted_iota(jnp.int32, (HEAD_DIM, width), 1) % HEAD_DIM
            == lax.broadcasted_iota(jnp.int32, (HEAD_DIM, width), 0)).astype(jnp.bfloat16)
    part_o[...] = mlp_ref[...]

    def step(head, carry):
        lanes = pl.ds(pl.multiple_of(head * width, width), width)
        q_row = q_ref[:, lanes].astype(jnp.float32)
        q_wide = jnp.where(spread, jnp.broadcast_to(q_row, spread.shape), 0.0).astype(jnp.bfloat16)
        q = lax.dot_general(q_wide, fold, (((1,), (1,)), ((), ())), preferred_element_type=jnp.float32)
        scores = jnp.dot(q.astype(jnp.bfloat16), k_buf[head], preferred_element_type=jnp.float32) * HEAD_DIM ** -0.5
        if last is not None:
            valid = lax.broadcasted_iota(jnp.int32, scores.shape, 1) <= last
            scores = jnp.where(valid, scores, -1e30)
        top = jnp.max(scores, axis=1, keepdims=True)
        expd = jnp.exp(scores - top)
        weights = (expd / jnp.sum(expd, axis=1, keepdims=True)).astype(jnp.bfloat16)
        mixed = lax.dot_general(weights, v_buf[head], (((1,), (1,)), ((), ())), preferred_element_type=jnp.float32)
        wide = jnp.dot(mixed.astype(jnp.bfloat16), fold, preferred_element_type=jnp.float32)
        row = jnp.sum(jnp.where(spread, wide, 0.0), axis=0, keepdims=True).astype(jnp.bfloat16)

        @pl.when(head == 0)
        def _():
            wo_copy.wait()

        row = jnp.broadcast_to(row, (8, width))
        part_o[...] += jnp.dot(row, wo_b[lanes, :], preferred_element_type=jnp.float32)[:1]
        return carry

    lax.fori_loop(0, kv_local, step, 0)


def window_kernel(layer, n_far, aliased, *refs):
    (lengths, q_ref, knew_ref, vnew_ref, mlp_ref, k_ref, v_ref, near_ref, mine_ref, other_ref, wo) = refs[:11]
    refs = refs[13:] if aliased else refs[11:]
    part_o, wk_o, wv_o, k_buf, v_buf, k_far, v_far, wo_b, near_sem, far_sem, wo_sem, out_sem = refs
    row, core, chip = place()
    turn = lengths[row] - WINDOW
    start, _ = far_chunks(lengths[row], chip == 0)
    _, count0 = far_chunks(lengths[2 * chip], chip == 0)
    base = jnp.where(core == 0, 0, count0)
    first = jnp.clip(base, 0, mine_ref.shape[0] - n_far)
    shift = base - first - start
    own = pl.ds(pl.multiple_of(core * SHARD, SHARD), SHARD)
    peer = pl.ds(pl.multiple_of((1 - core) * SHARD, SHARD), SHARD)
    loads = [pltpu.make_async_copy(k_ref.at[layer, row], k_buf.at[:, :, own], near_sem.at[0]),
             pltpu.make_async_copy(v_ref.at[layer, row], v_buf.at[:, :, own], near_sem.at[1]),
             pltpu.make_async_copy(near_ref.at[0, 0], k_buf.at[:, :, peer], near_sem.at[2]),
             pltpu.make_async_copy(near_ref.at[0, 1], v_buf.at[:, :, peer], near_sem.at[3])]
    chunks = pl.ds(first, n_far)

    @pl.when(core == 0)
    def _():
        pltpu.make_async_copy(mine_ref.at[chunks], k_far, far_sem.at[0]).start()
        pltpu.make_async_copy(other_ref.at[chunks], v_far, far_sem.at[1]).start()

    @pl.when(core == 1)
    def _():
        pltpu.make_async_copy(other_ref.at[chunks], k_far, far_sem.at[0]).start()
        pltpu.make_async_copy(mine_ref.at[chunks], v_far, far_sem.at[1]).start()

    for copy in loads:
        copy.start()
    wo_copy = pltpu.make_async_copy(wo.at[layer], wo_b, wo_sem)
    wo_copy.start()
    k_new = [as_column(knew_ref[...], head * HEAD_DIM) for head in range(2)]
    v_new = [as_column(vnew_ref[...], head * HEAD_DIM) for head in range(2)]
    for copy in loads:
        copy.wait()
    pltpu.make_async_copy(mine_ref.at[chunks], k_far, far_sem.at[0]).wait()
    pltpu.make_async_copy(mine_ref.at[chunks], v_far, far_sem.at[1]).wait()

    def step(c, carry):
        lanes = pl.ds(pl.multiple_of(c * CHUNK, CHUNK), CHUNK)
        piece = jnp.clip(c + shift, 0, n_far - 1)
        slots = c * CHUNK + lax.broadcasted_iota(jnp.int32, (HEAD_DIM, CHUNK), 1)
        from_far = jnp.where(chip == 0, turn - slots, slots - turn) > 0
        is_new = slots == turn
        for head in range(2):
            for buf, far, new in ((k_buf, k_far, k_new), (v_buf, v_far, v_new)):
                near = buf[head, :, lanes]
                mixed = jnp.where(from_far, far[piece, head], near)
                buf[head, :, lanes] = jnp.where(is_new, jnp.broadcast_to(new[head], near.shape), mixed)
        return carry

    lax.fori_loop(0, WINDOW // CHUNK, step, 0)
    stores = [pltpu.make_async_copy(k_buf, wk_o.at[layer], out_sem.at[0]),
              pltpu.make_async_copy(v_buf, wv_o.at[layer], out_sem.at[1])]
    for copy in stores:
        copy.start()
    attend(q_ref, k_buf, v_buf, None, wo_b, wo_copy, mlp_ref, part_o)
    for copy in stores:
        copy.wait()


def window(layer, lengths, q, k_new, v_new, mlp, k_t, v_t, near, mine, other, wo, outs):
    n_far = min(WINDOW // CHUNK, mine.shape[0])
    aliased = outs is not None
    args = [lengths, q, k_new, v_new, mlp, k_t, v_t, near, mine, other, wo]
    specs = [SMEM] + [VMEM] * 4 + [ANY] * 6
    aliases = {}
    if aliased:
        args += list(outs)
        specs += [ANY, ANY]
        aliases = {11: 1, 12: 2}
    buf = pltpu.VMEM((2, HEAD_DIM, WINDOW), jnp.bfloat16)
    far = pltpu.VMEM((n_far, 2, HEAD_DIM, CHUNK), jnp.bfloat16)
    out = jax.ShapeDtypeStruct((3, 2, HEAD_DIM, WINDOW), jnp.bfloat16)
    return pl.pallas_call(
        functools.partial(window_kernel, layer, n_far, aliased),
        out_shape=[jax.ShapeDtypeStruct(mlp.shape, jnp.float32), out, out],
        in_specs=specs, out_specs=[VMEM, ANY, ANY],
        scratch_shapes=[buf, buf, far, far, pltpu.VMEM(wo.shape[1:], jnp.bfloat16),
                        pltpu.SemaphoreType.DMA((4,)), pltpu.SemaphoreType.DMA((2,)),
                        pltpu.SemaphoreType.DMA, pltpu.SemaphoreType.DMA((2,))],
        input_output_aliases=aliases,
        compiler_params=params(),
        cost_estimate=pl.CostEstimate(flops=3 * 10**9, bytes_accessed=12 * 2**20, transcendentals=0),
    )(*args)


def global_kernel(layer, slot, lengths, q_ref, knew_ref, vnew_ref, mlp_ref, k_ref, v_ref, p1_ref, p2_ref, p3_ref, wo,
                  part_o, gk_o, gv_o, k_buf, v_buf, wo_b, load_sem, wo_sem, out_sem):
    row, core, chip = place()
    last = lengths[row]
    across = row + 2 - 4 * chip
    sources = (row + 1 - 2 * core, across, across + 1 - 2 * core)
    loads = [pltpu.make_async_copy(k_ref.at[layer, row], k_buf.at[:, :, pl.ds(pl.multiple_of(row * SHARD, SHARD), SHARD)], load_sem.at[0]),
             pltpu.make_async_copy(v_ref.at[layer, row], v_buf.at[:, :, pl.ds(pl.multiple_of(row * SHARD, SHARD), SHARD)], load_sem.at[1])]
    for i, ref in enumerate((p1_ref.at[slot], p2_ref, p3_ref)):
        lanes = pl.ds(pl.multiple_of(sources[i] * SHARD, SHARD), SHARD)
        loads += [pltpu.make_async_copy(ref.at[0], k_buf.at[:, :, lanes], load_sem.at[2 + 2 * i]),
                  pltpu.make_async_copy(ref.at[1], v_buf.at[:, :, lanes], load_sem.at[3 + 2 * i])]
    for copy in loads:
        copy.start()
    wo_copy = pltpu.make_async_copy(wo.at[layer], wo_b, wo_sem)
    wo_copy.start()
    k_new = [as_column(knew_ref[...], head * HEAD_DIM) for head in range(2)]
    v_new = [as_column(vnew_ref[...], head * HEAD_DIM) for head in range(2)]
    for copy in loads:
        copy.wait()

    def step(c, carry):
        lanes = pl.ds(pl.multiple_of(c * CHUNK, CHUNK), CHUNK)
        slots = c * CHUNK + lax.broadcasted_iota(jnp.int32, (HEAD_DIM, CHUNK), 1)
        for head in range(2):
            for buf, new in ((k_buf, k_new), (v_buf, v_new)):
                near = buf[head, :, lanes]
                kept = jnp.where(slots < last, near, jnp.zeros_like(near))
                buf[head, :, lanes] = jnp.where(slots == last, jnp.broadcast_to(new[head], near.shape), kept)
        return carry

    lax.fori_loop(WINDOW // CHUNK, 2 * WINDOW // CHUNK, step, 0)
    stores = [pltpu.make_async_copy(k_buf, gk_o, out_sem.at[0]), pltpu.make_async_copy(v_buf, gv_o, out_sem.at[1])]
    for copy in stores:
        copy.start()
    attend(q_ref, k_buf, v_buf, last, wo_b, wo_copy, mlp_ref, part_o)
    for copy in stores:
        copy.wait()


def global_layer(layer, slot, lengths, q, k_new, v_new, mlp, k_t, v_t, pieces, wo):
    buf = pltpu.VMEM((2, HEAD_DIM, 4 * SHARD), jnp.bfloat16)
    out = jax.ShapeDtypeStruct((2, HEAD_DIM, 4 * SHARD), jnp.bfloat16)
    return pl.pallas_call(
        functools.partial(global_kernel, layer, slot),
        out_shape=[jax.ShapeDtypeStruct(mlp.shape, jnp.float32), out, out],
        in_specs=[SMEM] + [VMEM] * 4 + [ANY] * 6, out_specs=[VMEM, ANY, ANY],
        scratch_shapes=[buf, buf, pltpu.VMEM(wo.shape[1:], jnp.bfloat16), pltpu.SemaphoreType.DMA((8,)),
                        pltpu.SemaphoreType.DMA, pltpu.SemaphoreType.DMA((2,))],
        compiler_params=params(),
        cost_estimate=pl.CostEstimate(flops=3 * 10**9, bytes_accessed=14 * 2**20, transcendentals=0),
        name="global",
    )(lengths, q, k_new, v_new, mlp, k_t, v_t, *pieces, wo)


def run_layers(n_chunks, k_t, v_t, lengths, residual, ln_gain, cos, sin, weights, w_out):
    last = w_out.shape[0] - 1
    streams = []
    for layer in range(last):
        traded = ((layer, True),) if layer < last - 1 else ((layer, True), (last, False))
        far, near = swap(traded, k_t, v_t, 5 + layer)
        packed = pack(layer, n_chunks, lengths, k_t, v_t, far)
        mine = lax.ppermute(packed, "sp", CROSS)
        other = lax.ppermute(mine, "sp", PARTNER)
        streams.append((near, mine, other))
    same, crossed = payload(last, k_t, v_t)
    same = lax.ppermute(same, "sp", CROSS)
    crossed = lax.ppermute(crossed, "sp", CROSS_SWAP)

    part, outs = None, None
    for layer in range(last + 1):
        q, k_new, v_new, mlp, residual = front(layer, layer < last, residual, part, ln_gain, cos, sin, weights)
        if layer < last:
            part, *outs = window(layer, lengths, q, k_new, v_new, mlp, k_t, v_t, *streams[layer], w_out, outs)
    return (q, k_new, v_new, mlp, residual), (near, same, crossed), outs


def decode(k_t, v_t, lengths, hidden, ln_gain, w_query, w_key, w_value, w_out, w_gate, w_up, w_down):
    my_length = lengths[lax.axis_index("sp")]
    half_dim = HEAD_DIM // 2
    inv_freq = 1.0 / (ROPE_BASE ** (jnp.arange(half_dim, dtype=jnp.float32) * 2.0 / HEAD_DIM))
    angles = my_length.astype(jnp.float32) * inv_freq
    cosine, sine = jnp.cos(angles), jnp.sin(angles)
    cos = jnp.tile(jnp.concatenate([cosine, cosine]), TILE // HEAD_DIM)[None]
    sin = jnp.tile(jnp.concatenate([-sine, sine]), TILE // HEAD_DIM)[None]
    weights = (w_query, w_key, w_value, w_gate, w_up, w_down)

    counts = far_chunks(lengths, jnp.arange(4) < 2)[1]
    needed = jnp.maximum(counts[0] + counts[1], counts[2] + counts[3])
    choice = sum((needed > size).astype(jnp.int32) for size in SIZES[:-1])

    def branch(i):
        def run(args):
            return run_layers(SIZES[i], *args)

        return run

    args = (k_t, v_t, lengths, hidden, ln_gain, cos, sin, weights, w_out)
    state, pieces, outs = lax.switch(choice, [branch(i) for i in range(len(SIZES))], args)
    *inputs, residual = state
    part, global_k, global_v = global_layer(w_out.shape[0] - 1, 1, lengths, *inputs, k_t, v_t, pieces, w_out)
    return final(residual, part), outs[0], outs[1], global_k, global_v


SIZES = (24, 32, 40, 48, 56, 64)


def solution(mesh):
    cache_spec = P(None, "dp", "tp", "sp", None)
    row_spec = P(("dp", "sp"), None)
    col_spec = P(None, None, "tp")
    inner_spec = P(None, "tp", None)
    window_spec = P(None, ("dp", "sp"), "tp", None, None)
    global_spec = P(("dp", "sp"), "tp", None, None)
    in_specs = (cache_spec, cache_spec, P("dp"), row_spec, P(None, None), col_spec, col_spec, col_spec, inner_spec, col_spec, col_spec, inner_spec)
    out_specs = (row_spec, window_spec, window_spec, global_spec, global_spec)

    def device_step(k_cache, v_cache, *rest):
        k_t, v_t = jnp.swapaxes(k_cache, 3, 4), jnp.swapaxes(v_cache, 3, 4)
        h, wk, wv, gk, gv = decode(k_t, v_t, *rest)
        turn = lambda x: jnp.swapaxes(x, -1, -2)
        return h, turn(wk)[:, None], turn(wv)[:, None], turn(gk)[None], turn(gv)[None]

    return jax.shard_map(device_step, mesh=mesh, in_specs=in_specs, out_specs=out_specs, check_vma=False)
```

```python
import functools

import jax
import jax.numpy as jnp
from jax import lax
from jax.experimental import pallas as pl
from jax.experimental.pallas import tpu as pltpu
from jax.sharding import PartitionSpec as P


WINDOW = 4096
ROPE_BASE = 50000
NORM_EPS = 1e-5
SHARD = 2048
CHUNK = 128
HEAD_DIM = 64
DEPTH = 4
TILE = 256
CROSS = [(0, 2), (2, 0), (1, 3), (3, 1)]
CROSS_SWAP = [(0, 3), (3, 0), (1, 2), (2, 1)]
PARTNER = [(0, 1), (1, 0), (2, 3), (3, 2)]


VMEM = pl.BlockSpec(memory_space=pltpu.VMEM)
SMEM = pl.BlockSpec(memory_space=pltpu.SMEM)
ANY = pl.BlockSpec(memory_space=pltpu.HBM)


def params(mib=40, **extra):
    return pltpu.CompilerParams(vmem_limit_bytes=mib * 2**20, **extra)


def place():
    sp = lax.axis_index("sp")
    return sp, lax.rem(sp, 2), sp // 2


def far_chunks(length, on_first_chip):
    turn = length - WINDOW
    start = jnp.where(on_first_chip, 0, (turn + 1) // CHUNK)
    count = jnp.where(on_first_chip, (turn + CHUNK - 1) // CHUNK, WINDOW // CHUNK - (turn + 1) // CHUNK)
    return start, count


def swap_kernel(layers, k_ref, v_ref, far_o, near_o, send_sem, recv_sem):
    sp, core, chip = place()
    peer = sp + 1 - 2 * core
    barrier = pltpu.get_barrier_semaphore()
    pl.semaphore_signal(barrier, inc=1, device_id={"sp": peer}, device_id_type=pl.DeviceIdType.MESH)
    pl.semaphore_wait(barrier, 1)
    far_rows = pl.ds(2 * (1 - chip), 2)

    def send(src, dst, i):
        return pltpu.make_async_remote_copy(
            src_ref=src, dst_ref=dst, send_sem=send_sem.at[i], recv_sem=recv_sem.at[i],
            device_id={"sp": peer}, device_id_type=pl.DeviceIdType.MESH)

    copies = []
    for i, (layer, sliding) in enumerate(layers):
        if sliding:
            @pl.when(core == 0)
            def _(layer=layer, i=i):
                send(v_ref.at[layer, far_rows], far_o.at[i], 3 * i).start()

            @pl.when(core == 1)
            def _(layer=layer, i=i):
                send(k_ref.at[layer, far_rows], far_o.at[i], 3 * i).start()

            copies.append(send(k_ref.at[layer, far_rows], far_o.at[i], 3 * i))
        pair = [send(k_ref.at[layer, peer], near_o.at[i, 0], 3 * i + 1),
                send(v_ref.at[layer, peer], near_o.at[i, 1], 3 * i + 2)]
        for copy in pair:
            copy.start()
        copies += pair
    for copy in copies:
        copy.wait()


def swap(layers, k_t, v_t, collective_id):
    n = len(layers)
    block = jax.ShapeDtypeStruct((n, 2, 2, HEAD_DIM, SHARD), jnp.bfloat16)
    return pl.pallas_call(
        functools.partial(swap_kernel, layers),
        out_shape=[block, block],
        in_specs=[ANY, ANY], out_specs=[ANY, ANY],
        scratch_shapes=[pltpu.SemaphoreType.DMA((3 * n,)), pltpu.SemaphoreType.DMA((3 * n,))],
        compiler_params=params(60, collective_id=collective_id, has_side_effects=True),
        cost_estimate=pl.CostEstimate(flops=10**9, bytes_accessed=4 * 2**20, transcendentals=0),
        name="swap",
    )(k_t, v_t)


def payload_kernel(layer, picks, k_ref, v_ref, *refs):
    sp, core, chip = place()
    rows = {"same": sp + 2 - 4 * chip, "cross": 2 * (1 - chip) + 1 - core}
    sems = refs[-1]
    copies = [pltpu.make_async_copy((k_ref, v_ref)[which].at[layer, rows[kind]], out, sems.at[i])
              for i, ((kind, which), out) in enumerate(zip(picks, refs))]
    for copy in copies:
        copy.start()
    for copy in copies:
        copy.wait()


def payload(layer, picks, k_t, v_t):
    block = jax.ShapeDtypeStruct((2, HEAD_DIM, SHARD), jnp.bfloat16)
    return pl.pallas_call(
        functools.partial(payload_kernel, layer, picks),
        out_shape=[block] * len(picks),
        in_specs=[ANY, ANY], out_specs=[VMEM] * len(picks),
        scratch_shapes=[pltpu.SemaphoreType.DMA((len(picks),))],
        compiler_params=params(60),
        cost_estimate=pl.CostEstimate(flops=10**9, bytes_accessed=len(picks) * 2**20, transcendentals=0),
        name="payload",
    )(k_t, v_t)


def swap_partials(part_ref, other_ref, sems):
    tp_peer = 1 - lax.axis_index("tp")
    barrier = pltpu.get_barrier_semaphore()
    pl.semaphore_signal(barrier, inc=1, device_id={"tp": tp_peer}, device_id_type=pl.DeviceIdType.MESH)
    pl.semaphore_wait(barrier, 1)
    copy = pltpu.make_async_remote_copy(
        src_ref=part_ref, dst_ref=other_ref, send_sem=sems.at[0], recv_sem=sems.at[1],
        device_id={"tp": tp_peer}, device_id_type=pl.DeviceIdType.MESH)
    copy.start()
    copy.wait()


def front_kernel(layer, sliding, exchange, *refs):
    if exchange:
        (h_ref, part_ref, gain_ref, cos_ref, sin_ref, wq, wk, wv, wg, wu, wd,
         q_o, k_o, v_o, m_o, h_o,
         wq_b, wk_b, wv_b, wg_b, wu_b, wd_b, qkv_sem, mlp_sem, other_ref, rdma_sem) = refs
    else:
        (h_ref, gain_ref, cos_ref, sin_ref, wq, wk, wv, wg, wu, wd,
         q_o, k_o, v_o, m_o, h_o,
         wq_b, wk_b, wv_b, wg_b, wu_b, wd_b, qkv_sem, mlp_sem) = refs
    n_tiles = wg.shape[2] // TILE
    qkv = [pltpu.make_async_copy(src.at[layer], dst, qkv_sem.at[i])
           for i, (src, dst) in enumerate(((wq, wq_b), (wk, wk_b), (wv, wv_b)))]

    def tile_copies(j, slot):
        cols = pl.ds(pl.multiple_of(j * TILE, TILE), TILE)
        return [pltpu.make_async_copy(wg.at[layer, :, cols], wg_b.at[slot], mlp_sem.at[0, slot]),
                pltpu.make_async_copy(wu.at[layer, :, cols], wu_b.at[slot], mlp_sem.at[1, slot]),
                pltpu.make_async_copy(wd.at[layer, cols, :], wd_b.at[slot], mlp_sem.at[2, slot])]

    for copy in qkv:
        copy.start()
    for j in range(DEPTH):
        for copy in tile_copies(j, j):
            copy.start()

    rows = h_ref[...].astype(jnp.float32)
    if exchange:
        swap_partials(part_ref, other_ref, rdma_sem)
        rows = (rows + (part_ref[...] + other_ref[...])).astype(jnp.bfloat16).astype(jnp.float32)
    h_o[...] = rows.astype(jnp.bfloat16)
    centered = rows - rows.mean(axis=-1, keepdims=True)
    variance = (centered * centered).mean(axis=-1, keepdims=True)
    scaled = centered * lax.rsqrt(variance + NORM_EPS)
    normed = (scaled * gain_ref[layer:layer + 1, :].astype(jnp.float32)).astype(jnp.bfloat16)
    normed = jnp.broadcast_to(normed, (8, normed.shape[1]))

    def rotate(x):
        if not sliding:
            return x
        width = x.shape[1]
        first = lax.broadcasted_iota(jnp.int32, x.shape, 1) % HEAD_DIM < HEAD_DIM // 2
        swapped = jnp.where(first, pltpu.roll(x, width - HEAD_DIM // 2, 1), pltpu.roll(x, HEAD_DIM // 2, 1))
        return x * cos_ref[:, :width] + swapped * sin_ref[:, :width]

    def query_step(j, carry):
        cols = pl.ds(pl.multiple_of(j * TILE, TILE), TILE)
        query = jnp.dot(normed, wq_b[:, cols], preferred_element_type=jnp.float32)
        q_o[:, cols] = rotate(query)[:1].astype(jnp.bfloat16)
        return carry

    for copy in qkv:
        copy.wait()
    lax.fori_loop(0, wq_b.shape[1] // TILE, query_step, 0)
    k_o[...] = rotate(jnp.dot(normed, wk_b[...], preferred_element_type=jnp.float32))[:1].astype(jnp.bfloat16)
    v_o[...] = jnp.dot(normed, wv_b[...], preferred_element_type=jnp.float32)[:1].astype(jnp.bfloat16)

    def tile_step(j, total):
        slot = lax.rem(j, DEPTH)
        for copy in tile_copies(j, slot):
            copy.wait()
        gate = jnp.dot(normed, wg_b[slot], preferred_element_type=jnp.float32)
        up = jnp.dot(normed, wu_b[slot], preferred_element_type=jnp.float32)
        act = (jax.nn.silu(gate) * up).astype(jnp.bfloat16)
        total = total + jnp.dot(act, wd_b[slot], preferred_element_type=jnp.float32)

        @pl.when(j + DEPTH < n_tiles)
        def _():
            for copy in tile_copies(j + DEPTH, slot):
                copy.start()

        return total

    total = lax.fori_loop(0, n_tiles, tile_step, jnp.zeros((8, m_o.shape[1]), jnp.float32))
    m_o[...] = total[:1]


def front(layer, sliding, h, part, gain, cos, sin, weights):
    exchange = part is not None
    dim = h.shape[1]
    q_width, kv_width = weights[0].shape[2], weights[1].shape[2]
    out = [jax.ShapeDtypeStruct((1, q_width), jnp.bfloat16), jax.ShapeDtypeStruct((1, kv_width), jnp.bfloat16),
           jax.ShapeDtypeStruct((1, kv_width), jnp.bfloat16), jax.ShapeDtypeStruct((1, dim), jnp.float32),
           jax.ShapeDtypeStruct((1, dim), jnp.bfloat16)]
    scratch = [pltpu.VMEM((dim, q_width), jnp.bfloat16), pltpu.VMEM((dim, kv_width), jnp.bfloat16),
               pltpu.VMEM((dim, kv_width), jnp.bfloat16), pltpu.VMEM((DEPTH, dim, TILE), jnp.bfloat16),
               pltpu.VMEM((DEPTH, dim, TILE), jnp.bfloat16), pltpu.VMEM((DEPTH, TILE, dim), jnp.bfloat16),
               pltpu.SemaphoreType.DMA((3,)), pltpu.SemaphoreType.DMA((3, DEPTH))]
    args = [h]
    extra = {}
    if exchange:
        args.append(part)
        scratch += [pltpu.VMEM((1, dim), jnp.float32), pltpu.SemaphoreType.DMA((2,))]
        extra = dict(collective_id=layer, has_side_effects=True)
    args += [gain, cos, sin]
    return pl.pallas_call(
        functools.partial(front_kernel, layer, sliding, exchange),
        out_shape=out,
        in_specs=[VMEM] * len(args) + [ANY] * 6,
        out_specs=[VMEM] * 5,
        scratch_shapes=scratch,
        compiler_params=params(**extra),
        cost_estimate=pl.CostEstimate(flops=6 * 10**9, bytes_accessed=40 * 10**6, transcendentals=0),
    )(*args, *weights)


def final_kernel(h_ref, part_ref, out_ref, other_ref, sems):
    swap_partials(part_ref, other_ref, sems)
    out_ref[...] = (h_ref[...].astype(jnp.float32) + (part_ref[...] + other_ref[...])).astype(jnp.bfloat16)


def final(h, part):
    return pl.pallas_call(
        final_kernel,
        out_shape=jax.ShapeDtypeStruct(h.shape, jnp.bfloat16),
        in_specs=[VMEM, VMEM], out_specs=VMEM,
        scratch_shapes=[pltpu.VMEM(part.shape, jnp.float32), pltpu.SemaphoreType.DMA((2,))],
        compiler_params=pltpu.CompilerParams(collective_id=8, has_side_effects=True),
        name="final",
    )(h, part)


def pack_kernel(layer, n_chunks, lengths, k_ref, v_ref, recv_ref, out_ref, sem):
    _, core, chip = place()
    far_row = 2 * (1 - chip)
    start0, count0 = far_chunks(lengths[far_row], chip == 1)
    start1, _ = far_chunks(lengths[far_row + 1], chip == 1)
    per_shard = SHARD // CHUNK

    def step(j, carry):
        second = j >= count0
        row = jnp.where(second, 1, 0)
        piece = jnp.clip(jnp.where(second, start1 + j - count0, start0 + j), 0, 2 * per_shard - 1)
        own = (piece // per_shard) == core
        lanes = pl.ds(pl.multiple_of(lax.rem(piece, per_shard) * CHUNK, CHUNK), CHUNK)

        @pl.when(own & (core == 0))
        def _():
            pltpu.make_async_copy(k_ref.at[layer, far_row + row, :, :, lanes], out_ref.at[j], sem).start()

        @pl.when(own & (core == 1))
        def _():
            pltpu.make_async_copy(v_ref.at[layer, far_row + row, :, :, lanes], out_ref.at[j], sem).start()

        @pl.when(jnp.logical_not(own))
        def _():
            pltpu.make_async_copy(recv_ref.at[0, row, :, :, lanes], out_ref.at[j], sem).start()

        return carry

    lax.fori_loop(0, n_chunks, step, 0)
    pltpu.make_async_copy(out_ref, out_ref, sem).wait()


def pack(layer, n_chunks, lengths, k_t, v_t, recv):
    return pl.pallas_call(
        functools.partial(pack_kernel, layer, n_chunks),
        out_shape=jax.ShapeDtypeStruct((n_chunks, 2, HEAD_DIM, CHUNK), jnp.bfloat16),
        in_specs=[SMEM, ANY, ANY, ANY], out_specs=VMEM,
        scratch_shapes=[pltpu.SemaphoreType.DMA],
        compiler_params=params(60),
        cost_estimate=pl.CostEstimate(flops=10**9, bytes_accessed=4 * 2**20, transcendentals=0),
    )(lengths, k_t, v_t, recv)


def as_column(row, base):
    wide = jnp.broadcast_to(row[:, base:base + HEAD_DIM].astype(jnp.float32), (HEAD_DIM, HEAD_DIM))
    eye = (lax.broadcasted_iota(jnp.int32, wide.shape, 0) == lax.broadcasted_iota(jnp.int32, wide.shape, 1))
    return jnp.sum(jnp.where(eye, wide, 0.0), axis=1, keepdims=True).astype(jnp.bfloat16)


def spread_mask(group):
    shape = (group, group * HEAD_DIM)
    return lax.broadcasted_iota(jnp.int32, shape, 1) // HEAD_DIM == lax.broadcasted_iota(jnp.int32, shape, 0)


def attend(q_ref, k_buf, v_buf, last, wo_b, wo_copy, mlp_ref, part_o):
    kv_local = k_buf.shape[0]
    width = q_ref.shape[1] // kv_local
    spread = spread_mask(width // HEAD_DIM)
    fold = (lax.broadcasted_iota(jnp.int32, (HEAD_DIM, width), 1) % HEAD_DIM
            == lax.broadcasted_iota(jnp.int32, (HEAD_DIM, width), 0)).astype(jnp.bfloat16)
    part_o[...] = mlp_ref[...]

    def step(head, carry):
        lanes = pl.ds(pl.multiple_of(head * width, width), width)
        q_row = q_ref[:, lanes].astype(jnp.float32)
        q_wide = jnp.where(spread, jnp.broadcast_to(q_row, spread.shape), 0.0).astype(jnp.bfloat16)
        q = lax.dot_general(q_wide, fold, (((1,), (1,)), ((), ())), preferred_element_type=jnp.float32)
        scores = jnp.dot(q.astype(jnp.bfloat16), k_buf[head], preferred_element_type=jnp.float32) * HEAD_DIM ** -0.5
        if last is not None:
            valid = lax.broadcasted_iota(jnp.int32, scores.shape, 1) <= last
            scores = jnp.where(valid, scores, -1e30)
        top = jnp.max(scores, axis=1, keepdims=True)
        expd = jnp.exp(scores - top)
        weights = (expd / jnp.sum(expd, axis=1, keepdims=True)).astype(jnp.bfloat16)
        mixed = lax.dot_general(weights, v_buf[head], (((1,), (1,)), ((), ())), preferred_element_type=jnp.float32)
        wide = jnp.dot(mixed.astype(jnp.bfloat16), fold, preferred_element_type=jnp.float32)
        row = jnp.sum(jnp.where(spread, wide, 0.0), axis=0, keepdims=True).astype(jnp.bfloat16)

        @pl.when(head == 0)
        def _():
            wo_copy.wait()

        row = jnp.broadcast_to(row, (8, width))
        part_o[...] += jnp.dot(row, wo_b[lanes, :], preferred_element_type=jnp.float32)[:1]
        return carry

    lax.fori_loop(0, kv_local, step, 0)


def window_kernel(layer, n_far, aliased, *refs):
    (lengths, q_ref, knew_ref, vnew_ref, mlp_ref, k_ref, v_ref, near_ref, mine_ref, other_ref, wo) = refs[:11]
    refs = refs[13:] if aliased else refs[11:]
    part_o, wk_o, wv_o, k_buf, v_buf, k_far, v_far, wo_b, near_sem, far_sem, wo_sem, out_sem = refs
    row, core, chip = place()
    turn = lengths[row] - WINDOW
    start, _ = far_chunks(lengths[row], chip == 0)
    _, count0 = far_chunks(lengths[2 * chip], chip == 0)
    base = jnp.where(core == 0, 0, count0)
    first = jnp.clip(base, 0, mine_ref.shape[0] - n_far)
    shift = base - first - start
    own = pl.ds(pl.multiple_of(core * SHARD, SHARD), SHARD)
    peer = pl.ds(pl.multiple_of((1 - core) * SHARD, SHARD), SHARD)
    loads = [pltpu.make_async_copy(k_ref.at[layer, row], k_buf.at[:, :, own], near_sem.at[0]),
             pltpu.make_async_copy(v_ref.at[layer, row], v_buf.at[:, :, own], near_sem.at[1]),
             pltpu.make_async_copy(near_ref.at[0, 0], k_buf.at[:, :, peer], near_sem.at[2]),
             pltpu.make_async_copy(near_ref.at[0, 1], v_buf.at[:, :, peer], near_sem.at[3])]
    chunks = pl.ds(first, n_far)

    @pl.when(core == 0)
    def _():
        pltpu.make_async_copy(mine_ref.at[chunks], k_far, far_sem.at[0]).start()
        pltpu.make_async_copy(other_ref.at[chunks], v_far, far_sem.at[1]).start()

    @pl.when(core == 1)
    def _():
        pltpu.make_async_copy(other_ref.at[chunks], k_far, far_sem.at[0]).start()
        pltpu.make_async_copy(mine_ref.at[chunks], v_far, far_sem.at[1]).start()

    for copy in loads:
        copy.start()
    wo_copy = pltpu.make_async_copy(wo.at[layer], wo_b, wo_sem)
    wo_copy.start()
    k_new = [as_column(knew_ref[...], head * HEAD_DIM) for head in range(2)]
    v_new = [as_column(vnew_ref[...], head * HEAD_DIM) for head in range(2)]
    for copy in loads:
        copy.wait()
    pltpu.make_async_copy(mine_ref.at[chunks], k_far, far_sem.at[0]).wait()
    pltpu.make_async_copy(mine_ref.at[chunks], v_far, far_sem.at[1]).wait()

    def step(c, carry):
        lanes = pl.ds(pl.multiple_of(c * CHUNK, CHUNK), CHUNK)
        piece = jnp.clip(c + shift, 0, n_far - 1)
        slots = c * CHUNK + lax.broadcasted_iota(jnp.int32, (HEAD_DIM, CHUNK), 1)
        from_far = jnp.where(chip == 0, turn - slots, slots - turn) > 0
        is_new = slots == turn
        for head in range(2):
            for buf, far, new in ((k_buf, k_far, k_new), (v_buf, v_far, v_new)):
                near = buf[head, :, lanes]
                mixed = jnp.where(from_far, far[piece, head], near)
                buf[head, :, lanes] = jnp.where(is_new, jnp.broadcast_to(new[head], near.shape), mixed)
        return carry

    lax.fori_loop(0, WINDOW // CHUNK, step, 0)
    stores = [pltpu.make_async_copy(k_buf, wk_o.at[layer], out_sem.at[0]),
              pltpu.make_async_copy(v_buf, wv_o.at[layer], out_sem.at[1])]
    for copy in stores:
        copy.start()
    attend(q_ref, k_buf, v_buf, None, wo_b, wo_copy, mlp_ref, part_o)
    for copy in stores:
        copy.wait()


def window(layer, lengths, q, k_new, v_new, mlp, k_t, v_t, near, mine, other, wo, outs):
    n_far = min(WINDOW // CHUNK, mine.shape[0])
    aliased = outs is not None
    args = [lengths, q, k_new, v_new, mlp, k_t, v_t, near, mine, other, wo]
    specs = [SMEM] + [VMEM] * 4 + [ANY] * 6
    aliases = {}
    if aliased:
        args += list(outs)
        specs += [ANY, ANY]
        aliases = {11: 1, 12: 2}
    buf = pltpu.VMEM((2, HEAD_DIM, WINDOW), jnp.bfloat16)
    far = pltpu.VMEM((n_far, 2, HEAD_DIM, CHUNK), jnp.bfloat16)
    out = jax.ShapeDtypeStruct((3, 2, HEAD_DIM, WINDOW), jnp.bfloat16)
    return pl.pallas_call(
        functools.partial(window_kernel, layer, n_far, aliased),
        out_shape=[jax.ShapeDtypeStruct(mlp.shape, jnp.float32), out, out],
        in_specs=specs, out_specs=[VMEM, ANY, ANY],
        scratch_shapes=[buf, buf, far, far, pltpu.VMEM(wo.shape[1:], jnp.bfloat16),
                        pltpu.SemaphoreType.DMA((4,)), pltpu.SemaphoreType.DMA((2,)),
                        pltpu.SemaphoreType.DMA, pltpu.SemaphoreType.DMA((2,))],
        input_output_aliases=aliases,
        compiler_params=params(),
        cost_estimate=pl.CostEstimate(flops=3 * 10**9, bytes_accessed=12 * 2**20, transcendentals=0),
    )(*args)


def global_kernel(layer, lengths, q_ref, knew_ref, vnew_ref, mlp_ref, k_ref, v_ref, near_ref, *refs):
    pieces, (wo, part_o, gk_o, gv_o, k_buf, v_buf, wo_b, load_sem, wo_sem, out_sem) = refs[:4], refs[4:]
    row, core, chip = place()
    last = lengths[row]
    across = row + 2 - 4 * chip
    sources = (row + 1 - 2 * core, across, across + 1 - 2 * core)
    lanes = [pl.ds(pl.multiple_of(shard * SHARD, SHARD), SHARD) for shard in (row,) + sources]
    parts = [k_ref.at[layer, row], v_ref.at[layer, row], near_ref.at[1, 0], near_ref.at[1, 1], *pieces]
    loads = [pltpu.make_async_copy(ref, (k_buf, v_buf)[i % 2].at[:, :, lanes[i // 2]], load_sem.at[i])
             for i, ref in enumerate(parts)]
    for copy in loads:
        copy.start()
    wo_copy = pltpu.make_async_copy(wo.at[layer], wo_b, wo_sem)
    wo_copy.start()
    k_new = [as_column(knew_ref[...], head * HEAD_DIM) for head in range(2)]
    v_new = [as_column(vnew_ref[...], head * HEAD_DIM) for head in range(2)]
    for copy in loads:
        copy.wait()

    def step(c, carry):
        lanes = pl.ds(pl.multiple_of(c * CHUNK, CHUNK), CHUNK)
        slots = c * CHUNK + lax.broadcasted_iota(jnp.int32, (HEAD_DIM, CHUNK), 1)
        for head in range(2):
            for buf, new in ((k_buf, k_new), (v_buf, v_new)):
                near = buf[head, :, lanes]
                kept = jnp.where(slots < last, near, jnp.zeros_like(near))
                buf[head, :, lanes] = jnp.where(slots == last, jnp.broadcast_to(new[head], near.shape), kept)
        return carry

    lax.fori_loop(last // CHUNK, 2 * WINDOW // CHUNK, step, 0)
    stores = [pltpu.make_async_copy(k_buf, gk_o, out_sem.at[0]), pltpu.make_async_copy(v_buf, gv_o, out_sem.at[1])]
    for copy in stores:
        copy.start()
    attend(q_ref, k_buf, v_buf, last, wo_b, wo_copy, mlp_ref, part_o)
    for copy in stores:
        copy.wait()


def global_layer(layer, lengths, q, k_new, v_new, mlp, k_t, v_t, pieces, wo):
    buf = pltpu.VMEM((2, HEAD_DIM, 4 * SHARD), jnp.bfloat16)
    out = jax.ShapeDtypeStruct((2, HEAD_DIM, 4 * SHARD), jnp.bfloat16)
    return pl.pallas_call(
        functools.partial(global_kernel, layer),
        out_shape=[jax.ShapeDtypeStruct(mlp.shape, jnp.float32), out, out],
        in_specs=[SMEM] + [VMEM] * 4 + [ANY] * 8, out_specs=[VMEM, ANY, ANY],
        scratch_shapes=[buf, buf, pltpu.VMEM(wo.shape[1:], jnp.bfloat16), pltpu.SemaphoreType.DMA((8,)),
                        pltpu.SemaphoreType.DMA, pltpu.SemaphoreType.DMA((2,))],
        compiler_params=params(),
        cost_estimate=pl.CostEstimate(flops=3 * 10**9, bytes_accessed=14 * 2**20, transcendentals=0),
        name="global",
    )(lengths, q, k_new, v_new, mlp, k_t, v_t, *pieces, wo)


def run_layers(n_chunks, k_t, v_t, lengths, residual, ln_gain, weights, w_out):
    last = w_out.shape[0] - 1
    (same_k,) = payload(last, (("same", 0),), k_t, v_t)
    same_k = lax.ppermute(same_k, "sp", CROSS)
    streams = []
    for layer in range(last):
        traded = ((layer, True),) if layer < last - 1 else ((layer, True), (last, False))
        far, near = swap(traded, k_t, v_t, 5 + layer)
        packed = pack(layer, n_chunks, lengths, k_t, v_t, far)
        mine = lax.ppermute(packed, "sp", CROSS)
        other = lax.ppermute(mine, "sp", PARTNER)
        streams.append((near, mine, other))
    same_v, cross_k, cross_v = payload(last, (("same", 1), ("cross", 0), ("cross", 1)), k_t, v_t)
    same_v = lax.ppermute(same_v, "sp", CROSS)
    cross_k = lax.ppermute(cross_k, "sp", CROSS_SWAP)
    cross_v = lax.ppermute(cross_v, "sp", CROSS_SWAP)

    my_length = lengths[lax.axis_index("sp")]
    half_dim = HEAD_DIM // 2
    inv_freq = 1.0 / (ROPE_BASE ** (jnp.arange(half_dim, dtype=jnp.float32) * 2.0 / HEAD_DIM))
    angles = my_length.astype(jnp.float32) * inv_freq
    cosine, sine = jnp.cos(angles), jnp.sin(angles)
    cos = jnp.tile(jnp.concatenate([cosine, cosine]), TILE // HEAD_DIM)[None]
    sin = jnp.tile(jnp.concatenate([-sine, sine]), TILE // HEAD_DIM)[None]

    part, outs = None, None
    for layer in range(last + 1):
        q, k_new, v_new, mlp, residual = front(layer, layer < last, residual, part, ln_gain, cos, sin, weights)
        if layer < last:
            part, *outs = window(layer, lengths, q, k_new, v_new, mlp, k_t, v_t, *streams[layer], w_out, outs)
    return (q, k_new, v_new, mlp, residual), (near, same_k, same_v, cross_k, cross_v), outs


def decode(k_t, v_t, lengths, hidden, ln_gain, w_query, w_key, w_value, w_out, w_gate, w_up, w_down):
    weights = (w_query, w_key, w_value, w_gate, w_up, w_down)

    counts = far_chunks(lengths, jnp.arange(4) < 2)[1]
    needed = jnp.maximum(counts[0] + counts[1], counts[2] + counts[3])
    choice = sum((needed > size).astype(jnp.int32) for size in SIZES[:-1])

    def branch(i):
        def run(args):
            return run_layers(SIZES[i], *args)

        return run

    args = (k_t, v_t, lengths, hidden, ln_gain, weights, w_out)
    state, pieces, outs = lax.switch(choice, [branch(i) for i in range(len(SIZES))], args)
    *inputs, residual = state
    part, global_k, global_v = global_layer(w_out.shape[0] - 1, lengths, *inputs, k_t, v_t, pieces, w_out)
    return final(residual, part), outs[0], outs[1], global_k, global_v


SIZES = (34, 50, 64)


def solution(mesh):
    cache_spec = P(None, "dp", "tp", "sp", None)
    row_spec = P(("dp", "sp"), None)
    col_spec = P(None, None, "tp")
    inner_spec = P(None, "tp", None)
    window_spec = P(None, ("dp", "sp"), "tp", None, None)
    global_spec = P(("dp", "sp"), "tp", None, None)
    in_specs = (cache_spec, cache_spec, P("dp"), row_spec, P(None, None), col_spec, col_spec, col_spec, inner_spec, col_spec, col_spec, inner_spec)
    out_specs = (row_spec, window_spec, window_spec, global_spec, global_spec)

    def device_step(k_cache, v_cache, *rest):
        k_t, v_t = jnp.swapaxes(k_cache, 3, 4), jnp.swapaxes(v_cache, 3, 4)
        h, wk, wv, gk, gv = decode(k_t, v_t, *rest)
        turn = lambda x: jnp.swapaxes(x, -1, -2)
        return h, turn(wk)[:, None], turn(wv)[:, None], turn(gk)[None], turn(gv)[None]

    return jax.shard_map(device_step, mesh=mesh, in_specs=in_specs, out_specs=out_specs, check_vma=False)
```

```python
import functools

import jax
import jax.numpy as jnp
from jax import lax
from jax.experimental import pallas as pl
from jax.experimental.pallas import tpu as pltpu
from jax.sharding import PartitionSpec as P


WINDOW = 4096
ROPE_BASE = 50000
NORM_EPS = 1e-5
SHARD = 2048
CHUNK = 128
HEAD_DIM = 64
DEPTH = 5
TILE = 256
CROSS = [(0, 2), (2, 0), (1, 3), (3, 1)]
CROSS_SWAP = [(0, 3), (3, 0), (1, 2), (2, 1)]
PARTNER = [(0, 1), (1, 0), (2, 3), (3, 2)]


VMEM = pl.BlockSpec(memory_space=pltpu.VMEM)
SMEM = pl.BlockSpec(memory_space=pltpu.SMEM)
ANY = pl.BlockSpec(memory_space=pltpu.HBM)
EITHER = pl.BlockSpec(memory_space=pl.ANY)


def params(mib=52, **extra):
    return pltpu.CompilerParams(vmem_limit_bytes=mib * 2**20, **extra)


def place():
    sp = lax.axis_index("sp")
    return sp, lax.rem(sp, 2), sp // 2


def far_chunks(length, on_first_chip):
    turn = length - WINDOW
    start = jnp.where(on_first_chip, 0, (turn + 1) // CHUNK)
    count = jnp.where(on_first_chip, (turn + CHUNK - 1) // CHUNK, WINDOW // CHUNK - (turn + 1) // CHUNK)
    return start, count


def swap_kernel(layers, k_ref, v_ref, far_o, near_o, send_sem, recv_sem):
    sp, core, chip = place()
    peer = sp + 1 - 2 * core
    barrier = pltpu.get_barrier_semaphore()
    pl.semaphore_signal(barrier, inc=1, device_id={"sp": peer}, device_id_type=pl.DeviceIdType.MESH)
    pl.semaphore_wait(barrier, 1)
    far_rows = pl.ds(2 * (1 - chip), 2)

    def send(src, dst, i):
        return pltpu.make_async_remote_copy(
            src_ref=src, dst_ref=dst, send_sem=send_sem.at[i], recv_sem=recv_sem.at[i],
            device_id={"sp": peer}, device_id_type=pl.DeviceIdType.MESH)

    copies = []
    for i, (layer, sliding) in enumerate(layers):
        if sliding:
            @pl.when(core == 0)
            def _(layer=layer, i=i):
                send(v_ref.at[layer, far_rows], far_o.at[i], 3 * i).start()

            @pl.when(core == 1)
            def _(layer=layer, i=i):
                send(k_ref.at[layer, far_rows], far_o.at[i], 3 * i).start()

            copies.append(send(k_ref.at[layer, far_rows], far_o.at[i], 3 * i))
        pair = [send(k_ref.at[layer, peer], near_o.at[i, 0], 3 * i + 1),
                send(v_ref.at[layer, peer], near_o.at[i, 1], 3 * i + 2)]
        for copy in pair:
            copy.start()
        copies += pair
    for copy in copies:
        copy.wait()


def swap(layers, k_t, v_t, collective_id):
    n = len(layers)
    block = jax.ShapeDtypeStruct((n, 2, 2, HEAD_DIM, SHARD), jnp.bfloat16)
    return pl.pallas_call(
        functools.partial(swap_kernel, layers),
        out_shape=[block, block],
        in_specs=[ANY, ANY], out_specs=[ANY, ANY],
        scratch_shapes=[pltpu.SemaphoreType.DMA((3 * n,)), pltpu.SemaphoreType.DMA((3 * n,))],
        compiler_params=params(60, collective_id=collective_id, has_side_effects=True),
        cost_estimate=pl.CostEstimate(flops=10**9, bytes_accessed=4 * 2**20, transcendentals=0),
        name="swap",
    )(k_t, v_t)


def pack_kernel(layer, n_chunks, lengths, k_ref, v_ref, recv_ref, out_ref, sem):
    _, core, chip = place()
    far_row = 2 * (1 - chip)
    start0, count0 = far_chunks(lengths[far_row], chip == 1)
    start1, _ = far_chunks(lengths[far_row + 1], chip == 1)
    per_shard = SHARD // CHUNK

    def step(j, carry):
        second = j >= count0
        row = jnp.where(second, 1, 0)
        piece = jnp.clip(jnp.where(second, start1 + j - count0, start0 + j), 0, 2 * per_shard - 1)
        own = (piece // per_shard) == core
        lanes = pl.ds(pl.multiple_of(lax.rem(piece, per_shard) * CHUNK, CHUNK), CHUNK)

        @pl.when(own & (core == 0))
        def _():
            pltpu.make_async_copy(k_ref.at[layer, far_row + row, :, :, lanes], out_ref.at[j], sem).start()

        @pl.when(own & (core == 1))
        def _():
            pltpu.make_async_copy(v_ref.at[layer, far_row + row, :, :, lanes], out_ref.at[j], sem).start()

        @pl.when(jnp.logical_not(own))
        def _():
            pltpu.make_async_copy(recv_ref.at[0, row, :, :, lanes], out_ref.at[j], sem).start()

        return carry

    lax.fori_loop(0, n_chunks, step, 0)
    pltpu.make_async_copy(out_ref, out_ref, sem).wait()


def pack(layer, n_chunks, lengths, k_t, v_t, recv):
    return pl.pallas_call(
        functools.partial(pack_kernel, layer, n_chunks),
        out_shape=jax.ShapeDtypeStruct((n_chunks, 2, HEAD_DIM, CHUNK), jnp.bfloat16),
        in_specs=[SMEM, ANY, ANY, ANY], out_specs=VMEM,
        scratch_shapes=[pltpu.SemaphoreType.DMA],
        compiler_params=params(60),
        cost_estimate=pl.CostEstimate(flops=10**9, bytes_accessed=4 * 2**20, transcendentals=0),
    )(lengths, k_t, v_t, recv)


def payload_kernel(layer, picks, k_ref, v_ref, *refs):
    sp, core, chip = place()
    rows = {"same": sp + 2 - 4 * chip, "cross": 2 * (1 - chip) + 1 - core}
    sems = refs[-1]
    copies = [pltpu.make_async_copy((k_ref, v_ref)[which].at[layer, rows[kind]], out, sems.at[i])
              for i, ((kind, which), out) in enumerate(zip(picks, refs))]
    for copy in copies:
        copy.start()
    for copy in copies:
        copy.wait()


def payload(layer, picks, k_t, v_t):
    block = jax.ShapeDtypeStruct((2, HEAD_DIM, SHARD), jnp.bfloat16)
    return pl.pallas_call(
        functools.partial(payload_kernel, layer, picks),
        out_shape=[block] * len(picks),
        in_specs=[ANY, ANY], out_specs=[VMEM] * len(picks),
        scratch_shapes=[pltpu.SemaphoreType.DMA((len(picks),))],
        compiler_params=params(60),
        cost_estimate=pl.CostEstimate(flops=10**9, bytes_accessed=len(picks) * 2**20, transcendentals=0),
        name="payload",
    )(k_t, v_t)


def greet_peer():
    pl.semaphore_signal(pltpu.get_barrier_semaphore(), inc=1, device_id={"tp": 1 - lax.axis_index("tp")},
                        device_id_type=pl.DeviceIdType.MESH)


def swap_partials(part_ref, other_ref, sems):
    pl.semaphore_wait(pltpu.get_barrier_semaphore(), 1)
    copy = pltpu.make_async_remote_copy(
        src_ref=part_ref, dst_ref=other_ref, send_sem=sems.at[0], recv_sem=sems.at[1],
        device_id={"tp": 1 - lax.axis_index("tp")}, device_id_type=pl.DeviceIdType.MESH)
    copy.start()
    copy.wait()


class Front:
    def __init__(self, layer, sliding, refs):
        self.layer, self.sliding = layer, sliding
        (self.gain, self.cos, self.sin, self.wq, self.wk, self.wv, self.wg, self.wu, self.wd) = refs[:9]
        (self.q_o, self.k_o, self.v_o, self.m_o, self.h_o) = refs[9:14]
        (self.wq_b, self.wk_b, self.wv_b, self.wg_b, self.wu_b, self.wd_b, self.qkv_sem, self.mlp_sem) = refs[14:]

    def qkv_copies(self):
        pairs = ((self.wq, self.wq_b), (self.wk, self.wk_b), (self.wv, self.wv_b))
        return [pltpu.make_async_copy(src.at[self.layer], dst, self.qkv_sem.at[i]) for i, (src, dst) in enumerate(pairs)]

    def tile_copies(self, j, slot):
        cols = pl.ds(pl.multiple_of(j * TILE, TILE), TILE)
        return [pltpu.make_async_copy(self.wg.at[self.layer, :, cols], self.wg_b.at[slot], self.mlp_sem.at[0, slot]),
                pltpu.make_async_copy(self.wu.at[self.layer, :, cols], self.wu_b.at[slot], self.mlp_sem.at[1, slot]),
                pltpu.make_async_copy(self.wd.at[self.layer, cols, :], self.wd_b.at[slot], self.mlp_sem.at[2, slot])]

    def prefetch(self):
        for copy in self.qkv_copies():
            copy.start()
        for j in range(DEPTH):
            for copy in self.tile_copies(j, j):
                copy.start()

    def rotate(self, x):
        if not self.sliding:
            return x
        width = x.shape[1]
        first = lax.broadcasted_iota(jnp.int32, x.shape, 1) % HEAD_DIM < HEAD_DIM // 2
        swapped = jnp.where(first, pltpu.roll(x, width - HEAD_DIM // 2, 1), pltpu.roll(x, HEAD_DIM // 2, 1))
        return x * self.cos[:, :width] + swapped * self.sin[:, :width]

    def run(self, rows):
        self.h_o[...] = rows.astype(jnp.bfloat16)
        centered = rows - rows.mean(axis=-1, keepdims=True)
        variance = (centered * centered).mean(axis=-1, keepdims=True)
        scaled = centered * lax.rsqrt(variance + NORM_EPS)
        normed = (scaled * self.gain[self.layer:self.layer + 1, :].astype(jnp.float32)).astype(jnp.bfloat16)
        normed = jnp.broadcast_to(normed, (8, normed.shape[1]))
        for copy in self.qkv_copies():
            copy.wait()

        def query_step(j, carry):
            cols = pl.ds(pl.multiple_of(j * TILE, TILE), TILE)
            query = jnp.dot(normed, self.wq_b[:, cols], preferred_element_type=jnp.float32)
            self.q_o[:, cols] = self.rotate(query)[:1].astype(jnp.bfloat16)
            return carry

        lax.fori_loop(0, self.wq_b.shape[1] // TILE, query_step, 0)
        self.k_o[...] = self.rotate(jnp.dot(normed, self.wk_b[...], preferred_element_type=jnp.float32))[:1].astype(jnp.bfloat16)
        self.v_o[...] = jnp.dot(normed, self.wv_b[...], preferred_element_type=jnp.float32)[:1].astype(jnp.bfloat16)
        n_tiles = self.wg.shape[2] // TILE

        def tile_step(j, total):
            slot = lax.rem(j, DEPTH)
            for copy in self.tile_copies(j, slot):
                copy.wait()
            gate = jnp.dot(normed, self.wg_b[slot], preferred_element_type=jnp.float32)
            up = jnp.dot(normed, self.wu_b[slot], preferred_element_type=jnp.float32)
            act = (jax.nn.silu(gate) * up).astype(jnp.bfloat16)
            total = total + jnp.dot(act, self.wd_b[slot], preferred_element_type=jnp.float32)

            @pl.when(j + DEPTH < n_tiles)
            def _():
                for copy in self.tile_copies(j + DEPTH, slot):
                    copy.start()

            return total

        total = lax.fori_loop(0, n_tiles, tile_step, jnp.zeros((8, self.m_o.shape[1]), jnp.float32))
        self.m_o[...] = total[:1]


def front_shapes(dim, weights):
    q_width, kv_width = weights[0].shape[2], weights[1].shape[2]
    out = [jax.ShapeDtypeStruct((1, q_width), jnp.bfloat16), jax.ShapeDtypeStruct((1, kv_width), jnp.bfloat16),
           jax.ShapeDtypeStruct((1, kv_width), jnp.bfloat16), jax.ShapeDtypeStruct((1, dim), jnp.float32),
           jax.ShapeDtypeStruct((1, dim), jnp.bfloat16)]
    scratch = [pltpu.VMEM((dim, q_width), jnp.bfloat16), pltpu.VMEM((dim, kv_width), jnp.bfloat16),
               pltpu.VMEM((dim, kv_width), jnp.bfloat16), pltpu.VMEM((DEPTH, dim, TILE), jnp.bfloat16),
               pltpu.VMEM((DEPTH, dim, TILE), jnp.bfloat16), pltpu.VMEM((DEPTH, TILE, dim), jnp.bfloat16),
               pltpu.SemaphoreType.DMA((3,)), pltpu.SemaphoreType.DMA((3, DEPTH))]
    return out, scratch


def front_kernel(h_ref, *refs):
    part = Front(0, True, refs)
    part.prefetch()
    part.run(h_ref[...].astype(jnp.float32))


def front(h, gain, cos, sin, weights):
    out, scratch = front_shapes(h.shape[1], weights)
    return pl.pallas_call(
        front_kernel,
        out_shape=out,
        in_specs=[VMEM] * 4 + [ANY] * 6,
        out_specs=[VMEM] * 5,
        scratch_shapes=scratch,
        compiler_params=params(),
        cost_estimate=pl.CostEstimate(flops=6 * 10**9, bytes_accessed=40 * 10**6, transcendentals=0),
        name="front",
    )(h, gain, cos, sin, *weights)


def final_kernel(h_ref, part_ref, out_ref, other_ref, sems):
    greet_peer()
    swap_partials(part_ref, other_ref, sems)
    out_ref[...] = (h_ref[...].astype(jnp.float32) + (part_ref[...] + other_ref[...])).astype(jnp.bfloat16)


def final(h, part):
    return pl.pallas_call(
        final_kernel,
        out_shape=jax.ShapeDtypeStruct(h.shape, jnp.bfloat16),
        in_specs=[VMEM, VMEM], out_specs=VMEM,
        scratch_shapes=[pltpu.VMEM(part.shape, jnp.float32), pltpu.SemaphoreType.DMA((2,))],
        compiler_params=params(4, collective_id=1, has_side_effects=True),
        name="final",
    )(h, part)


def as_column(row, base):
    wide = jnp.broadcast_to(row[:, base:base + HEAD_DIM].astype(jnp.float32), (HEAD_DIM, HEAD_DIM))
    eye = (lax.broadcasted_iota(jnp.int32, wide.shape, 0) == lax.broadcasted_iota(jnp.int32, wide.shape, 1))
    return jnp.sum(jnp.where(eye, wide, 0.0), axis=1, keepdims=True).astype(jnp.bfloat16)


def spread_mask(group):
    shape = (group, group * HEAD_DIM)
    return lax.broadcasted_iota(jnp.int32, shape, 1) // HEAD_DIM == lax.broadcasted_iota(jnp.int32, shape, 0)


def attend(q_ref, k_buf, v_buf, last, wo_b, wo_copy, mlp_ref, part_o):
    kv_local = k_buf.shape[0]
    width = q_ref.shape[1] // kv_local
    spread = spread_mask(width // HEAD_DIM)
    fold = (lax.broadcasted_iota(jnp.int32, (HEAD_DIM, width), 1) % HEAD_DIM
            == lax.broadcasted_iota(jnp.int32, (HEAD_DIM, width), 0)).astype(jnp.bfloat16)
    part_o[...] = mlp_ref[...]

    def step(head, carry):
        lanes = pl.ds(pl.multiple_of(head * width, width), width)
        q_row = q_ref[:, lanes].astype(jnp.float32)
        q_wide = jnp.where(spread, jnp.broadcast_to(q_row, spread.shape), 0.0).astype(jnp.bfloat16)
        q = lax.dot_general(q_wide, fold, (((1,), (1,)), ((), ())), preferred_element_type=jnp.float32)
        scores = jnp.dot(q.astype(jnp.bfloat16), k_buf[head], preferred_element_type=jnp.float32) * HEAD_DIM ** -0.5
        if last is not None:
            valid = lax.broadcasted_iota(jnp.int32, scores.shape, 1) <= last
            scores = jnp.where(valid, scores, -1e30)
        top = jnp.max(scores, axis=1, keepdims=True)
        expd = jnp.exp(scores - top)
        weights = (expd / jnp.sum(expd, axis=1, keepdims=True)).astype(jnp.bfloat16)
        mixed = lax.dot_general(weights, v_buf[head], (((1,), (1,)), ((), ())), preferred_element_type=jnp.float32)
        wide = jnp.dot(mixed.astype(jnp.bfloat16), fold, preferred_element_type=jnp.float32)
        row = jnp.sum(jnp.where(spread, wide, 0.0), axis=0, keepdims=True).astype(jnp.bfloat16)

        @pl.when(head == 0)
        def _():
            wo_copy.wait()

        row = jnp.broadcast_to(row, (8, width))
        part_o[...] += jnp.dot(row, wo_b[lanes, :], preferred_element_type=jnp.float32)[:1]
        return carry

    lax.fori_loop(0, kv_local, step, 0)


def layer_kernel(layer, sliding_next, *refs):
    (lengths, q_ref, knew_ref, vnew_ref, mlp_ref, h_ref, k_ref, v_ref, near_ref, mine_ref, other_ref, wo) = refs[:12]
    ins, refs = refs[12:21], refs[21:]
    outs, (wk_o, wv_o), scratch = refs[:5], refs[5:7], refs[7:]
    (k_buf, v_buf, k_far, v_far, wo_b, near_sem, far_sem, wo_sem, out_sem, part_b, other_b, rdma_sem) = scratch[:12]
    front_part = Front(layer + 1, sliding_next, (*ins, *outs, *scratch[12:]))
    greet_peer()
    row, core, chip = place()
    turn = lengths[row] - WINDOW
    start, _ = far_chunks(lengths[row], chip == 0)
    _, count0 = far_chunks(lengths[2 * chip], chip == 0)
    shift = jnp.where(core == 0, 0, count0) - start
    n_far = k_far.shape[0]
    own = pl.ds(pl.multiple_of(core * SHARD, SHARD), SHARD)
    peer = pl.ds(pl.multiple_of((1 - core) * SHARD, SHARD), SHARD)
    loads = [pltpu.make_async_copy(k_ref.at[layer, row], k_buf.at[:, :, own], near_sem.at[0]),
             pltpu.make_async_copy(v_ref.at[layer, row], v_buf.at[:, :, own], near_sem.at[1]),
             pltpu.make_async_copy(near_ref.at[0, 0], k_buf.at[:, :, peer], near_sem.at[2]),
             pltpu.make_async_copy(near_ref.at[0, 1], v_buf.at[:, :, peer], near_sem.at[3])]

    @pl.when(core == 0)
    def _():
        pltpu.make_async_copy(mine_ref, k_far, far_sem.at[0]).start()
        pltpu.make_async_copy(other_ref, v_far, far_sem.at[1]).start()

    @pl.when(core == 1)
    def _():
        pltpu.make_async_copy(other_ref, k_far, far_sem.at[0]).start()
        pltpu.make_async_copy(mine_ref, v_far, far_sem.at[1]).start()

    for copy in loads:
        copy.start()
    wo_copy = pltpu.make_async_copy(wo.at[layer], wo_b, wo_sem)
    wo_copy.start()
    k_new = [as_column(knew_ref[...], head * HEAD_DIM) for head in range(2)]
    v_new = [as_column(vnew_ref[...], head * HEAD_DIM) for head in range(2)]
    for copy in loads:
        copy.wait()
    pltpu.make_async_copy(mine_ref, k_far, far_sem.at[0]).wait()
    pltpu.make_async_copy(mine_ref, v_far, far_sem.at[1]).wait()
    front_part.prefetch()

    def step(c, carry):
        lanes = pl.ds(pl.multiple_of(c * CHUNK, CHUNK), CHUNK)
        piece = jnp.clip(c + shift, 0, n_far - 1)
        slots = c * CHUNK + lax.broadcasted_iota(jnp.int32, (HEAD_DIM, CHUNK), 1)
        from_far = jnp.where(chip == 0, turn - slots, slots - turn) > 0
        is_new = slots == turn
        for head in range(2):
            for buf, far, new in ((k_buf, k_far, k_new), (v_buf, v_far, v_new)):
                near = buf[head, :, lanes]
                mixed = jnp.where(from_far, far[piece, head], near)
                buf[head, :, lanes] = jnp.where(is_new, jnp.broadcast_to(new[head], near.shape), mixed)
        return carry

    lax.fori_loop(0, WINDOW // CHUNK, step, 0)
    stores = [pltpu.make_async_copy(k_buf, wk_o, out_sem.at[0]),
              pltpu.make_async_copy(v_buf, wv_o, out_sem.at[1])]
    for copy in stores:
        copy.start()
    attend(q_ref, k_buf, v_buf, None, wo_b, wo_copy, mlp_ref, part_b)
    swap_partials(part_b, other_b, rdma_sem)
    rows = h_ref[...].astype(jnp.float32) + (part_b[...] + other_b[...])
    front_part.run(rows.astype(jnp.bfloat16).astype(jnp.float32))
    for copy in stores:
        copy.wait()


def sliding_layer(layer, sliding_next, lengths, state, k_t, v_t, near, mine, other, wo, gain, cos, sin, weights):
    dim = state[-1].shape[1]
    args = [lengths, *state, k_t, v_t, near, mine, other, wo, gain, cos, sin, *weights]
    specs = [SMEM] + [VMEM] * 5 + [ANY] * 3 + [EITHER] * 2 + [ANY] + [VMEM] * 3 + [ANY] * 6
    buf = pltpu.VMEM((2, HEAD_DIM, WINDOW), jnp.bfloat16)
    far = pltpu.VMEM(mine.shape, jnp.bfloat16)
    out = jax.ShapeDtypeStruct((2, HEAD_DIM, WINDOW), jnp.bfloat16)
    front_out, front_scratch = front_shapes(dim, weights)
    result = pl.pallas_call(
        functools.partial(layer_kernel, layer, sliding_next),
        out_shape=front_out + [out, out],
        in_specs=specs, out_specs=[VMEM] * 5 + [ANY, ANY],
        scratch_shapes=[buf, buf, far, far, pltpu.VMEM(wo.shape[1:], jnp.bfloat16),
                        pltpu.SemaphoreType.DMA((4,)), pltpu.SemaphoreType.DMA((2,)),
                        pltpu.SemaphoreType.DMA, pltpu.SemaphoreType.DMA((2,)),
                        pltpu.VMEM((1, dim), jnp.float32), pltpu.VMEM((1, dim), jnp.float32),
                        pltpu.SemaphoreType.DMA((2,))] + front_scratch,
        compiler_params=params(collective_id=5 + 6 * SIZES.index(mine.shape[0]) + layer, has_side_effects=True),
        cost_estimate=pl.CostEstimate(flops=8 * 10**9, bytes_accessed=52 * 2**20, transcendentals=0),
    )(*args)
    return result[:5], result[5:]


def emit_kernel(layer, wk_ref, wv_ref, *refs):
    wk_o, wv_o, buf, in_sem, out_sem = refs[-5:]
    arrivals = [pltpu.make_async_copy(ref, buf.at[i], in_sem.at[i]) for i, ref in enumerate((wk_ref, wv_ref))]
    departures = [pltpu.make_async_copy(buf.at[i], ref.at[layer], out_sem.at[i]) for i, ref in enumerate((wk_o, wv_o))]
    for copy in arrivals:
        copy.start()
    for arrival, departure in zip(arrivals, departures):
        arrival.wait()
        departure.start()
    for copy in departures:
        copy.wait()


def emit(layer, windows, outs):
    out = jax.ShapeDtypeStruct((3,) + windows[0].shape, jnp.bfloat16)
    return pl.pallas_call(
        functools.partial(emit_kernel, layer),
        out_shape=[out, out],
        in_specs=[ANY] * (2 + len(outs)), out_specs=[ANY] * 2,
        scratch_shapes=[pltpu.VMEM((2,) + windows[0].shape, jnp.bfloat16), pltpu.SemaphoreType.DMA((2,)),
                        pltpu.SemaphoreType.DMA((2,))],
        input_output_aliases={2: 0, 3: 1} if outs else {},
        compiler_params=params(),
        cost_estimate=pl.CostEstimate(flops=10**9, bytes_accessed=4 * 2**20, transcendentals=0),
    )(*windows, *outs)


def global_kernel(layer, lengths, q_ref, knew_ref, vnew_ref, mlp_ref, k_ref, v_ref, near_ref, *refs):
    pieces = refs[:4]
    (wo, wk_ref, wv_ref, _, _, part_o, gk_o, gv_o, wk_o, wv_o, k_buf, v_buf, wo_b, w_buf, load_sem, wo_sem, out_sem,
     pass_in, pass_out) = refs[4:]
    arrivals = [pltpu.make_async_copy(ref, w_buf.at[i], pass_in.at[i]) for i, ref in enumerate((wk_ref, wv_ref))]
    departures = [pltpu.make_async_copy(w_buf.at[i], ref.at[layer - 1], pass_out.at[i]) for i, ref in enumerate((wk_o, wv_o))]
    row, core, chip = place()
    last = lengths[row]
    across = row + 2 - 4 * chip
    sources = (row + 1 - 2 * core, across, across + 1 - 2 * core)
    lanes = [pl.ds(pl.multiple_of(shard * SHARD, SHARD), SHARD) for shard in (row,) + sources]
    parts = [k_ref.at[layer, row], v_ref.at[layer, row], near_ref.at[1, 0], near_ref.at[1, 1], *pieces]
    loads = [pltpu.make_async_copy(ref, (k_buf, v_buf)[i % 2].at[:, :, lanes[i // 2]], load_sem.at[i])
             for i, ref in enumerate(parts)]
    for copy in loads:
        copy.start()
    wo_copy = pltpu.make_async_copy(wo.at[layer], wo_b, wo_sem)
    wo_copy.start()
    for copy in arrivals:
        copy.start()
    k_new = [as_column(knew_ref[...], head * HEAD_DIM) for head in range(2)]
    v_new = [as_column(vnew_ref[...], head * HEAD_DIM) for head in range(2)]
    for copy in loads:
        copy.wait()

    def step(c, carry):
        lanes = pl.ds(pl.multiple_of(c * CHUNK, CHUNK), CHUNK)
        slots = c * CHUNK + lax.broadcasted_iota(jnp.int32, (HEAD_DIM, CHUNK), 1)
        for head in range(2):
            for buf, new in ((k_buf, k_new), (v_buf, v_new)):
                near = buf[head, :, lanes]
                kept = jnp.where(slots < last, near, jnp.zeros_like(near))
                buf[head, :, lanes] = jnp.where(slots == last, jnp.broadcast_to(new[head], near.shape), kept)
        return carry

    lax.fori_loop(last // CHUNK, 2 * WINDOW // CHUNK, step, 0)
    stores = [pltpu.make_async_copy(k_buf, gk_o, out_sem.at[0]), pltpu.make_async_copy(v_buf, gv_o, out_sem.at[1])]
    for copy in stores:
        copy.start()
    for arrival, departure in zip(arrivals, departures):
        arrival.wait()
        departure.start()
    attend(q_ref, k_buf, v_buf, last, wo_b, wo_copy, mlp_ref, part_o)
    for copy in stores + departures:
        copy.wait()


def global_layer(layer, lengths, q, k_new, v_new, mlp, k_t, v_t, pieces, wo, windows, outs):
    buf = pltpu.VMEM((2, HEAD_DIM, 4 * SHARD), jnp.bfloat16)
    out = jax.ShapeDtypeStruct((2, HEAD_DIM, 4 * SHARD), jnp.bfloat16)
    window = jax.ShapeDtypeStruct(outs[0].shape, jnp.bfloat16)
    return pl.pallas_call(
        functools.partial(global_kernel, layer),
        out_shape=[jax.ShapeDtypeStruct(mlp.shape, jnp.float32), out, out, window, window],
        in_specs=[SMEM] + [VMEM] * 4 + [ANY] * 12, out_specs=[VMEM] + [ANY] * 4,
        scratch_shapes=[buf, buf, pltpu.VMEM(wo.shape[1:], jnp.bfloat16), pltpu.VMEM((2,) + windows[0].shape, jnp.bfloat16),
                        pltpu.SemaphoreType.DMA((8,)), pltpu.SemaphoreType.DMA, pltpu.SemaphoreType.DMA((2,)),
                        pltpu.SemaphoreType.DMA((2,)), pltpu.SemaphoreType.DMA((2,))],
        input_output_aliases={15: 3, 16: 4},
        compiler_params=params(),
        cost_estimate=pl.CostEstimate(flops=3 * 10**9, bytes_accessed=26 * 2**20, transcendentals=0),
        name="global",
    )(lengths, q, k_new, v_new, mlp, k_t, v_t, *pieces, wo, *windows, *outs)


def run_layers(n_chunks, same_k, k_t, v_t, lengths, residual, ln_gain, weights, w_out):
    last = w_out.shape[0] - 1
    same_k = lax.ppermute(same_k, "sp", CROSS)
    streams = []
    for layer in range(last):
        traded = ((layer, True),) if layer < last - 1 else ((layer, True), (last, False))
        far, near = swap(traded, k_t, v_t, 2 + layer)
        packed = pack(layer, n_chunks, lengths, k_t, v_t, far)
        mine = lax.ppermute(packed, "sp", CROSS)
        other = lax.ppermute(mine, "sp", PARTNER)
        streams.append((near, mine, other))
    same_v, cross_k, cross_v = payload(last, (("same", 1), ("cross", 0), ("cross", 1)), k_t, v_t)
    same_v = lax.ppermute(same_v, "sp", CROSS)
    cross_k = lax.ppermute(cross_k, "sp", CROSS_SWAP)
    cross_v = lax.ppermute(cross_v, "sp", CROSS_SWAP)

    my_length = lengths[lax.axis_index("sp")]
    half_dim = HEAD_DIM // 2
    inv_freq = 1.0 / (ROPE_BASE ** (jnp.arange(half_dim, dtype=jnp.float32) * 2.0 / HEAD_DIM))
    angles = my_length.astype(jnp.float32) * inv_freq
    cosine, sine = jnp.cos(angles), jnp.sin(angles)
    cos = jnp.tile(jnp.concatenate([cosine, cosine]), TILE // HEAD_DIM)[None]
    sin = jnp.tile(jnp.concatenate([-sine, sine]), TILE // HEAD_DIM)[None]

    state = front(residual, ln_gain, cos, sin, weights)
    outs = ()
    for layer in range(last):
        state, windows = sliding_layer(layer, layer + 1 < last, lengths, state, k_t, v_t, *streams[layer], w_out,
                                       ln_gain, cos, sin, weights)
        if layer + 1 < last:
            outs = emit(layer, windows, outs)
    return state, (near, same_k, same_v, cross_k, cross_v), windows, outs


def decode(k_t, v_t, lengths, hidden, ln_gain, w_query, w_key, w_value, w_out, w_gate, w_up, w_down):
    weights = (w_query, w_key, w_value, w_gate, w_up, w_down)

    counts = far_chunks(lengths, jnp.arange(4) < 2)[1]
    needed = jnp.maximum(counts[0] + counts[1], counts[2] + counts[3])
    choice = sum((needed > size).astype(jnp.int32) for size in SIZES[:-1])

    def branch(i):
        def run(args):
            return run_layers(SIZES[i], *args)

        return run

    (same_k,) = payload(w_out.shape[0] - 1, (("same", 0),), k_t, v_t)
    args = (same_k, k_t, v_t, lengths, hidden, ln_gain, weights, w_out)
    state, pieces, windows, outs = lax.switch(choice, [branch(i) for i in range(len(SIZES))], args)
    *inputs, residual = state
    part, *caches = global_layer(w_out.shape[0] - 1, lengths, *inputs, k_t, v_t, pieces, w_out, windows, outs)
    global_k, global_v, window_k, window_v = caches
    return final(residual, part), window_k, window_v, global_k, global_v


SIZES = (34, 50, 64)


def solution(mesh):
    cache_spec = P(None, "dp", "tp", "sp", None)
    row_spec = P(("dp", "sp"), None)
    col_spec = P(None, None, "tp")
    inner_spec = P(None, "tp", None)
    window_spec = P(None, ("dp", "sp"), "tp", None, None)
    global_spec = P(("dp", "sp"), "tp", None, None)
    in_specs = (cache_spec, cache_spec, P("dp"), row_spec, P(None, None), col_spec, col_spec, col_spec, inner_spec, col_spec, col_spec, inner_spec)
    out_specs = (row_spec, window_spec, window_spec, global_spec, global_spec)

    def device_step(k_cache, v_cache, *rest):
        k_t, v_t = jnp.swapaxes(k_cache, 3, 4), jnp.swapaxes(v_cache, 3, 4)
        h, wk, wv, gk, gv = decode(k_t, v_t, *rest)
        turn = lambda x: jnp.swapaxes(x, -1, -2)
        return h, turn(wk)[:, None], turn(wv)[:, None], turn(gk)[None], turn(gv)[None]

    return jax.shard_map(device_step, mesh=mesh, in_specs=in_specs, out_specs=out_specs, check_vma=False)
```

```python
import functools

import jax
import jax.numpy as jnp
from jax import lax
from jax.experimental import pallas as pl
from jax.experimental.pallas import tpu as pltpu
from jax.sharding import PartitionSpec as P


WINDOW = 4096
ROPE_BASE = 50000
NORM_EPS = 1e-5
SHARD = 2048
CHUNK = 128
HEAD_DIM = 64
DEPTH = 5
TILE = 256
CROSS = [(0, 2), (2, 0), (1, 3), (3, 1)]
CROSS_SWAP = [(0, 3), (3, 0), (1, 2), (2, 1)]
PARTNER = [(0, 1), (1, 0), (2, 3), (3, 2)]


VMEM = pl.BlockSpec(memory_space=pltpu.VMEM)
SMEM = pl.BlockSpec(memory_space=pltpu.SMEM)
ANY = pl.BlockSpec(memory_space=pltpu.HBM)
EITHER = pl.BlockSpec(memory_space=pl.ANY)


def params(mib=52, **extra):
    return pltpu.CompilerParams(vmem_limit_bytes=mib * 2**20, **extra)


def place():
    sp = lax.axis_index("sp")
    return sp, lax.rem(sp, 2), sp // 2


def far_chunks(length, on_first_chip):
    turn = length - WINDOW
    start = jnp.where(on_first_chip, 0, (turn + 1) // CHUNK)
    count = jnp.where(on_first_chip, (turn + CHUNK - 1) // CHUNK, WINDOW // CHUNK - (turn + 1) // CHUNK)
    return start, count


def trade_kernel(layers, n_chunks, lengths, k_ref, v_ref, out_ref, near_o, both, own_sem, send_sem, recv_sem):
    sp, core, chip = place()
    peer = sp + 1 - 2 * core
    layer = layers[0]
    per_shard = SHARD // CHUNK
    far_row = 2 * (1 - chip)
    barrier = pltpu.get_barrier_semaphore()
    pl.semaphore_signal(barrier, inc=1, device_id={"sp": peer}, device_id_type=pl.DeviceIdType.MESH)

    def send(src, dst, i):
        return pltpu.make_async_remote_copy(
            src_ref=src, dst_ref=dst, send_sem=send_sem.at[i], recv_sem=recv_sem.at[i],
            device_id={"sp": peer}, device_id_type=pl.DeviceIdType.MESH)

    def chunk(ref, i):
        return ref.at[layer, far_row + i // per_shard, :, :, pl.ds(pl.multiple_of(lax.rem(i, per_shard) * CHUNK, CHUNK), CHUNK)]

    def spot(i):
        return both.at[core * 2 * per_shard + i]

    def load(i, carry):
        @pl.when(core == 0)
        def _():
            pltpu.make_async_copy(chunk(k_ref, i), spot(i), own_sem).start()

        @pl.when(core == 1)
        def _():
            pltpu.make_async_copy(chunk(v_ref, i), spot(i), own_sem).start()

        return carry

    def give(i, carry):
        @pl.when(core == 0)
        def _():
            send(chunk(v_ref, i), spot(i), 0).start()

        @pl.when(core == 1)
        def _():
            send(chunk(k_ref, i), spot(i), 0).start()

        return carry

    pl.semaphore_wait(barrier, 1)
    lax.fori_loop(0, 2 * per_shard, give, 0)
    lax.fori_loop(0, 2 * per_shard, load, 0)
    nears = [send(ref.at[layers[i // 2], peer], near_o.at[i // 2, i % 2], 1 + i)
             for i, ref in enumerate((k_ref, v_ref) * len(layers))]
    for copy in nears:
        copy.start()
    start0, count0 = far_chunks(lengths[far_row], chip == 1)
    start1, _ = far_chunks(lengths[far_row + 1], chip == 1)
    half = pl.ds(core * 2 * per_shard, 2 * per_shard)
    other = pl.ds((1 - core) * 2 * per_shard, 2 * per_shard)
    pltpu.make_async_copy(both.at[half], both.at[half], own_sem).wait()
    send(both.at[half], both.at[other], 0).wait_recv()

    def step(j, carry):
        second = j >= count0
        piece = jnp.clip(jnp.where(second, start1 + j - count0, start0 + j), 0, 2 * per_shard - 1)
        out_ref[j] = both[piece + jnp.where(piece >= per_shard, per_shard, 0) + jnp.where(second, per_shard, 0)]
        return carry

    lax.fori_loop(0, n_chunks, step, 0)
    send(both.at[half], both.at[other], 0).wait_send()
    for copy in nears:
        copy.wait()


def trade(layers, n_chunks, lengths, k_t, v_t):
    n = len(layers)
    n_copies = 1 + 2 * n
    return pl.pallas_call(
        functools.partial(trade_kernel, layers, n_chunks),
        out_shape=[jax.ShapeDtypeStruct((n_chunks, 2, HEAD_DIM, CHUNK), jnp.bfloat16),
                   jax.ShapeDtypeStruct((n, 2, 2, HEAD_DIM, SHARD), jnp.bfloat16)],
        in_specs=[SMEM, ANY, ANY], out_specs=[VMEM, ANY],
        scratch_shapes=[pltpu.VMEM((4 * SHARD // CHUNK, 2, HEAD_DIM, CHUNK), jnp.bfloat16), pltpu.SemaphoreType.DMA,
                        pltpu.SemaphoreType.DMA((n_copies,)), pltpu.SemaphoreType.DMA((n_copies,))],
        compiler_params=params(60, collective_id=2 + 6 * SIZES.index(n_chunks) + layers[0], has_side_effects=True),
        cost_estimate=pl.CostEstimate(flops=10**9, bytes_accessed=6 * 2**20, transcendentals=0),
    )(lengths, k_t, v_t)


def payload_kernel(layer, picks, k_ref, v_ref, *refs):
    sp, core, chip = place()
    rows = {"same": sp + 2 - 4 * chip, "cross": 2 * (1 - chip) + 1 - core}
    sems = refs[-1]
    copies = [pltpu.make_async_copy((k_ref, v_ref)[which].at[layer, rows[kind]], out, sems.at[i])
              for i, ((kind, which), out) in enumerate(zip(picks, refs))]
    for copy in copies:
        copy.start()
    for copy in copies:
        copy.wait()


def payload(layer, picks, k_t, v_t):
    block = jax.ShapeDtypeStruct((2, HEAD_DIM, SHARD), jnp.bfloat16)
    return pl.pallas_call(
        functools.partial(payload_kernel, layer, picks),
        out_shape=[block] * len(picks),
        in_specs=[ANY, ANY], out_specs=[VMEM] * len(picks),
        scratch_shapes=[pltpu.SemaphoreType.DMA((len(picks),))],
        compiler_params=params(60),
        cost_estimate=pl.CostEstimate(flops=10**9, bytes_accessed=len(picks) * 2**20, transcendentals=0),
        name="payload",
    )(k_t, v_t)


def greet_peer():
    pl.semaphore_signal(pltpu.get_barrier_semaphore(), inc=1, device_id={"tp": 1 - lax.axis_index("tp")},
                        device_id_type=pl.DeviceIdType.MESH)


def swap_partials(part_ref, other_ref, sems):
    pl.semaphore_wait(pltpu.get_barrier_semaphore(), 1)
    copy = pltpu.make_async_remote_copy(
        src_ref=part_ref, dst_ref=other_ref, send_sem=sems.at[0], recv_sem=sems.at[1],
        device_id={"tp": 1 - lax.axis_index("tp")}, device_id_type=pl.DeviceIdType.MESH)
    copy.start()
    copy.wait()


class Front:
    def __init__(self, layer, sliding, refs):
        self.layer, self.sliding = layer, sliding
        (self.gain, self.cos, self.sin, self.wq, self.wk, self.wv, self.wg, self.wu, self.wd) = refs[:9]
        (self.q_o, self.k_o, self.v_o, self.m_o, self.h_o) = refs[9:14]
        (self.wq_b, self.wk_b, self.wv_b, self.wg_b, self.wu_b, self.wd_b, self.qkv_sem, self.mlp_sem) = refs[14:]

    def qkv_copies(self):
        pairs = ((self.wq, self.wq_b), (self.wk, self.wk_b), (self.wv, self.wv_b))
        return [pltpu.make_async_copy(src.at[self.layer], dst, self.qkv_sem.at[i]) for i, (src, dst) in enumerate(pairs)]

    def tile_copies(self, j, slot):
        cols = pl.ds(pl.multiple_of(j * TILE, TILE), TILE)
        return [pltpu.make_async_copy(self.wg.at[self.layer, :, cols], self.wg_b.at[slot], self.mlp_sem.at[0, slot]),
                pltpu.make_async_copy(self.wu.at[self.layer, :, cols], self.wu_b.at[slot], self.mlp_sem.at[1, slot]),
                pltpu.make_async_copy(self.wd.at[self.layer, cols, :], self.wd_b.at[slot], self.mlp_sem.at[2, slot])]

    def prefetch(self):
        for copy in self.qkv_copies():
            copy.start()
        for j in range(DEPTH):
            for copy in self.tile_copies(j, j):
                copy.start()

    def rotate(self, x):
        if not self.sliding:
            return x
        width = x.shape[1]
        first = lax.broadcasted_iota(jnp.int32, x.shape, 1) % HEAD_DIM < HEAD_DIM // 2
        swapped = jnp.where(first, pltpu.roll(x, width - HEAD_DIM // 2, 1), pltpu.roll(x, HEAD_DIM // 2, 1))
        return x * self.cos[:, :width] + swapped * self.sin[:, :width]

    def run(self, rows):
        self.h_o[...] = rows.astype(jnp.bfloat16)
        centered = rows - rows.mean(axis=-1, keepdims=True)
        variance = (centered * centered).mean(axis=-1, keepdims=True)
        scaled = centered * lax.rsqrt(variance + NORM_EPS)
        normed = (scaled * self.gain[self.layer:self.layer + 1, :].astype(jnp.float32)).astype(jnp.bfloat16)
        normed = jnp.broadcast_to(normed, (8, normed.shape[1]))
        for copy in self.qkv_copies():
            copy.wait()

        def query_step(j, carry):
            cols = pl.ds(pl.multiple_of(j * TILE, TILE), TILE)
            query = jnp.dot(normed, self.wq_b[:, cols], preferred_element_type=jnp.float32)
            self.q_o[:, cols] = self.rotate(query)[:1].astype(jnp.bfloat16)
            return carry

        lax.fori_loop(0, self.wq_b.shape[1] // TILE, query_step, 0)
        self.k_o[...] = self.rotate(jnp.dot(normed, self.wk_b[...], preferred_element_type=jnp.float32))[:1].astype(jnp.bfloat16)
        self.v_o[...] = jnp.dot(normed, self.wv_b[...], preferred_element_type=jnp.float32)[:1].astype(jnp.bfloat16)
        n_tiles = self.wg.shape[2] // TILE

        def tile_step(j, total):
            slot = lax.rem(j, DEPTH)
            for copy in self.tile_copies(j, slot):
                copy.wait()
            gate = jnp.dot(normed, self.wg_b[slot], preferred_element_type=jnp.float32)
            up = jnp.dot(normed, self.wu_b[slot], preferred_element_type=jnp.float32)
            act = (jax.nn.silu(gate) * up).astype(jnp.bfloat16)
            total = total + jnp.dot(act, self.wd_b[slot], preferred_element_type=jnp.float32)

            @pl.when(j + DEPTH < n_tiles)
            def _():
                for copy in self.tile_copies(j + DEPTH, slot):
                    copy.start()

            return total

        total = lax.fori_loop(0, n_tiles, tile_step, jnp.zeros((8, self.m_o.shape[1]), jnp.float32))
        self.m_o[...] = total[:1]


def front_shapes(dim, weights):
    q_width, kv_width = weights[0].shape[2], weights[1].shape[2]
    out = [jax.ShapeDtypeStruct((1, q_width), jnp.bfloat16), jax.ShapeDtypeStruct((1, kv_width), jnp.bfloat16),
           jax.ShapeDtypeStruct((1, kv_width), jnp.bfloat16), jax.ShapeDtypeStruct((1, dim), jnp.float32),
           jax.ShapeDtypeStruct((1, dim), jnp.bfloat16)]
    scratch = [pltpu.VMEM((dim, q_width), jnp.bfloat16), pltpu.VMEM((dim, kv_width), jnp.bfloat16),
               pltpu.VMEM((dim, kv_width), jnp.bfloat16), pltpu.VMEM((DEPTH, dim, TILE), jnp.bfloat16),
               pltpu.VMEM((DEPTH, dim, TILE), jnp.bfloat16), pltpu.VMEM((DEPTH, TILE, dim), jnp.bfloat16),
               pltpu.SemaphoreType.DMA((3,)), pltpu.SemaphoreType.DMA((3, DEPTH))]
    return out, scratch


def front_kernel(h_ref, *refs):
    part = Front(0, True, refs)
    part.prefetch()
    part.run(h_ref[...].astype(jnp.float32))


def front(h, gain, cos, sin, weights):
    out, scratch = front_shapes(h.shape[1], weights)
    return pl.pallas_call(
        front_kernel,
        out_shape=out,
        in_specs=[VMEM] * 4 + [ANY] * 6,
        out_specs=[VMEM] * 5,
        scratch_shapes=scratch,
        compiler_params=params(),
        cost_estimate=pl.CostEstimate(flops=6 * 10**9, bytes_accessed=40 * 10**6, transcendentals=0),
        name="front",
    )(h, gain, cos, sin, *weights)


def final_kernel(h_ref, part_ref, out_ref, other_ref, sems):
    greet_peer()
    swap_partials(part_ref, other_ref, sems)
    out_ref[...] = (h_ref[...].astype(jnp.float32) + (part_ref[...] + other_ref[...])).astype(jnp.bfloat16)


def final(h, part):
    return pl.pallas_call(
        final_kernel,
        out_shape=jax.ShapeDtypeStruct(h.shape, jnp.bfloat16),
        in_specs=[VMEM, VMEM], out_specs=VMEM,
        scratch_shapes=[pltpu.VMEM(part.shape, jnp.float32), pltpu.SemaphoreType.DMA((2,))],
        compiler_params=params(4, collective_id=1, has_side_effects=True),
        name="final",
    )(h, part)


def open_kernel(layer, lengths, k_ref, v_ref, same_o, choice_o, sem):
    sp, _, chip = place()
    copy = pltpu.make_async_copy(k_ref.at[layer, sp + 2 - 4 * chip], same_o, sem)
    copy.start()
    counts = [far_chunks(lengths[row], row < 2)[1] for row in range(4)]
    needed = jnp.maximum(counts[0] + counts[1], counts[2] + counts[3])
    choice_o[0] = sum(jnp.where(needed > size, 1, 0) for size in SIZES[:-1])
    copy.wait()


def open_step(layer, lengths, k_t, v_t):
    return pl.pallas_call(
        functools.partial(open_kernel, layer),
        out_shape=[jax.ShapeDtypeStruct((2, HEAD_DIM, SHARD), jnp.bfloat16), jax.ShapeDtypeStruct((1,), jnp.int32)],
        in_specs=[SMEM, ANY, ANY], out_specs=[VMEM, SMEM],
        scratch_shapes=[pltpu.SemaphoreType.DMA],
        compiler_params=params(60),
        cost_estimate=pl.CostEstimate(flops=10**9, bytes_accessed=2**20, transcendentals=0),
        name="open",
    )(lengths, k_t, v_t)


def as_column(row, base):
    wide = jnp.broadcast_to(row[:, base:base + HEAD_DIM].astype(jnp.float32), (HEAD_DIM, HEAD_DIM))
    eye = (lax.broadcasted_iota(jnp.int32, wide.shape, 0) == lax.broadcasted_iota(jnp.int32, wide.shape, 1))
    return jnp.sum(jnp.where(eye, wide, 0.0), axis=1, keepdims=True).astype(jnp.bfloat16)


def spread_mask(group):
    shape = (group, group * HEAD_DIM)
    return lax.broadcasted_iota(jnp.int32, shape, 1) // HEAD_DIM == lax.broadcasted_iota(jnp.int32, shape, 0)


def attend(q_ref, k_buf, v_buf, last, wo_b, wo_copy, mlp_ref, part_o):
    kv_local = k_buf.shape[0]
    width = q_ref.shape[1] // kv_local
    spread = spread_mask(width // HEAD_DIM)
    fold = (lax.broadcasted_iota(jnp.int32, (HEAD_DIM, width), 1) % HEAD_DIM
            == lax.broadcasted_iota(jnp.int32, (HEAD_DIM, width), 0)).astype(jnp.bfloat16)
    part_o[...] = mlp_ref[...]

    def step(head, carry):
        lanes = pl.ds(pl.multiple_of(head * width, width), width)
        q_row = q_ref[:, lanes].astype(jnp.float32)
        q_wide = jnp.where(spread, jnp.broadcast_to(q_row, spread.shape), 0.0).astype(jnp.bfloat16)
        q = lax.dot_general(q_wide, fold, (((1,), (1,)), ((), ())), preferred_element_type=jnp.float32)
        scores = jnp.dot(q.astype(jnp.bfloat16), k_buf[head], preferred_element_type=jnp.float32) * HEAD_DIM ** -0.5
        if last is not None:
            valid = lax.broadcasted_iota(jnp.int32, scores.shape, 1) <= last
            scores = jnp.where(valid, scores, -1e30)
        top = jnp.max(scores, axis=1, keepdims=True)
        expd = jnp.exp(scores - top)
        weights = (expd / jnp.sum(expd, axis=1, keepdims=True)).astype(jnp.bfloat16)
        mixed = lax.dot_general(weights, v_buf[head], (((1,), (1,)), ((), ())), preferred_element_type=jnp.float32)
        wide = jnp.dot(mixed.astype(jnp.bfloat16), fold, preferred_element_type=jnp.float32)
        row = jnp.sum(jnp.where(spread, wide, 0.0), axis=0, keepdims=True).astype(jnp.bfloat16)

        @pl.when(head == 0)
        def _():
            wo_copy.wait()

        row = jnp.broadcast_to(row, (8, width))
        part_o[...] += jnp.dot(row, wo_b[lanes, :], preferred_element_type=jnp.float32)[:1]
        return carry

    lax.fori_loop(0, kv_local, step, 0)


def layer_kernel(layer, sliding_next, *refs):
    (lengths, q_ref, knew_ref, vnew_ref, mlp_ref, h_ref, k_ref, v_ref, near_ref, mine_ref, other_ref, wo) = refs[:12]
    ins, refs = refs[12:21], refs[21:]
    outs, (wk_o, wv_o), scratch = refs[:5], refs[5:7], refs[7:]
    (k_buf, v_buf, k_far, v_far, wo_b, near_sem, far_sem, wo_sem, out_sem, part_b, other_b, rdma_sem) = scratch[:12]
    front_part = Front(layer + 1, sliding_next, (*ins, *outs, *scratch[12:]))
    greet_peer()
    row, core, chip = place()
    turn = lengths[row] - WINDOW
    start, _ = far_chunks(lengths[row], chip == 0)
    _, count0 = far_chunks(lengths[2 * chip], chip == 0)
    shift = jnp.where(core == 0, 0, count0) - start
    n_far = k_far.shape[0]
    own = pl.ds(pl.multiple_of(core * SHARD, SHARD), SHARD)
    peer = pl.ds(pl.multiple_of((1 - core) * SHARD, SHARD), SHARD)
    loads = [pltpu.make_async_copy(k_ref.at[layer, row], k_buf.at[:, :, own], near_sem.at[0]),
             pltpu.make_async_copy(v_ref.at[layer, row], v_buf.at[:, :, own], near_sem.at[1]),
             pltpu.make_async_copy(near_ref.at[0, 0], k_buf.at[:, :, peer], near_sem.at[2]),
             pltpu.make_async_copy(near_ref.at[0, 1], v_buf.at[:, :, peer], near_sem.at[3])]

    @pl.when(core == 0)
    def _():
        pltpu.make_async_copy(mine_ref, k_far, far_sem.at[0]).start()
        pltpu.make_async_copy(other_ref, v_far, far_sem.at[1]).start()

    @pl.when(core == 1)
    def _():
        pltpu.make_async_copy(other_ref, k_far, far_sem.at[0]).start()
        pltpu.make_async_copy(mine_ref, v_far, far_sem.at[1]).start()

    for copy in loads:
        copy.start()
    wo_copy = pltpu.make_async_copy(wo.at[layer], wo_b, wo_sem)
    wo_copy.start()
    k_new = [as_column(knew_ref[...], head * HEAD_DIM) for head in range(2)]
    v_new = [as_column(vnew_ref[...], head * HEAD_DIM) for head in range(2)]
    for copy in loads:
        copy.wait()
    pltpu.make_async_copy(mine_ref, k_far, far_sem.at[0]).wait()
    pltpu.make_async_copy(mine_ref, v_far, far_sem.at[1]).wait()
    front_part.prefetch()

    def step(c, carry):
        lanes = pl.ds(pl.multiple_of(c * CHUNK, CHUNK), CHUNK)
        piece = jnp.clip(c + shift, 0, n_far - 1)
        slots = c * CHUNK + lax.broadcasted_iota(jnp.int32, (HEAD_DIM, CHUNK), 1)
        from_far = jnp.where(chip == 0, turn - slots, slots - turn) > 0
        is_new = slots == turn
        for head in range(2):
            for buf, far, new in ((k_buf, k_far, k_new), (v_buf, v_far, v_new)):
                near = buf[head, :, lanes]
                mixed = jnp.where(from_far, far[piece, head], near)
                buf[head, :, lanes] = jnp.where(is_new, jnp.broadcast_to(new[head], near.shape), mixed)
        return carry

    lax.fori_loop(0, WINDOW // CHUNK, step, 0)
    stores = [pltpu.make_async_copy(k_buf, wk_o, out_sem.at[0]),
              pltpu.make_async_copy(v_buf, wv_o, out_sem.at[1])]
    for copy in stores:
        copy.start()
    attend(q_ref, k_buf, v_buf, None, wo_b, wo_copy, mlp_ref, part_b)
    swap_partials(part_b, other_b, rdma_sem)
    rows = h_ref[...].astype(jnp.float32) + (part_b[...] + other_b[...])
    front_part.run(rows.astype(jnp.bfloat16).astype(jnp.float32))
    for copy in stores:
        copy.wait()


def sliding_layer(layer, sliding_next, lengths, state, k_t, v_t, near, mine, other, wo, gain, cos, sin, weights):
    dim = state[-1].shape[1]
    args = [lengths, *state, k_t, v_t, near, mine, other, wo, gain, cos, sin, *weights]
    specs = [SMEM] + [VMEM] * 5 + [ANY] * 3 + [EITHER] * 2 + [ANY] + [VMEM] * 3 + [ANY] * 6
    buf = pltpu.VMEM((2, HEAD_DIM, WINDOW), jnp.bfloat16)
    far = pltpu.VMEM(mine.shape, jnp.bfloat16)
    out = jax.ShapeDtypeStruct((2, HEAD_DIM, WINDOW), jnp.bfloat16)
    front_out, front_scratch = front_shapes(dim, weights)
    result = pl.pallas_call(
        functools.partial(layer_kernel, layer, sliding_next),
        out_shape=front_out + [out, out],
        in_specs=specs, out_specs=[VMEM] * 5 + [ANY, ANY],
        scratch_shapes=[buf, buf, far, far, pltpu.VMEM(wo.shape[1:], jnp.bfloat16),
                        pltpu.SemaphoreType.DMA((4,)), pltpu.SemaphoreType.DMA((2,)),
                        pltpu.SemaphoreType.DMA, pltpu.SemaphoreType.DMA((2,)),
                        pltpu.VMEM((1, dim), jnp.float32), pltpu.VMEM((1, dim), jnp.float32),
                        pltpu.SemaphoreType.DMA((2,))] + front_scratch,
        compiler_params=params(collective_id=5 + 6 * SIZES.index(mine.shape[0]) + layer, has_side_effects=True),
        cost_estimate=pl.CostEstimate(flops=8 * 10**9, bytes_accessed=52 * 2**20, transcendentals=0),
    )(*args)
    return result[:5], result[5:]


def emit_kernel(layer, wk_ref, wv_ref, *refs):
    wk_o, wv_o, buf, in_sem, out_sem = refs[-5:]
    arrivals = [pltpu.make_async_copy(ref, buf.at[i], in_sem.at[i]) for i, ref in enumerate((wk_ref, wv_ref))]
    departures = [pltpu.make_async_copy(buf.at[i], ref.at[layer], out_sem.at[i]) for i, ref in enumerate((wk_o, wv_o))]
    for copy in arrivals:
        copy.start()
    for arrival, departure in zip(arrivals, departures):
        arrival.wait()
        departure.start()
    for copy in departures:
        copy.wait()


def emit(layer, windows, outs):
    out = jax.ShapeDtypeStruct((3,) + windows[0].shape, jnp.bfloat16)
    return pl.pallas_call(
        functools.partial(emit_kernel, layer),
        out_shape=[out, out],
        in_specs=[ANY] * (2 + len(outs)), out_specs=[ANY] * 2,
        scratch_shapes=[pltpu.VMEM((2,) + windows[0].shape, jnp.bfloat16), pltpu.SemaphoreType.DMA((2,)),
                        pltpu.SemaphoreType.DMA((2,))],
        input_output_aliases={2: 0, 3: 1} if outs else {},
        compiler_params=params(),
        cost_estimate=pl.CostEstimate(flops=10**9, bytes_accessed=4 * 2**20, transcendentals=0),
    )(*windows, *outs)


def global_kernel(layer, lengths, q_ref, knew_ref, vnew_ref, mlp_ref, k_ref, v_ref, near_ref, *refs):
    pieces = refs[:4]
    (wo, wk_ref, wv_ref, _, _, part_o, gk_o, gv_o, wk_o, wv_o, k_buf, v_buf, wo_b, w_buf, load_sem, wo_sem, out_sem,
     pass_in, pass_out) = refs[4:]
    arrivals = [pltpu.make_async_copy(ref, w_buf.at[i], pass_in.at[i]) for i, ref in enumerate((wk_ref, wv_ref))]
    departures = [pltpu.make_async_copy(w_buf.at[i], ref.at[layer - 1], pass_out.at[i]) for i, ref in enumerate((wk_o, wv_o))]
    row, core, chip = place()
    last = lengths[row]
    across = row + 2 - 4 * chip
    sources = (row + 1 - 2 * core, across, across + 1 - 2 * core)
    lanes = [pl.ds(pl.multiple_of(shard * SHARD, SHARD), SHARD) for shard in (row,) + sources]
    parts = [k_ref.at[layer, row], v_ref.at[layer, row], near_ref.at[1, 0], near_ref.at[1, 1], *pieces]
    loads = [pltpu.make_async_copy(ref, (k_buf, v_buf)[i % 2].at[:, :, lanes[i // 2]], load_sem.at[i])
             for i, ref in enumerate(parts)]
    for copy in loads:
        copy.start()
    wo_copy = pltpu.make_async_copy(wo.at[layer], wo_b, wo_sem)
    wo_copy.start()
    for copy in arrivals:
        copy.start()
    k_new = [as_column(knew_ref[...], head * HEAD_DIM) for head in range(2)]
    v_new = [as_column(vnew_ref[...], head * HEAD_DIM) for head in range(2)]
    for copy in loads:
        copy.wait()

    def step(c, carry):
        lanes = pl.ds(pl.multiple_of(c * CHUNK, CHUNK), CHUNK)
        slots = c * CHUNK + lax.broadcasted_iota(jnp.int32, (HEAD_DIM, CHUNK), 1)
        for head in range(2):
            for buf, new in ((k_buf, k_new), (v_buf, v_new)):
                near = buf[head, :, lanes]
                kept = jnp.where(slots < last, near, jnp.zeros_like(near))
                buf[head, :, lanes] = jnp.where(slots == last, jnp.broadcast_to(new[head], near.shape), kept)
        return carry

    lax.fori_loop(last // CHUNK, 2 * WINDOW // CHUNK, step, 0)
    stores = [pltpu.make_async_copy(k_buf, gk_o, out_sem.at[0]), pltpu.make_async_copy(v_buf, gv_o, out_sem.at[1])]
    for copy in stores:
        copy.start()
    for arrival, departure in zip(arrivals, departures):
        arrival.wait()
        departure.start()
    attend(q_ref, k_buf, v_buf, last, wo_b, wo_copy, mlp_ref, part_o)
    for copy in stores + departures:
        copy.wait()


def global_layer(layer, lengths, q, k_new, v_new, mlp, k_t, v_t, pieces, wo, windows, outs):
    buf = pltpu.VMEM((2, HEAD_DIM, 4 * SHARD), jnp.bfloat16)
    out = jax.ShapeDtypeStruct((2, HEAD_DIM, 4 * SHARD), jnp.bfloat16)
    window = jax.ShapeDtypeStruct(outs[0].shape, jnp.bfloat16)
    return pl.pallas_call(
        functools.partial(global_kernel, layer),
        out_shape=[jax.ShapeDtypeStruct(mlp.shape, jnp.float32), out, out, window, window],
        in_specs=[SMEM] + [VMEM] * 4 + [ANY] * 12, out_specs=[VMEM] + [ANY] * 4,
        scratch_shapes=[buf, buf, pltpu.VMEM(wo.shape[1:], jnp.bfloat16), pltpu.VMEM((2,) + windows[0].shape, jnp.bfloat16),
                        pltpu.SemaphoreType.DMA((8,)), pltpu.SemaphoreType.DMA, pltpu.SemaphoreType.DMA((2,)),
                        pltpu.SemaphoreType.DMA((2,)), pltpu.SemaphoreType.DMA((2,))],
        input_output_aliases={15: 3, 16: 4},
        compiler_params=params(),
        cost_estimate=pl.CostEstimate(flops=3 * 10**9, bytes_accessed=26 * 2**20, transcendentals=0),
        name="global",
    )(lengths, q, k_new, v_new, mlp, k_t, v_t, *pieces, wo, *windows, *outs)


def run_layers(n_chunks, same_k, k_t, v_t, lengths, residual, ln_gain, weights, w_out):
    last = w_out.shape[0] - 1
    same_k = lax.ppermute(same_k, "sp", CROSS)
    streams = []
    for layer in range(last):
        packed, near = trade((layer,) if layer < last - 1 else (layer, last), n_chunks, lengths, k_t, v_t)
        mine = lax.ppermute(packed, "sp", CROSS)
        other = lax.ppermute(mine, "sp", PARTNER)
        streams.append((near, mine, other))
    same_v, cross_k, cross_v = payload(last, (("same", 1), ("cross", 0), ("cross", 1)), k_t, v_t)
    same_v = lax.ppermute(same_v, "sp", CROSS)
    cross_k = lax.ppermute(cross_k, "sp", CROSS_SWAP)
    cross_v = lax.ppermute(cross_v, "sp", CROSS_SWAP)

    my_length = lengths[lax.axis_index("sp")]
    half_dim = HEAD_DIM // 2
    inv_freq = 1.0 / (ROPE_BASE ** (jnp.arange(half_dim, dtype=jnp.float32) * 2.0 / HEAD_DIM))
    angles = my_length.astype(jnp.float32) * inv_freq
    cosine, sine = jnp.cos(angles), jnp.sin(angles)
    cos = jnp.tile(jnp.concatenate([cosine, cosine]), TILE // HEAD_DIM)[None]
    sin = jnp.tile(jnp.concatenate([-sine, sine]), TILE // HEAD_DIM)[None]

    state = front(residual, ln_gain, cos, sin, weights)
    outs = ()
    for layer in range(last):
        state, windows = sliding_layer(layer, layer + 1 < last, lengths, state, k_t, v_t, *streams[layer], w_out,
                                       ln_gain, cos, sin, weights)
        if layer + 1 < last:
            outs = emit(layer, windows, outs)
    return state, (near, same_k, same_v, cross_k, cross_v), windows, outs


def decode(k_t, v_t, lengths, hidden, ln_gain, w_query, w_key, w_value, w_out, w_gate, w_up, w_down):
    weights = (w_query, w_key, w_value, w_gate, w_up, w_down)

    same_k, choice = open_step(w_out.shape[0] - 1, lengths, k_t, v_t)

    def branch(i):
        def run(args):
            return run_layers(SIZES[i], *args)

        return run

    args = (same_k, k_t, v_t, lengths, hidden, ln_gain, weights, w_out)
    state, pieces, windows, outs = lax.switch(choice[0], [branch(i) for i in range(len(SIZES))], args)
    *inputs, residual = state
    part, *caches = global_layer(w_out.shape[0] - 1, lengths, *inputs, k_t, v_t, pieces, w_out, windows, outs)
    global_k, global_v, window_k, window_v = caches
    return final(residual, part), window_k, window_v, global_k, global_v


SIZES = (34, 45, 55, 64)


def solution(mesh):
    cache_spec = P(None, "dp", "tp", "sp", None)
    row_spec = P(("dp", "sp"), None)
    col_spec = P(None, None, "tp")
    inner_spec = P(None, "tp", None)
    window_spec = P(None, ("dp", "sp"), "tp", None, None)
    global_spec = P(("dp", "sp"), "tp", None, None)
    in_specs = (cache_spec, cache_spec, P("dp"), row_spec, P(None, None), col_spec, col_spec, col_spec, inner_spec, col_spec, col_spec, inner_spec)
    out_specs = (row_spec, window_spec, window_spec, global_spec, global_spec)

    def device_step(k_cache, v_cache, *rest):
        k_t, v_t = jnp.swapaxes(k_cache, 3, 4), jnp.swapaxes(v_cache, 3, 4)
        h, wk, wv, gk, gv = decode(k_t, v_t, *rest)
        turn = lambda x: jnp.swapaxes(x, -1, -2)
        return h, turn(wk)[:, None], turn(wv)[:, None], turn(gk)[None], turn(gv)[None]

    return jax.shard_map(device_step, mesh=mesh, in_specs=in_specs, out_specs=out_specs, check_vma=False)
```

```python
import functools

import jax
import jax.numpy as jnp
from jax import lax
from jax.experimental import pallas as pl
from jax.experimental.pallas import tpu as pltpu
from jax.sharding import PartitionSpec as P


WINDOW = 4096
ROPE_BASE = 50000
NORM_EPS = 1e-5
SHARD = 2048
CHUNK = 128
HEAD_DIM = 64
DEPTH = 5
TILE = 256
CROSS = [(0, 2), (2, 0), (1, 3), (3, 1)]
CROSS_SWAP = [(0, 3), (3, 0), (1, 2), (2, 1)]
PARTNER = [(0, 1), (1, 0), (2, 3), (3, 2)]


VMEM = pl.BlockSpec(memory_space=pltpu.VMEM)
SMEM = pl.BlockSpec(memory_space=pltpu.SMEM)
ANY = pl.BlockSpec(memory_space=pltpu.HBM)
EITHER = pl.BlockSpec(memory_space=pl.ANY)


def params(mib=52, **extra):
    return pltpu.CompilerParams(vmem_limit_bytes=mib * 2**20, **extra)


def place():
    sp = lax.axis_index("sp")
    return sp, lax.rem(sp, 2), sp // 2


def far_chunks(length, on_first_chip):
    turn = length - WINDOW
    start = jnp.where(on_first_chip, 0, (turn + 1) // CHUNK)
    count = jnp.where(on_first_chip, (turn + CHUNK - 1) // CHUNK, WINDOW // CHUNK - (turn + 1) // CHUNK)
    return start, count


def trade_kernel(layers, n_chunks, lengths, k_ref, v_ref, out_ref, near_o, both, packed, own_sem, out_sem, send_sem, recv_sem):
    sp, core, chip = place()
    peer = sp + 1 - 2 * core
    layer = layers[0]
    per_shard = SHARD // CHUNK
    far_row = 2 * (1 - chip)
    barrier = pltpu.get_barrier_semaphore()
    pl.semaphore_signal(barrier, inc=1, device_id={"sp": peer}, device_id_type=pl.DeviceIdType.MESH)

    def send(src, dst, i):
        return pltpu.make_async_remote_copy(
            src_ref=src, dst_ref=dst, send_sem=send_sem.at[i], recv_sem=recv_sem.at[i],
            device_id={"sp": peer}, device_id_type=pl.DeviceIdType.MESH)

    def chunk(ref, i):
        return ref.at[layer, far_row + i // per_shard, :, :, pl.ds(pl.multiple_of(lax.rem(i, per_shard) * CHUNK, CHUNK), CHUNK)]

    def spot(i):
        return both.at[core * 2 * per_shard + i]

    def load(i, carry):
        @pl.when(core == 0)
        def _():
            pltpu.make_async_copy(chunk(k_ref, i), spot(i), own_sem).start()

        @pl.when(core == 1)
        def _():
            pltpu.make_async_copy(chunk(v_ref, i), spot(i), own_sem).start()

        return carry

    def give(i, carry):
        @pl.when(core == 0)
        def _():
            send(chunk(v_ref, i), spot(i), 0).start()

        @pl.when(core == 1)
        def _():
            send(chunk(k_ref, i), spot(i), 0).start()

        return carry

    pl.semaphore_wait(barrier, 1)
    lax.fori_loop(0, 2 * per_shard, give, 0)
    lax.fori_loop(0, 2 * per_shard, load, 0)
    nears = [send(ref.at[layers[i // 2], peer], near_o.at[i // 2, i % 2], 1 + i)
             for i, ref in enumerate((k_ref, v_ref) * len(layers))]
    for copy in nears:
        copy.start()
    start0, count0 = far_chunks(lengths[far_row], chip == 1)
    start1, _ = far_chunks(lengths[far_row + 1], chip == 1)
    half = pl.ds(core * 2 * per_shard, 2 * per_shard)
    other = pl.ds((1 - core) * 2 * per_shard, 2 * per_shard)
    pltpu.make_async_copy(both.at[half], both.at[half], own_sem).wait()
    send(both.at[half], both.at[other], 0).wait_recv()

    def step(j, carry):
        second = j >= count0
        piece = jnp.clip(jnp.where(second, start1 + j - count0, start0 + j), 0, 2 * per_shard - 1)
        packed[j] = both[piece + jnp.where(piece >= per_shard, per_shard, 0) + jnp.where(second, per_shard, 0)]
        return carry

    lax.fori_loop(0, n_chunks, step, 0)
    out = pltpu.make_async_copy(packed, out_ref, out_sem)
    out.start()
    send(both.at[half], both.at[other], 0).wait_send()
    for copy in nears:
        copy.wait()
    out.wait()


def trade(layers, n_chunks, lengths, k_t, v_t):
    n = len(layers)
    n_copies = 1 + 2 * n
    return pl.pallas_call(
        functools.partial(trade_kernel, layers, n_chunks),
        out_shape=[jax.ShapeDtypeStruct((n_chunks, 2, HEAD_DIM, CHUNK), jnp.bfloat16),
                   jax.ShapeDtypeStruct((n, 2, 2, HEAD_DIM, SHARD), jnp.bfloat16)],
        in_specs=[SMEM, ANY, ANY], out_specs=[ANY, ANY],
        scratch_shapes=[pltpu.VMEM((4 * SHARD // CHUNK, 2, HEAD_DIM, CHUNK), jnp.bfloat16),
                        pltpu.VMEM((n_chunks, 2, HEAD_DIM, CHUNK), jnp.bfloat16),
                        pltpu.SemaphoreType.DMA, pltpu.SemaphoreType.DMA,
                        pltpu.SemaphoreType.DMA((n_copies,)), pltpu.SemaphoreType.DMA((n_copies,))],
        compiler_params=params(60, collective_id=2 + 6 * SIZES.index(n_chunks) + layers[0], has_side_effects=True),
        cost_estimate=pl.CostEstimate(flops=10**9, bytes_accessed=6 * 2**20, transcendentals=0),
    )(lengths, k_t, v_t)


def payload_kernel(layer, picks, k_ref, v_ref, *refs):
    sp, core, chip = place()
    rows = {"same": sp + 2 - 4 * chip, "cross": 2 * (1 - chip) + 1 - core}
    sems = refs[-1]
    copies = [pltpu.make_async_copy((k_ref, v_ref)[which].at[layer, rows[kind]], out, sems.at[i])
              for i, ((kind, which), out) in enumerate(zip(picks, refs))]
    for copy in copies:
        copy.start()
    for copy in copies:
        copy.wait()


def payload(layer, picks, k_t, v_t):
    block = jax.ShapeDtypeStruct((2, HEAD_DIM, SHARD), jnp.bfloat16)
    return pl.pallas_call(
        functools.partial(payload_kernel, layer, picks),
        out_shape=[block] * len(picks),
        in_specs=[ANY, ANY], out_specs=[VMEM] * len(picks),
        scratch_shapes=[pltpu.SemaphoreType.DMA((len(picks),))],
        compiler_params=params(60),
        cost_estimate=pl.CostEstimate(flops=10**9, bytes_accessed=len(picks) * 2**20, transcendentals=0),
        name="payload",
    )(k_t, v_t)


def greet_peer():
    pl.semaphore_signal(pltpu.get_barrier_semaphore(), inc=1, device_id={"tp": 1 - lax.axis_index("tp")},
                        device_id_type=pl.DeviceIdType.MESH)


def swap_partials(part_ref, other_ref, sems):
    pl.semaphore_wait(pltpu.get_barrier_semaphore(), 1)
    copy = pltpu.make_async_remote_copy(
        src_ref=part_ref, dst_ref=other_ref, send_sem=sems.at[0], recv_sem=sems.at[1],
        device_id={"tp": 1 - lax.axis_index("tp")}, device_id_type=pl.DeviceIdType.MESH)
    copy.start()
    copy.wait()


class Front:
    def __init__(self, layer, sliding, refs):
        self.layer, self.sliding = layer, sliding
        (self.gain, self.cos, self.sin, self.wq, self.wk, self.wv, self.wg, self.wu, self.wd) = refs[:9]
        (self.q_o, self.k_o, self.v_o, self.m_o, self.h_o) = refs[9:14]
        (self.wq_b, self.wk_b, self.wv_b, self.wg_b, self.wu_b, self.wd_b, self.qkv_sem, self.mlp_sem) = refs[14:]

    def qkv_copies(self):
        pairs = ((self.wq, self.wq_b), (self.wk, self.wk_b), (self.wv, self.wv_b))
        return [pltpu.make_async_copy(src.at[self.layer], dst, self.qkv_sem.at[i]) for i, (src, dst) in enumerate(pairs)]

    def tile_copies(self, j, slot):
        cols = pl.ds(pl.multiple_of(j * TILE, TILE), TILE)
        return [pltpu.make_async_copy(self.wg.at[self.layer, :, cols], self.wg_b.at[slot], self.mlp_sem.at[0, slot]),
                pltpu.make_async_copy(self.wu.at[self.layer, :, cols], self.wu_b.at[slot], self.mlp_sem.at[1, slot]),
                pltpu.make_async_copy(self.wd.at[self.layer, cols, :], self.wd_b.at[slot], self.mlp_sem.at[2, slot])]

    def prefetch(self):
        for copy in self.qkv_copies():
            copy.start()
        for j in range(DEPTH):
            for copy in self.tile_copies(j, j):
                copy.start()

    def rotate(self, x):
        if not self.sliding:
            return x
        width = x.shape[1]
        first = lax.broadcasted_iota(jnp.int32, x.shape, 1) % HEAD_DIM < HEAD_DIM // 2
        swapped = jnp.where(first, pltpu.roll(x, width - HEAD_DIM // 2, 1), pltpu.roll(x, HEAD_DIM // 2, 1))
        return x * self.cos[:, :width] + swapped * self.sin[:, :width]

    def run(self, rows):
        self.h_o[...] = rows.astype(jnp.bfloat16)
        centered = rows - rows.mean(axis=-1, keepdims=True)
        variance = (centered * centered).mean(axis=-1, keepdims=True)
        scaled = centered * lax.rsqrt(variance + NORM_EPS)
        normed = (scaled * self.gain[self.layer:self.layer + 1, :].astype(jnp.float32)).astype(jnp.bfloat16)
        normed = jnp.broadcast_to(normed, (8, normed.shape[1]))
        for copy in self.qkv_copies():
            copy.wait()

        def query_step(j, carry):
            cols = pl.ds(pl.multiple_of(j * TILE, TILE), TILE)
            query = jnp.dot(normed, self.wq_b[:, cols], preferred_element_type=jnp.float32)
            self.q_o[:, cols] = self.rotate(query)[:1].astype(jnp.bfloat16)
            return carry

        lax.fori_loop(0, self.wq_b.shape[1] // TILE, query_step, 0)
        self.k_o[...] = self.rotate(jnp.dot(normed, self.wk_b[...], preferred_element_type=jnp.float32))[:1].astype(jnp.bfloat16)
        self.v_o[...] = jnp.dot(normed, self.wv_b[...], preferred_element_type=jnp.float32)[:1].astype(jnp.bfloat16)
        n_tiles = self.wg.shape[2] // TILE

        def tile_step(j, total):
            slot = lax.rem(j, DEPTH)
            for copy in self.tile_copies(j, slot):
                copy.wait()
            gate = jnp.dot(normed, self.wg_b[slot], preferred_element_type=jnp.float32)
            up = jnp.dot(normed, self.wu_b[slot], preferred_element_type=jnp.float32)
            act = (jax.nn.silu(gate) * up).astype(jnp.bfloat16)
            total = total + jnp.dot(act, self.wd_b[slot], preferred_element_type=jnp.float32)

            @pl.when(j + DEPTH < n_tiles)
            def _():
                for copy in self.tile_copies(j + DEPTH, slot):
                    copy.start()

            return total

        total = lax.fori_loop(0, n_tiles, tile_step, jnp.zeros((8, self.m_o.shape[1]), jnp.float32))
        self.m_o[...] = total[:1]


def front_shapes(dim, weights):
    q_width, kv_width = weights[0].shape[2], weights[1].shape[2]
    out = [jax.ShapeDtypeStruct((1, q_width), jnp.bfloat16), jax.ShapeDtypeStruct((1, kv_width), jnp.bfloat16),
           jax.ShapeDtypeStruct((1, kv_width), jnp.bfloat16), jax.ShapeDtypeStruct((1, dim), jnp.float32),
           jax.ShapeDtypeStruct((1, dim), jnp.bfloat16)]
    scratch = [pltpu.VMEM((dim, q_width), jnp.bfloat16), pltpu.VMEM((dim, kv_width), jnp.bfloat16),
               pltpu.VMEM((dim, kv_width), jnp.bfloat16), pltpu.VMEM((DEPTH, dim, TILE), jnp.bfloat16),
               pltpu.VMEM((DEPTH, dim, TILE), jnp.bfloat16), pltpu.VMEM((DEPTH, TILE, dim), jnp.bfloat16),
               pltpu.SemaphoreType.DMA((3,)), pltpu.SemaphoreType.DMA((3, DEPTH))]
    return out, scratch


def front_kernel(h_ref, *refs):
    part = Front(0, True, refs)
    part.prefetch()
    part.run(h_ref[...].astype(jnp.float32))


def front(h, gain, cos, sin, weights):
    out, scratch = front_shapes(h.shape[1], weights)
    return pl.pallas_call(
        front_kernel,
        out_shape=out,
        in_specs=[VMEM] * 4 + [ANY] * 6,
        out_specs=[VMEM] * 5,
        scratch_shapes=scratch,
        compiler_params=params(),
        cost_estimate=pl.CostEstimate(flops=6 * 10**9, bytes_accessed=40 * 10**6, transcendentals=0),
        name="front",
    )(h, gain, cos, sin, *weights)


def final_kernel(h_ref, part_ref, out_ref, other_ref, sems):
    greet_peer()
    swap_partials(part_ref, other_ref, sems)
    out_ref[...] = (h_ref[...].astype(jnp.float32) + (part_ref[...] + other_ref[...])).astype(jnp.bfloat16)


def final(h, part):
    return pl.pallas_call(
        final_kernel,
        out_shape=jax.ShapeDtypeStruct(h.shape, jnp.bfloat16),
        in_specs=[VMEM, VMEM], out_specs=VMEM,
        scratch_shapes=[pltpu.VMEM(part.shape, jnp.float32), pltpu.SemaphoreType.DMA((2,))],
        compiler_params=params(4, collective_id=1, has_side_effects=True),
        name="final",
    )(h, part)


def open_kernel(layer, lengths, k_ref, v_ref, same_o, choice_o, sem):
    sp, _, chip = place()
    copy = pltpu.make_async_copy(k_ref.at[layer, sp + 2 - 4 * chip], same_o, sem)
    copy.start()
    counts = [far_chunks(lengths[row], row < 2)[1] for row in range(4)]
    needed = jnp.maximum(counts[0] + counts[1], counts[2] + counts[3])
    choice_o[0] = sum(jnp.where(needed > size, 1, 0) for size in SIZES[:-1])
    copy.wait()


def open_step(layer, lengths, k_t, v_t):
    return pl.pallas_call(
        functools.partial(open_kernel, layer),
        out_shape=[jax.ShapeDtypeStruct((2, HEAD_DIM, SHARD), jnp.bfloat16), jax.ShapeDtypeStruct((1,), jnp.int32)],
        in_specs=[SMEM, ANY, ANY], out_specs=[VMEM, SMEM],
        scratch_shapes=[pltpu.SemaphoreType.DMA],
        compiler_params=params(60),
        cost_estimate=pl.CostEstimate(flops=10**9, bytes_accessed=2**20, transcendentals=0),
        name="open",
    )(lengths, k_t, v_t)


def as_column(row, base):
    wide = jnp.broadcast_to(row[:, base:base + HEAD_DIM].astype(jnp.float32), (HEAD_DIM, HEAD_DIM))
    eye = (lax.broadcasted_iota(jnp.int32, wide.shape, 0) == lax.broadcasted_iota(jnp.int32, wide.shape, 1))
    return jnp.sum(jnp.where(eye, wide, 0.0), axis=1, keepdims=True).astype(jnp.bfloat16)


def spread_mask(group):
    shape = (group, group * HEAD_DIM)
    return lax.broadcasted_iota(jnp.int32, shape, 1) // HEAD_DIM == lax.broadcasted_iota(jnp.int32, shape, 0)


def attend(q_ref, k_buf, v_buf, last, wo_b, wo_copy, mlp_ref, part_o):
    kv_local = k_buf.shape[0]
    width = q_ref.shape[1] // kv_local
    spread = spread_mask(width // HEAD_DIM)
    fold = (lax.broadcasted_iota(jnp.int32, (HEAD_DIM, width), 1) % HEAD_DIM
            == lax.broadcasted_iota(jnp.int32, (HEAD_DIM, width), 0)).astype(jnp.bfloat16)
    part_o[...] = mlp_ref[...]

    def step(head, carry):
        lanes = pl.ds(pl.multiple_of(head * width, width), width)
        q_row = q_ref[:, lanes].astype(jnp.float32)
        q_wide = jnp.where(spread, jnp.broadcast_to(q_row, spread.shape), 0.0).astype(jnp.bfloat16)
        q = lax.dot_general(q_wide, fold, (((1,), (1,)), ((), ())), preferred_element_type=jnp.float32)
        scores = jnp.dot(q.astype(jnp.bfloat16), k_buf[head], preferred_element_type=jnp.float32) * HEAD_DIM ** -0.5
        if last is not None:
            valid = lax.broadcasted_iota(jnp.int32, scores.shape, 1) <= last
            scores = jnp.where(valid, scores, -1e30)
        top = jnp.max(scores, axis=1, keepdims=True)
        expd = jnp.exp(scores - top)
        weights = (expd / jnp.sum(expd, axis=1, keepdims=True)).astype(jnp.bfloat16)
        mixed = lax.dot_general(weights, v_buf[head], (((1,), (1,)), ((), ())), preferred_element_type=jnp.float32)
        wide = jnp.dot(mixed.astype(jnp.bfloat16), fold, preferred_element_type=jnp.float32)
        row = jnp.sum(jnp.where(spread, wide, 0.0), axis=0, keepdims=True).astype(jnp.bfloat16)

        @pl.when(head == 0)
        def _():
            wo_copy.wait()

        row = jnp.broadcast_to(row, (8, width))
        part_o[...] += jnp.dot(row, wo_b[lanes, :], preferred_element_type=jnp.float32)[:1]
        return carry

    lax.fori_loop(0, kv_local, step, 0)


def layer_kernel(layer, sliding_next, *refs):
    (lengths, q_ref, knew_ref, vnew_ref, mlp_ref, h_ref, k_ref, v_ref, near_ref, mine_ref, other_ref, wo) = refs[:12]
    ins, refs = refs[12:21], refs[21:]
    outs, (wk_o, wv_o), scratch = refs[:5], refs[5:7], refs[7:]
    (k_buf, v_buf, k_far, v_far, wo_b, near_sem, far_sem, wo_sem, out_sem, part_b, other_b, rdma_sem) = scratch[:12]
    front_part = Front(layer + 1, sliding_next, (*ins, *outs, *scratch[12:]))
    greet_peer()
    row, core, chip = place()
    turn = lengths[row] - WINDOW
    start, _ = far_chunks(lengths[row], chip == 0)
    _, count0 = far_chunks(lengths[2 * chip], chip == 0)
    shift = jnp.where(core == 0, 0, count0) - start
    n_far = k_far.shape[0]
    own = pl.ds(pl.multiple_of(core * SHARD, SHARD), SHARD)
    peer = pl.ds(pl.multiple_of((1 - core) * SHARD, SHARD), SHARD)
    loads = [pltpu.make_async_copy(k_ref.at[layer, row], k_buf.at[:, :, own], near_sem.at[0]),
             pltpu.make_async_copy(v_ref.at[layer, row], v_buf.at[:, :, own], near_sem.at[1]),
             pltpu.make_async_copy(near_ref.at[0, 0], k_buf.at[:, :, peer], near_sem.at[2]),
             pltpu.make_async_copy(near_ref.at[0, 1], v_buf.at[:, :, peer], near_sem.at[3])]

    @pl.when(core == 0)
    def _():
        pltpu.make_async_copy(mine_ref, k_far, far_sem.at[0]).start()
        pltpu.make_async_copy(other_ref, v_far, far_sem.at[1]).start()

    @pl.when(core == 1)
    def _():
        pltpu.make_async_copy(other_ref, k_far, far_sem.at[0]).start()
        pltpu.make_async_copy(mine_ref, v_far, far_sem.at[1]).start()

    for copy in loads:
        copy.start()
    wo_copy = pltpu.make_async_copy(wo.at[layer], wo_b, wo_sem)
    wo_copy.start()
    k_new = [as_column(knew_ref[...], head * HEAD_DIM) for head in range(2)]
    v_new = [as_column(vnew_ref[...], head * HEAD_DIM) for head in range(2)]
    for copy in loads:
        copy.wait()
    pltpu.make_async_copy(mine_ref, k_far, far_sem.at[0]).wait()
    pltpu.make_async_copy(mine_ref, v_far, far_sem.at[1]).wait()
    front_part.prefetch()

    def step(c, carry):
        lanes = pl.ds(pl.multiple_of(c * CHUNK, CHUNK), CHUNK)
        piece = jnp.clip(c + shift, 0, n_far - 1)
        slots = c * CHUNK + lax.broadcasted_iota(jnp.int32, (HEAD_DIM, CHUNK), 1)
        from_far = jnp.where(chip == 0, turn - slots, slots - turn) > 0
        is_new = slots == turn
        for head in range(2):
            for buf, far, new in ((k_buf, k_far, k_new), (v_buf, v_far, v_new)):
                near = buf[head, :, lanes]
                mixed = jnp.where(from_far, far[piece, head], near)
                buf[head, :, lanes] = jnp.where(is_new, jnp.broadcast_to(new[head], near.shape), mixed)
        return carry

    lax.fori_loop(0, WINDOW // CHUNK, step, 0)
    stores = [pltpu.make_async_copy(k_buf, wk_o, out_sem.at[0]),
              pltpu.make_async_copy(v_buf, wv_o, out_sem.at[1])]
    for copy in stores:
        copy.start()
    attend(q_ref, k_buf, v_buf, None, wo_b, wo_copy, mlp_ref, part_b)
    swap_partials(part_b, other_b, rdma_sem)
    rows = h_ref[...].astype(jnp.float32) + (part_b[...] + other_b[...])
    front_part.run(rows.astype(jnp.bfloat16).astype(jnp.float32))
    for copy in stores:
        copy.wait()


def sliding_layer(layer, sliding_next, lengths, state, k_t, v_t, near, mine, other, wo, gain, cos, sin, weights):
    dim = state[-1].shape[1]
    args = [lengths, *state, k_t, v_t, near, mine, other, wo, gain, cos, sin, *weights]
    specs = [SMEM] + [VMEM] * 5 + [ANY] * 3 + [EITHER] * 2 + [ANY] + [VMEM] * 3 + [ANY] * 6
    buf = pltpu.VMEM((2, HEAD_DIM, WINDOW), jnp.bfloat16)
    far = pltpu.VMEM(mine.shape, jnp.bfloat16)
    out = jax.ShapeDtypeStruct((2, HEAD_DIM, WINDOW), jnp.bfloat16)
    front_out, front_scratch = front_shapes(dim, weights)
    result = pl.pallas_call(
        functools.partial(layer_kernel, layer, sliding_next),
        out_shape=front_out + [out, out],
        in_specs=specs, out_specs=[VMEM] * 5 + [ANY, ANY],
        scratch_shapes=[buf, buf, far, far, pltpu.VMEM(wo.shape[1:], jnp.bfloat16),
                        pltpu.SemaphoreType.DMA((4,)), pltpu.SemaphoreType.DMA((2,)),
                        pltpu.SemaphoreType.DMA, pltpu.SemaphoreType.DMA((2,)),
                        pltpu.VMEM((1, dim), jnp.float32), pltpu.VMEM((1, dim), jnp.float32),
                        pltpu.SemaphoreType.DMA((2,))] + front_scratch,
        compiler_params=params(collective_id=5 + 6 * SIZES.index(mine.shape[0]) + layer, has_side_effects=True),
        cost_estimate=pl.CostEstimate(flops=8 * 10**9, bytes_accessed=52 * 2**20, transcendentals=0),
    )(*args)
    return result[:5], result[5:]


def emit_kernel(layer, wk_ref, wv_ref, *refs):
    wk_o, wv_o, buf, in_sem, out_sem = refs[-5:]
    arrivals = [pltpu.make_async_copy(ref, buf.at[i], in_sem.at[i]) for i, ref in enumerate((wk_ref, wv_ref))]
    departures = [pltpu.make_async_copy(buf.at[i], ref.at[layer], out_sem.at[i]) for i, ref in enumerate((wk_o, wv_o))]
    for copy in arrivals:
        copy.start()
    for arrival, departure in zip(arrivals, departures):
        arrival.wait()
        departure.start()
    for copy in departures:
        copy.wait()


def emit(layer, windows, outs):
    out = jax.ShapeDtypeStruct((3,) + windows[0].shape, jnp.bfloat16)
    return pl.pallas_call(
        functools.partial(emit_kernel, layer),
        out_shape=[out, out],
        in_specs=[ANY] * (2 + len(outs)), out_specs=[ANY] * 2,
        scratch_shapes=[pltpu.VMEM((2,) + windows[0].shape, jnp.bfloat16), pltpu.SemaphoreType.DMA((2,)),
                        pltpu.SemaphoreType.DMA((2,))],
        input_output_aliases={2: 0, 3: 1} if outs else {},
        compiler_params=params(),
        cost_estimate=pl.CostEstimate(flops=10**9, bytes_accessed=4 * 2**20, transcendentals=0),
    )(*windows, *outs)


def global_kernel(layer, lengths, q_ref, knew_ref, vnew_ref, mlp_ref, k_ref, v_ref, near_ref, *refs):
    pieces, (wo, part_o, gk_o, gv_o, k_buf, v_buf, wo_b, load_sem, wo_sem, out_sem) = refs[:4], refs[4:]
    row, core, chip = place()
    last = lengths[row]
    across = row + 2 - 4 * chip
    sources = (row + 1 - 2 * core, across, across + 1 - 2 * core)
    lanes = [pl.ds(pl.multiple_of(shard * SHARD, SHARD), SHARD) for shard in (row,) + sources]
    parts = [k_ref.at[layer, row], v_ref.at[layer, row], near_ref.at[1, 0], near_ref.at[1, 1], *pieces]
    loads = [pltpu.make_async_copy(ref, (k_buf, v_buf)[i % 2].at[:, :, lanes[i // 2]], load_sem.at[i])
             for i, ref in enumerate(parts)]
    for copy in loads:
        copy.start()
    wo_copy = pltpu.make_async_copy(wo.at[layer], wo_b, wo_sem)
    wo_copy.start()
    k_new = [as_column(knew_ref[...], head * HEAD_DIM) for head in range(2)]
    v_new = [as_column(vnew_ref[...], head * HEAD_DIM) for head in range(2)]
    for copy in loads:
        copy.wait()

    def step(c, carry):
        lanes = pl.ds(pl.multiple_of(c * CHUNK, CHUNK), CHUNK)
        slots = c * CHUNK + lax.broadcasted_iota(jnp.int32, (HEAD_DIM, CHUNK), 1)
        for head in range(2):
            for buf, new in ((k_buf, k_new), (v_buf, v_new)):
                near = buf[head, :, lanes]
                kept = jnp.where(slots < last, near, jnp.zeros_like(near))
                buf[head, :, lanes] = jnp.where(slots == last, jnp.broadcast_to(new[head], near.shape), kept)
        return carry

    lax.fori_loop(last // CHUNK, 2 * WINDOW // CHUNK, step, 0)
    stores = [pltpu.make_async_copy(k_buf, gk_o, out_sem.at[0]), pltpu.make_async_copy(v_buf, gv_o, out_sem.at[1])]
    for copy in stores:
        copy.start()
    attend(q_ref, k_buf, v_buf, last, wo_b, wo_copy, mlp_ref, part_o)
    for copy in stores:
        copy.wait()


def global_layer(layer, lengths, q, k_new, v_new, mlp, k_t, v_t, pieces, wo):
    buf = pltpu.VMEM((2, HEAD_DIM, 4 * SHARD), jnp.bfloat16)
    out = jax.ShapeDtypeStruct((2, HEAD_DIM, 4 * SHARD), jnp.bfloat16)
    return pl.pallas_call(
        functools.partial(global_kernel, layer),
        out_shape=[jax.ShapeDtypeStruct(mlp.shape, jnp.float32), out, out],
        in_specs=[SMEM] + [VMEM] * 4 + [ANY] * 8, out_specs=[VMEM, ANY, ANY],
        scratch_shapes=[buf, buf, pltpu.VMEM(wo.shape[1:], jnp.bfloat16), pltpu.SemaphoreType.DMA((8,)),
                        pltpu.SemaphoreType.DMA, pltpu.SemaphoreType.DMA((2,))],
        compiler_params=params(),
        cost_estimate=pl.CostEstimate(flops=3 * 10**9, bytes_accessed=14 * 2**20, transcendentals=0),
        name="global",
    )(lengths, q, k_new, v_new, mlp, k_t, v_t, *pieces, wo)


def run_layers(n_chunks, same_k, k_t, v_t, lengths, residual, ln_gain, weights, w_out):
    last = w_out.shape[0] - 1
    same_k = lax.ppermute(same_k, "sp", CROSS)
    streams = []
    for layer in range(last):
        packed, near = trade((layer,) if layer < last - 1 else (layer, last), n_chunks, lengths, k_t, v_t)
        mine = lax.ppermute(packed, "sp", CROSS)
        other = lax.ppermute(mine, "sp", PARTNER)
        streams.append((near, mine, other))
    same_v, cross_k, cross_v = payload(last, (("same", 1), ("cross", 0), ("cross", 1)), k_t, v_t)
    same_v = lax.ppermute(same_v, "sp", CROSS)
    cross_k = lax.ppermute(cross_k, "sp", CROSS_SWAP)
    cross_v = lax.ppermute(cross_v, "sp", CROSS_SWAP)

    my_length = lengths[lax.axis_index("sp")]
    half_dim = HEAD_DIM // 2
    inv_freq = 1.0 / (ROPE_BASE ** (jnp.arange(half_dim, dtype=jnp.float32) * 2.0 / HEAD_DIM))
    angles = my_length.astype(jnp.float32) * inv_freq
    cosine, sine = jnp.cos(angles), jnp.sin(angles)
    cos = jnp.tile(jnp.concatenate([cosine, cosine]), TILE // HEAD_DIM)[None]
    sin = jnp.tile(jnp.concatenate([-sine, sine]), TILE // HEAD_DIM)[None]

    state = front(residual, ln_gain, cos, sin, weights)
    outs = ()
    for layer in range(last):
        state, windows = sliding_layer(layer, layer + 1 < last, lengths, state, k_t, v_t, *streams[layer], w_out,
                                       ln_gain, cos, sin, weights)
        outs = emit(layer, windows, outs)
    return state, (near, same_k, same_v, cross_k, cross_v), outs


def decode(k_t, v_t, lengths, hidden, ln_gain, w_query, w_key, w_value, w_out, w_gate, w_up, w_down):
    weights = (w_query, w_key, w_value, w_gate, w_up, w_down)

    same_k, choice = open_step(w_out.shape[0] - 1, lengths, k_t, v_t)

    def branch(i):
        def run(args):
            return run_layers(SIZES[i], *args)

        return run

    args = (same_k, k_t, v_t, lengths, hidden, ln_gain, weights, w_out)
    state, pieces, outs = lax.switch(choice[0], [branch(i) for i in range(len(SIZES))], args)
    *inputs, residual = state
    part, global_k, global_v = global_layer(w_out.shape[0] - 1, lengths, *inputs, k_t, v_t, pieces, w_out)
    return final(residual, part), outs[0], outs[1], global_k, global_v


SIZES = (34, 45, 55, 64)


def solution(mesh):
    cache_spec = P(None, "dp", "tp", "sp", None)
    row_spec = P(("dp", "sp"), None)
    col_spec = P(None, None, "tp")
    inner_spec = P(None, "tp", None)
    window_spec = P(None, ("dp", "sp"), "tp", None, None)
    global_spec = P(("dp", "sp"), "tp", None, None)
    in_specs = (cache_spec, cache_spec, P("dp"), row_spec, P(None, None), col_spec, col_spec, col_spec, inner_spec, col_spec, col_spec, inner_spec)
    out_specs = (row_spec, window_spec, window_spec, global_spec, global_spec)

    def device_step(k_cache, v_cache, *rest):
        k_t, v_t = jnp.swapaxes(k_cache, 3, 4), jnp.swapaxes(v_cache, 3, 4)
        h, wk, wv, gk, gv = decode(k_t, v_t, *rest)
        turn = lambda x: jnp.swapaxes(x, -1, -2)
        return h, turn(wk)[:, None], turn(wv)[:, None], turn(gk)[None], turn(gv)[None]

    return jax.shard_map(device_step, mesh=mesh, in_specs=in_specs, out_specs=out_specs, check_vma=False)
```

```python
import functools

import jax
import jax.numpy as jnp
from jax import lax
from jax.experimental import pallas as pl
from jax.experimental.pallas import tpu as pltpu
from jax.sharding import PartitionSpec as P


WINDOW = 4096
ROPE_BASE = 50000
NORM_EPS = 1e-5
SHARD = 2048
CHUNK = 128
HEAD_DIM = 64
DEPTH = 5
TILE = 256
CROSS = [(0, 2), (2, 0), (1, 3), (3, 1)]
CROSS_SWAP = [(0, 3), (3, 0), (1, 2), (2, 1)]
PARTNER = [(0, 1), (1, 0), (2, 3), (3, 2)]


VMEM = pl.BlockSpec(memory_space=pltpu.VMEM)
SMEM = pl.BlockSpec(memory_space=pltpu.SMEM)
ANY = pl.BlockSpec(memory_space=pltpu.HBM)
EITHER = pl.BlockSpec(memory_space=pl.ANY)


def params(mib=52, **extra):
    return pltpu.CompilerParams(vmem_limit_bytes=mib * 2**20, **extra)


def place():
    sp = lax.axis_index("sp")
    return sp, lax.rem(sp, 2), sp // 2


def far_chunks(length, on_first_chip):
    turn = length - WINDOW
    start = jnp.where(on_first_chip, 0, (turn + 1) // CHUNK)
    count = jnp.where(on_first_chip, (turn + CHUNK - 1) // CHUNK, WINDOW // CHUNK - (turn + 1) // CHUNK)
    return start, count


def trade_kernel(layers, n_chunks, lengths, k_ref, v_ref, out_ref, near_o, both, packed, own_sem, out_sem, send_sem, recv_sem):
    sp, core, chip = place()
    peer = sp + 1 - 2 * core
    layer = layers[0]
    per_shard = SHARD // CHUNK
    far_row = 2 * (1 - chip)
    barrier = pltpu.get_barrier_semaphore()
    pl.semaphore_signal(barrier, inc=1, device_id={"sp": peer}, device_id_type=pl.DeviceIdType.MESH)

    def send(src, dst, i):
        return pltpu.make_async_remote_copy(
            src_ref=src, dst_ref=dst, send_sem=send_sem.at[i], recv_sem=recv_sem.at[i],
            device_id={"sp": peer}, device_id_type=pl.DeviceIdType.MESH)

    def chunk(ref, i):
        return ref.at[layer, far_row + i // per_shard, :, :, pl.ds(pl.multiple_of(lax.rem(i, per_shard) * CHUNK, CHUNK), CHUNK)]

    def spot(i):
        return both.at[core * 2 * per_shard + i]

    def load(i, carry):
        @pl.when(core == 0)
        def _():
            pltpu.make_async_copy(chunk(k_ref, i), spot(i), own_sem).start()

        @pl.when(core == 1)
        def _():
            pltpu.make_async_copy(chunk(v_ref, i), spot(i), own_sem).start()

        return carry

    def give(i, carry):
        @pl.when(core == 0)
        def _():
            send(chunk(v_ref, i), spot(i), 0).start()

        @pl.when(core == 1)
        def _():
            send(chunk(k_ref, i), spot(i), 0).start()

        return carry

    pl.semaphore_wait(barrier, 1)
    lax.fori_loop(0, 2 * per_shard, give, 0)
    lax.fori_loop(0, 2 * per_shard, load, 0)
    nears = [send(ref.at[layers[i // 2], peer], near_o.at[i // 2, i % 2], 1 + i)
             for i, ref in enumerate((k_ref, v_ref) * len(layers))]
    for copy in nears:
        copy.start()
    start0, count0 = far_chunks(lengths[far_row], chip == 1)
    start1, _ = far_chunks(lengths[far_row + 1], chip == 1)
    half = pl.ds(core * 2 * per_shard, 2 * per_shard)
    other = pl.ds((1 - core) * 2 * per_shard, 2 * per_shard)
    pltpu.make_async_copy(both.at[half], both.at[half], own_sem).wait()
    send(both.at[half], both.at[other], 0).wait_recv()

    def step(j, carry):
        second = j >= count0
        piece = jnp.clip(jnp.where(second, start1 + j - count0, start0 + j), 0, 2 * per_shard - 1)
        packed[j] = both[piece + jnp.where(piece >= per_shard, per_shard, 0) + jnp.where(second, per_shard, 0)]
        return carry

    lax.fori_loop(0, n_chunks, step, 0)
    out = pltpu.make_async_copy(packed, out_ref, out_sem)
    out.start()
    send(both.at[half], both.at[other], 0).wait_send()
    for copy in nears:
        copy.wait()
    out.wait()


def trade(layers, n_chunks, lengths, k_t, v_t):
    n = len(layers)
    n_copies = 1 + 2 * n
    return pl.pallas_call(
        functools.partial(trade_kernel, layers, n_chunks),
        out_shape=[jax.ShapeDtypeStruct((n_chunks, 2, HEAD_DIM, CHUNK), jnp.bfloat16),
                   jax.ShapeDtypeStruct((n, 2, 2, HEAD_DIM, SHARD), jnp.bfloat16)],
        in_specs=[SMEM, ANY, ANY], out_specs=[ANY, ANY],
        scratch_shapes=[pltpu.VMEM((4 * SHARD // CHUNK, 2, HEAD_DIM, CHUNK), jnp.bfloat16),
                        pltpu.VMEM((n_chunks, 2, HEAD_DIM, CHUNK), jnp.bfloat16),
                        pltpu.SemaphoreType.DMA, pltpu.SemaphoreType.DMA,
                        pltpu.SemaphoreType.DMA((n_copies,)), pltpu.SemaphoreType.DMA((n_copies,))],
        compiler_params=params(60, collective_id=2 + 6 * SIZES.index(n_chunks) + layers[0], has_side_effects=True),
        cost_estimate=pl.CostEstimate(flops=10**9, bytes_accessed=6 * 2**20, transcendentals=0),
    )(lengths, k_t, v_t)


def payload_kernel(layer, picks, k_ref, v_ref, *refs):
    sp, core, chip = place()
    rows = {"same": sp + 2 - 4 * chip, "cross": 2 * (1 - chip) + 1 - core}
    sems = refs[-1]
    copies = [pltpu.make_async_copy((k_ref, v_ref)[which].at[layer, rows[kind]], out, sems.at[i])
              for i, ((kind, which), out) in enumerate(zip(picks, refs))]
    for copy in copies:
        copy.start()
    for copy in copies:
        copy.wait()


def payload(layer, picks, k_t, v_t):
    block = jax.ShapeDtypeStruct((2, HEAD_DIM, SHARD), jnp.bfloat16)
    return pl.pallas_call(
        functools.partial(payload_kernel, layer, picks),
        out_shape=[block] * len(picks),
        in_specs=[ANY, ANY], out_specs=[VMEM] * len(picks),
        scratch_shapes=[pltpu.SemaphoreType.DMA((len(picks),))],
        compiler_params=params(60),
        cost_estimate=pl.CostEstimate(flops=10**9, bytes_accessed=len(picks) * 2**20, transcendentals=0),
        name="payload",
    )(k_t, v_t)


def greet_peer():
    pl.semaphore_signal(pltpu.get_barrier_semaphore(), inc=1, device_id={"tp": 1 - lax.axis_index("tp")},
                        device_id_type=pl.DeviceIdType.MESH)


def swap_partials(part_ref, other_ref, sems):
    pl.semaphore_wait(pltpu.get_barrier_semaphore(), 1)
    copy = pltpu.make_async_remote_copy(
        src_ref=part_ref, dst_ref=other_ref, send_sem=sems.at[0], recv_sem=sems.at[1],
        device_id={"tp": 1 - lax.axis_index("tp")}, device_id_type=pl.DeviceIdType.MESH)
    copy.start()
    copy.wait()


class Front:
    def __init__(self, layer, sliding, refs):
        self.layer, self.sliding = layer, sliding
        (self.gain, self.cos, self.sin, self.wq, self.wk, self.wv, self.wg, self.wu, self.wd) = refs[:9]
        (self.q_o, self.k_o, self.v_o, self.m_o, self.h_o) = refs[9:14]
        (self.wq_b, self.wk_b, self.wv_b, self.wg_b, self.wu_b, self.wd_b, self.qkv_sem, self.mlp_sem) = refs[14:]

    def qkv_copies(self):
        pairs = ((self.wq, self.wq_b), (self.wk, self.wk_b), (self.wv, self.wv_b))
        return [pltpu.make_async_copy(src.at[self.layer], dst, self.qkv_sem.at[i]) for i, (src, dst) in enumerate(pairs)]

    def tile_copies(self, j, slot):
        cols = pl.ds(pl.multiple_of(j * TILE, TILE), TILE)
        return [pltpu.make_async_copy(self.wg.at[self.layer, :, cols], self.wg_b.at[slot], self.mlp_sem.at[0, slot]),
                pltpu.make_async_copy(self.wu.at[self.layer, :, cols], self.wu_b.at[slot], self.mlp_sem.at[1, slot]),
                pltpu.make_async_copy(self.wd.at[self.layer, cols, :], self.wd_b.at[slot], self.mlp_sem.at[2, slot])]

    def prefetch(self):
        for copy in self.qkv_copies():
            copy.start()
        for j in range(DEPTH):
            for copy in self.tile_copies(j, j):
                copy.start()

    def rotate(self, x):
        if not self.sliding:
            return x
        width = x.shape[1]
        first = lax.broadcasted_iota(jnp.int32, x.shape, 1) % HEAD_DIM < HEAD_DIM // 2
        swapped = jnp.where(first, pltpu.roll(x, width - HEAD_DIM // 2, 1), pltpu.roll(x, HEAD_DIM // 2, 1))
        return x * self.cos[:, :width] + swapped * self.sin[:, :width]

    def run(self, rows):
        self.h_o[...] = rows.astype(jnp.bfloat16)
        centered = rows - rows.mean(axis=-1, keepdims=True)
        variance = (centered * centered).mean(axis=-1, keepdims=True)
        scaled = centered * lax.rsqrt(variance + NORM_EPS)
        normed = (scaled * self.gain[self.layer:self.layer + 1, :].astype(jnp.float32)).astype(jnp.bfloat16)
        normed = jnp.broadcast_to(normed, (8, normed.shape[1]))
        for copy in self.qkv_copies():
            copy.wait()

        def query_step(j, carry):
            cols = pl.ds(pl.multiple_of(j * TILE, TILE), TILE)
            query = jnp.dot(normed, self.wq_b[:, cols], preferred_element_type=jnp.float32)
            self.q_o[:, cols] = self.rotate(query)[:1].astype(jnp.bfloat16)
            return carry

        lax.fori_loop(0, self.wq_b.shape[1] // TILE, query_step, 0)
        self.k_o[...] = self.rotate(jnp.dot(normed, self.wk_b[...], preferred_element_type=jnp.float32))[:1].astype(jnp.bfloat16)
        self.v_o[...] = jnp.dot(normed, self.wv_b[...], preferred_element_type=jnp.float32)[:1].astype(jnp.bfloat16)
        n_tiles = self.wg.shape[2] // TILE

        def tile_step(j, total):
            slot = lax.rem(j, DEPTH)
            for copy in self.tile_copies(j, slot):
                copy.wait()
            gate = jnp.dot(normed, self.wg_b[slot], preferred_element_type=jnp.float32)
            up = jnp.dot(normed, self.wu_b[slot], preferred_element_type=jnp.float32)
            act = (jax.nn.silu(gate) * up).astype(jnp.bfloat16)
            total = total + jnp.dot(act, self.wd_b[slot], preferred_element_type=jnp.float32)

            @pl.when(j + DEPTH < n_tiles)
            def _():
                for copy in self.tile_copies(j + DEPTH, slot):
                    copy.start()

            return total

        total = lax.fori_loop(0, n_tiles, tile_step, jnp.zeros((8, self.m_o.shape[1]), jnp.float32))
        self.m_o[...] = total[:1]


def front_shapes(dim, weights):
    q_width, kv_width = weights[0].shape[2], weights[1].shape[2]
    out = [jax.ShapeDtypeStruct((1, q_width), jnp.bfloat16), jax.ShapeDtypeStruct((1, kv_width), jnp.bfloat16),
           jax.ShapeDtypeStruct((1, kv_width), jnp.bfloat16), jax.ShapeDtypeStruct((1, dim), jnp.float32),
           jax.ShapeDtypeStruct((1, dim), jnp.bfloat16)]
    scratch = [pltpu.VMEM((dim, q_width), jnp.bfloat16), pltpu.VMEM((dim, kv_width), jnp.bfloat16),
               pltpu.VMEM((dim, kv_width), jnp.bfloat16), pltpu.VMEM((DEPTH, dim, TILE), jnp.bfloat16),
               pltpu.VMEM((DEPTH, dim, TILE), jnp.bfloat16), pltpu.VMEM((DEPTH, TILE, dim), jnp.bfloat16),
               pltpu.SemaphoreType.DMA((3,)), pltpu.SemaphoreType.DMA((3, DEPTH))]
    return out, scratch


def front_kernel(h_ref, *refs):
    part = Front(0, True, refs)
    part.prefetch()
    part.run(h_ref[...].astype(jnp.float32))


def front(h, gain, cos, sin, weights):
    out, scratch = front_shapes(h.shape[1], weights)
    return pl.pallas_call(
        front_kernel,
        out_shape=out,
        in_specs=[VMEM] * 4 + [ANY] * 6,
        out_specs=[VMEM] * 5,
        scratch_shapes=scratch,
        compiler_params=params(),
        cost_estimate=pl.CostEstimate(flops=6 * 10**9, bytes_accessed=40 * 10**6, transcendentals=0),
        name="front",
    )(h, gain, cos, sin, *weights)


def final_kernel(h_ref, part_ref, out_ref, other_ref, sems):
    greet_peer()
    swap_partials(part_ref, other_ref, sems)
    out_ref[...] = (h_ref[...].astype(jnp.float32) + (part_ref[...] + other_ref[...])).astype(jnp.bfloat16)


def final(h, part):
    return pl.pallas_call(
        final_kernel,
        out_shape=jax.ShapeDtypeStruct(h.shape, jnp.bfloat16),
        in_specs=[VMEM, VMEM], out_specs=VMEM,
        scratch_shapes=[pltpu.VMEM(part.shape, jnp.float32), pltpu.SemaphoreType.DMA((2,))],
        compiler_params=params(4, collective_id=1, has_side_effects=True),
        name="final",
    )(h, part)


def open_kernel(layer, lengths, k_ref, v_ref, same_o, choice_o, sem):
    sp, _, chip = place()
    copy = pltpu.make_async_copy(k_ref.at[layer, sp + 2 - 4 * chip], same_o, sem)
    copy.start()
    counts = [far_chunks(lengths[row], row < 2)[1] for row in range(4)]
    needed = jnp.maximum(counts[0] + counts[1], counts[2] + counts[3])
    choice_o[0] = sum(jnp.where(needed > size, 1, 0) for size in SIZES[:-1])
    copy.wait()


def open_step(layer, lengths, k_t, v_t):
    return pl.pallas_call(
        functools.partial(open_kernel, layer),
        out_shape=[jax.ShapeDtypeStruct((2, HEAD_DIM, SHARD), jnp.bfloat16), jax.ShapeDtypeStruct((1,), jnp.int32)],
        in_specs=[SMEM, ANY, ANY], out_specs=[VMEM, SMEM],
        scratch_shapes=[pltpu.SemaphoreType.DMA],
        compiler_params=params(60),
        cost_estimate=pl.CostEstimate(flops=10**9, bytes_accessed=2**20, transcendentals=0),
        name="open",
    )(lengths, k_t, v_t)


def as_column(row, base):
    wide = jnp.broadcast_to(row[:, base:base + HEAD_DIM].astype(jnp.float32), (HEAD_DIM, HEAD_DIM))
    eye = (lax.broadcasted_iota(jnp.int32, wide.shape, 0) == lax.broadcasted_iota(jnp.int32, wide.shape, 1))
    return jnp.sum(jnp.where(eye, wide, 0.0), axis=1, keepdims=True).astype(jnp.bfloat16)


def spread_mask(group):
    shape = (group, group * HEAD_DIM)
    return lax.broadcasted_iota(jnp.int32, shape, 1) // HEAD_DIM == lax.broadcasted_iota(jnp.int32, shape, 0)


def fold_matrix(width):
    shape = (HEAD_DIM, width)
    return (lax.broadcasted_iota(jnp.int32, shape, 1) % HEAD_DIM == lax.broadcasted_iota(jnp.int32, shape, 0)).astype(jnp.bfloat16)


def mix_values(weights, values, width):
    mixed = lax.dot_general(weights, values, (((1,), (1,)), ((), ())), preferred_element_type=jnp.float32)
    wide = jnp.dot(mixed.astype(jnp.bfloat16), fold_matrix(width), preferred_element_type=jnp.float32)
    return jnp.sum(jnp.where(spread_mask(width // HEAD_DIM), wide, 0.0), axis=0, keepdims=True).astype(jnp.bfloat16)


def attend(q_ref, k_buf, v_buf, wo_b, wo_copy, mlp_ref, part_o):
    kv_local = k_buf.shape[0]
    width = q_ref.shape[1] // kv_local
    spread = spread_mask(width // HEAD_DIM)
    fold = fold_matrix(width)
    part_o[...] = mlp_ref[...]

    def step(head, carry):
        lanes = pl.ds(pl.multiple_of(head * width, width), width)
        q_row = q_ref[:, lanes].astype(jnp.float32)
        q_wide = jnp.where(spread, jnp.broadcast_to(q_row, spread.shape), 0.0).astype(jnp.bfloat16)
        q = lax.dot_general(q_wide, fold, (((1,), (1,)), ((), ())), preferred_element_type=jnp.float32)
        scores = jnp.dot(q.astype(jnp.bfloat16), k_buf[head], preferred_element_type=jnp.float32) * HEAD_DIM ** -0.5
        top = jnp.max(scores, axis=1, keepdims=True)
        expd = jnp.exp(scores - top)
        weights = (expd / jnp.sum(expd, axis=1, keepdims=True)).astype(jnp.bfloat16)
        row = mix_values(weights, v_buf[head], width)

        @pl.when(head == 0)
        def _():
            wo_copy.wait()

        row = jnp.broadcast_to(row, (8, width))
        part_o[...] += jnp.dot(row, wo_b[lanes, :], preferred_element_type=jnp.float32)[:1]
        return carry

    lax.fori_loop(0, kv_local, step, 0)


def layer_kernel(layer, sliding_next, *refs):
    (lengths, q_ref, knew_ref, vnew_ref, mlp_ref, h_ref, k_ref, v_ref, near_ref, mine_ref, other_ref, wo) = refs[:12]
    ins, refs = refs[12:21], refs[21:]
    outs, (wk_o, wv_o), scratch = refs[:5], refs[5:7], refs[7:]
    (k_buf, v_buf, k_far, v_far, wo_b, near_sem, far_sem, wo_sem, out_sem, part_b, other_b, rdma_sem) = scratch[:12]
    front_part = Front(layer + 1, sliding_next, (*ins, *outs, *scratch[12:]))
    greet_peer()
    row, core, chip = place()
    turn = lengths[row] - WINDOW
    start, _ = far_chunks(lengths[row], chip == 0)
    _, count0 = far_chunks(lengths[2 * chip], chip == 0)
    shift = jnp.where(core == 0, 0, count0) - start
    n_far = k_far.shape[0]
    own = pl.ds(pl.multiple_of(core * SHARD, SHARD), SHARD)
    peer = pl.ds(pl.multiple_of((1 - core) * SHARD, SHARD), SHARD)
    loads = [pltpu.make_async_copy(k_ref.at[layer, row], k_buf.at[:, :, own], near_sem.at[0]),
             pltpu.make_async_copy(v_ref.at[layer, row], v_buf.at[:, :, own], near_sem.at[1]),
             pltpu.make_async_copy(near_ref.at[0, 0], k_buf.at[:, :, peer], near_sem.at[2]),
             pltpu.make_async_copy(near_ref.at[0, 1], v_buf.at[:, :, peer], near_sem.at[3])]

    @pl.when(core == 0)
    def _():
        pltpu.make_async_copy(mine_ref, k_far, far_sem.at[0]).start()
        pltpu.make_async_copy(other_ref, v_far, far_sem.at[1]).start()

    @pl.when(core == 1)
    def _():
        pltpu.make_async_copy(other_ref, k_far, far_sem.at[0]).start()
        pltpu.make_async_copy(mine_ref, v_far, far_sem.at[1]).start()

    for copy in loads:
        copy.start()
    wo_copy = pltpu.make_async_copy(wo.at[layer], wo_b, wo_sem)
    wo_copy.start()
    k_new = [as_column(knew_ref[...], head * HEAD_DIM) for head in range(2)]
    v_new = [as_column(vnew_ref[...], head * HEAD_DIM) for head in range(2)]
    for copy in loads:
        copy.wait()
    pltpu.make_async_copy(mine_ref, k_far, far_sem.at[0]).wait()
    pltpu.make_async_copy(mine_ref, v_far, far_sem.at[1]).wait()
    front_part.prefetch()

    def step(c, carry):
        lanes = pl.ds(pl.multiple_of(c * CHUNK, CHUNK), CHUNK)
        piece = jnp.clip(c + shift, 0, n_far - 1)
        slots = c * CHUNK + lax.broadcasted_iota(jnp.int32, (HEAD_DIM, CHUNK), 1)
        from_far = jnp.where(chip == 0, turn - slots, slots - turn) > 0
        is_new = slots == turn
        for head in range(2):
            for buf, far, new in ((k_buf, k_far, k_new), (v_buf, v_far, v_new)):
                near = buf[head, :, lanes]
                mixed = jnp.where(from_far, far[piece, head], near)
                buf[head, :, lanes] = jnp.where(is_new, jnp.broadcast_to(new[head], near.shape), mixed)
        return carry

    lax.fori_loop(0, WINDOW // CHUNK, step, 0)
    stores = [pltpu.make_async_copy(k_buf, wk_o, out_sem.at[0]),
              pltpu.make_async_copy(v_buf, wv_o, out_sem.at[1])]
    for copy in stores:
        copy.start()
    attend(q_ref, k_buf, v_buf, wo_b, wo_copy, mlp_ref, part_b)
    swap_partials(part_b, other_b, rdma_sem)
    rows = h_ref[...].astype(jnp.float32) + (part_b[...] + other_b[...])
    front_part.run(rows.astype(jnp.bfloat16).astype(jnp.float32))
    for copy in stores:
        copy.wait()


def sliding_layer(layer, sliding_next, lengths, state, k_t, v_t, near, mine, other, wo, gain, cos, sin, weights):
    dim = state[-1].shape[1]
    args = [lengths, *state, k_t, v_t, near, mine, other, wo, gain, cos, sin, *weights]
    specs = [SMEM] + [VMEM] * 5 + [ANY] * 3 + [EITHER] * 2 + [ANY] + [VMEM] * 3 + [ANY] * 6
    buf = pltpu.VMEM((2, HEAD_DIM, WINDOW), jnp.bfloat16)
    far = pltpu.VMEM(mine.shape, jnp.bfloat16)
    out = jax.ShapeDtypeStruct((2, HEAD_DIM, WINDOW), jnp.bfloat16)
    front_out, front_scratch = front_shapes(dim, weights)
    result = pl.pallas_call(
        functools.partial(layer_kernel, layer, sliding_next),
        out_shape=front_out + [out, out],
        in_specs=specs, out_specs=[VMEM] * 5 + [ANY, ANY],
        scratch_shapes=[buf, buf, far, far, pltpu.VMEM(wo.shape[1:], jnp.bfloat16),
                        pltpu.SemaphoreType.DMA((4,)), pltpu.SemaphoreType.DMA((2,)),
                        pltpu.SemaphoreType.DMA, pltpu.SemaphoreType.DMA((2,)),
                        pltpu.VMEM((1, dim), jnp.float32), pltpu.VMEM((1, dim), jnp.float32),
                        pltpu.SemaphoreType.DMA((2,))] + front_scratch,
        compiler_params=params(40, collective_id=5 + 6 * SIZES.index(mine.shape[0]) + layer, has_side_effects=True),
        cost_estimate=pl.CostEstimate(flops=8 * 10**9, bytes_accessed=52 * 2**20, transcendentals=0),
    )(*args)
    return result[:5], result[5:]


def emit_kernel(layer, wk_ref, wv_ref, *refs):
    wk_o, wv_o, buf, in_sem, out_sem = refs[-5:]
    arrivals = [pltpu.make_async_copy(ref, buf.at[i], in_sem.at[i]) for i, ref in enumerate((wk_ref, wv_ref))]
    departures = [pltpu.make_async_copy(buf.at[i], ref.at[layer], out_sem.at[i]) for i, ref in enumerate((wk_o, wv_o))]
    for copy in arrivals:
        copy.start()
    for arrival, departure in zip(arrivals, departures):
        arrival.wait()
        departure.start()
    for copy in departures:
        copy.wait()


def emit(layer, windows, outs):
    out = jax.ShapeDtypeStruct((3,) + windows[0].shape, jnp.bfloat16)
    return pl.pallas_call(
        functools.partial(emit_kernel, layer),
        out_shape=[out, out],
        in_specs=[ANY] * (2 + len(outs)), out_specs=[ANY] * 2,
        scratch_shapes=[pltpu.VMEM((2,) + windows[0].shape, jnp.bfloat16), pltpu.SemaphoreType.DMA((2,)),
                        pltpu.SemaphoreType.DMA((2,))],
        input_output_aliases={2: 0, 3: 1} if outs else {},
        compiler_params=params(),
        cost_estimate=pl.CostEstimate(flops=10**9, bytes_accessed=4 * 2**20, transcendentals=0),
    )(*windows, *outs)


def shard_lanes():
    row, core, chip = place()
    across = row + 2 - 4 * chip
    shards = (row, row + 1 - 2 * core, across, across + 1 - 2 * core)
    return row, [pl.ds(pl.multiple_of(shard * SHARD, SHARD), SHARD) for shard in shards]


def settle(buf, new, last):
    def step(c, carry):
        lanes = pl.ds(pl.multiple_of(c * CHUNK, CHUNK), CHUNK)
        slots = c * CHUNK + lax.broadcasted_iota(jnp.int32, (HEAD_DIM, CHUNK), 1)
        for head in range(2):
            old = buf[head, :, lanes]
            kept = jnp.where(slots < last, old, jnp.zeros_like(old))
            buf[head, :, lanes] = jnp.where(slots == last, jnp.broadcast_to(new[head], old.shape), kept)
        return carry

    lax.fori_loop(last // CHUNK, 2 * WINDOW // CHUNK, step, 0)


def score_kernel(layer, lengths, q_ref, knew_ref, k_ref, near_ref, same_ref, cross_ref, weights_o, gk_o, k_buf, load_sem, out_sem):
    row, lanes = shard_lanes()
    last = lengths[row]
    parts = (k_ref.at[layer, row], near_ref.at[1, 0], same_ref, cross_ref)
    loads = [pltpu.make_async_copy(ref, k_buf.at[:, :, at], load_sem.at[i]) for i, (ref, at) in enumerate(zip(parts, lanes))]
    for copy in loads:
        copy.start()
    k_new = [as_column(knew_ref[...], head * HEAD_DIM) for head in range(2)]
    for copy in loads:
        copy.wait()
    settle(k_buf, k_new, last)
    store = pltpu.make_async_copy(k_buf, gk_o, out_sem)
    store.start()
    width = q_ref.shape[1] // 2
    spread = spread_mask(width // HEAD_DIM)
    fold = fold_matrix(width)

    def step(head, carry):
        q_row = q_ref[:, pl.ds(pl.multiple_of(head * width, width), width)].astype(jnp.float32)
        q_wide = jnp.where(spread, jnp.broadcast_to(q_row, spread.shape), 0.0).astype(jnp.bfloat16)
        q = lax.dot_general(q_wide, fold, (((1,), (1,)), ((), ())), preferred_element_type=jnp.float32)
        scores = jnp.dot(q.astype(jnp.bfloat16), k_buf[head], preferred_element_type=jnp.float32) * HEAD_DIM ** -0.5
        valid = lax.broadcasted_iota(jnp.int32, scores.shape, 1) <= last
        scores = jnp.where(valid, scores, -1e30)
        top = jnp.max(scores, axis=1, keepdims=True)
        expd = jnp.exp(scores - top)
        weights_o[head] = (expd / jnp.sum(expd, axis=1, keepdims=True)).astype(jnp.bfloat16)
        return carry

    lax.fori_loop(0, 2, step, 0)
    store.wait()


def score(layer, lengths, q, k_new, k_t, near, same, cross):
    shape = (2, HEAD_DIM, 4 * SHARD)
    group = q.shape[1] // (2 * HEAD_DIM)
    return pl.pallas_call(
        functools.partial(score_kernel, layer),
        out_shape=[jax.ShapeDtypeStruct((2, group, 4 * SHARD), jnp.bfloat16), jax.ShapeDtypeStruct(shape, jnp.bfloat16)],
        in_specs=[SMEM, VMEM, VMEM] + [ANY] * 4, out_specs=[VMEM, ANY],
        scratch_shapes=[pltpu.VMEM(shape, jnp.bfloat16), pltpu.SemaphoreType.DMA((4,)), pltpu.SemaphoreType.DMA],
        compiler_params=params(),
        cost_estimate=pl.CostEstimate(flops=2 * 10**9, bytes_accessed=4 * 2**20, transcendentals=0),
        name="score",
    )(lengths, q, k_new, k_t, near, same, cross)


def value_kernel(layer, lengths, weights_ref, vnew_ref, mlp_ref, v_ref, near_ref, same_ref, cross_ref, wo, part_o, gv_o,
                 v_buf, wo_b, load_sem, wo_sem, out_sem):
    row, lanes = shard_lanes()
    parts = (v_ref.at[layer, row], near_ref.at[1, 1], same_ref, cross_ref)
    loads = [pltpu.make_async_copy(ref, v_buf.at[:, :, at], load_sem.at[i]) for i, (ref, at) in enumerate(zip(parts, lanes))]
    for copy in loads:
        copy.start()
    wo_copy = pltpu.make_async_copy(wo.at[layer], wo_b, wo_sem)
    wo_copy.start()
    v_new = [as_column(vnew_ref[...], head * HEAD_DIM) for head in range(2)]
    for copy in loads:
        copy.wait()
    settle(v_buf, v_new, lengths[row])
    store = pltpu.make_async_copy(v_buf, gv_o, out_sem)
    store.start()
    width = wo_b.shape[0] // 2
    rows = [mix_values(weights_ref[head], v_buf[head], width) for head in range(2)]
    wo_copy.wait()
    total = mlp_ref[...]
    for head, mixed in enumerate(rows):
        wide = jnp.broadcast_to(mixed, (8, width))
        total = total + jnp.dot(wide, wo_b[head * width:(head + 1) * width, :], preferred_element_type=jnp.float32)[:1]
    part_o[...] = total
    store.wait()


def value(layer, lengths, weights, v_new, mlp, v_t, near, same, cross, wo):
    shape = (2, HEAD_DIM, 4 * SHARD)
    return pl.pallas_call(
        functools.partial(value_kernel, layer),
        out_shape=[jax.ShapeDtypeStruct(mlp.shape, jnp.float32), jax.ShapeDtypeStruct(shape, jnp.bfloat16)],
        in_specs=[SMEM] + [VMEM] * 3 + [ANY] * 5, out_specs=[VMEM, ANY],
        scratch_shapes=[pltpu.VMEM(shape, jnp.bfloat16), pltpu.VMEM(wo.shape[1:], jnp.bfloat16),
                        pltpu.SemaphoreType.DMA((4,)), pltpu.SemaphoreType.DMA, pltpu.SemaphoreType.DMA],
        compiler_params=params(),
        cost_estimate=pl.CostEstimate(flops=2 * 10**9, bytes_accessed=8 * 2**20, transcendentals=0),
        name="value",
    )(lengths, weights, v_new, mlp, v_t, near, same, cross, wo)


def run_layers(n_chunks, same_k, k_t, v_t, lengths, residual, ln_gain, weights, w_out):
    last = w_out.shape[0] - 1
    same_k = lax.ppermute(same_k, "sp", CROSS)
    streams = []
    for layer in range(last):
        packed, near = trade((layer,) if layer < last - 1 else (layer, last), n_chunks, lengths, k_t, v_t)
        mine = lax.ppermute(packed, "sp", CROSS)
        other = lax.ppermute(mine, "sp", PARTNER)
        streams.append((near, mine, other))
    same_v, cross_k, cross_v = payload(last, (("same", 1), ("cross", 0), ("cross", 1)), k_t, v_t)
    same_v = lax.ppermute(same_v, "sp", CROSS)
    cross_k = lax.ppermute(cross_k, "sp", CROSS_SWAP)
    cross_v = lax.ppermute(cross_v, "sp", CROSS_SWAP)

    my_length = lengths[lax.axis_index("sp")]
    half_dim = HEAD_DIM // 2
    inv_freq = 1.0 / (ROPE_BASE ** (jnp.arange(half_dim, dtype=jnp.float32) * 2.0 / HEAD_DIM))
    angles = my_length.astype(jnp.float32) * inv_freq
    cosine, sine = jnp.cos(angles), jnp.sin(angles)
    cos = jnp.tile(jnp.concatenate([cosine, cosine]), TILE // HEAD_DIM)[None]
    sin = jnp.tile(jnp.concatenate([-sine, sine]), TILE // HEAD_DIM)[None]

    state = front(residual, ln_gain, cos, sin, weights)
    outs = ()
    for layer in range(last):
        state, windows = sliding_layer(layer, layer + 1 < last, lengths, state, k_t, v_t, *streams[layer], w_out,
                                       ln_gain, cos, sin, weights)
        outs = emit(layer, windows, outs)
    q, k_new, v_new, mlp, residual = state
    attention, global_k = score(last, lengths, q, k_new, k_t, near, same_k, cross_k)
    return (attention, v_new, mlp), residual, (near, same_v, cross_v), (*outs, global_k)


def decode(k_t, v_t, lengths, hidden, ln_gain, w_query, w_key, w_value, w_out, w_gate, w_up, w_down):
    weights = (w_query, w_key, w_value, w_gate, w_up, w_down)

    same_k, choice = open_step(w_out.shape[0] - 1, lengths, k_t, v_t)

    def branch(i):
        def run(args):
            return run_layers(SIZES[i], *args)

        return run

    args = (same_k, k_t, v_t, lengths, hidden, ln_gain, weights, w_out)
    inputs, residual, pieces, caches = lax.switch(choice[0], [branch(i) for i in range(len(SIZES))], args)
    window_k, window_v, global_k = caches
    part, global_v = value(w_out.shape[0] - 1, lengths, *inputs, v_t, *pieces, w_out)
    return final(residual, part), window_k, window_v, global_k, global_v


SIZES = (33, 45, 55, 64)


def solution(mesh):
    cache_spec = P(None, "dp", "tp", "sp", None)
    row_spec = P(("dp", "sp"), None)
    col_spec = P(None, None, "tp")
    inner_spec = P(None, "tp", None)
    window_spec = P(None, ("dp", "sp"), "tp", None, None)
    global_spec = P(("dp", "sp"), "tp", None, None)
    in_specs = (cache_spec, cache_spec, P("dp"), row_spec, P(None, None), col_spec, col_spec, col_spec, inner_spec, col_spec, col_spec, inner_spec)
    out_specs = (row_spec, window_spec, window_spec, global_spec, global_spec)

    def device_step(k_cache, v_cache, *rest):
        k_t, v_t = jnp.swapaxes(k_cache, 3, 4), jnp.swapaxes(v_cache, 3, 4)
        h, wk, wv, gk, gv = decode(k_t, v_t, *rest)
        turn = lambda x: jnp.swapaxes(x, -1, -2)
        return h, turn(wk)[:, None], turn(wv)[:, None], turn(gk)[None], turn(gv)[None]

    return jax.shard_map(device_step, mesh=mesh, in_specs=in_specs, out_specs=out_specs, check_vma=False)
```
